128 devices in a mesh: grp: 4 (over y), row: 32 (over z, x, core).
Axes of the slice: x: 4, y: 4, z: 4, core: 2. Of those that a mesh axis runs over, the one named last changes fastest.
Arguments:
- tiles: bfloat16 [4, 32, 32, 256, 256], P('grp', 'row'), may hold values from -0.046875 to 0.046875
- tile_rows: int32 [4, 32, 32], P('grp', 'row'), may hold values from 0 to 3, as said below
- tile_cols: int32 [4, 32, 32], P('grp', 'row'), may hold values from 0 to 31, as said below
- live_tiles: int32 [4, 32], P('grp', 'row'), may hold values from 16 to 32, as said below
- dual_shift: float32 [32768], P('row'), may hold values from 0.5 to 2
- start_block: float32 [32, 32768], P(None, 'row'), may hold values from -6 to 6
Outputs:
- projections: float32 [4, 32, 128], replicated
- factors: float32 [4, 32, 32], replicated
- next_block: float32 [32, 32768], P(None, 'row')
The draws below stay inside these ranges and needn't reach their ends.
Inputs may be any that keep to these rules, and one draw needn't show every extreme that they name: `tile_rows`: the tile slots of one device sit at distinct positions (block row, column block), padding slots included. `tile_cols`: column block j of group g is global block column (j // 1) * 4 + g * 1 + j % 1. Slots from live_tiles on are padding with arbitrary values; in every draw some device has all 32 slots live.
All inputs are finite; a program needn't handle non-finite values.
Results may differ from the reference program's by a relative error of at most 0.013.
Values may be sent and summed in bfloat16 or wider, within the bound.
No kernel may reach another device: no remote copies, remote signals or barrier semaphores. Data moves between devices by JAX's collectives and lax.ppermute only.
A program may use at most 64 MiB of HBM per device.

```python
import math
import jax
import jax.numpy as jnp
from jax import lax

K = 32
BS = 256
BR_DEV = 4
KB = 32
ITERS = 4
N = 32768
QB = 1
NCG = 32
M = 128
N_GRP = 4
N_ROW = 32


def tile_slots(key):
    keys = jax.random.split(jax.random.fold_in(key, 7), N_GRP * N_ROW)
    slots = jax.vmap(lambda one_key: jax.random.permutation(one_key, BR_DEV * NCG)[:KB])(keys)
    return slots.reshape(N_GRP, N_ROW, KB).astype(jnp.int32)


def draw_tile_rows(key, part):
    return (tile_slots(key) // NCG).astype(jnp.int32)


def draw_tile_cols(key, part):
    return (tile_slots(key) % NCG).astype(jnp.int32)


def draw_live_tiles(key, part):
    count_key = jax.random.fold_in(key, 11)
    pick_key = jax.random.fold_in(key, 13)
    counts = jax.random.randint(count_key, (N_GRP * N_ROW,), KB // 2, KB + 1)
    picked = jax.random.randint(pick_key, (), 0, N_GRP * N_ROW)
    counts = jnp.where(jnp.arange(N_GRP * N_ROW) == picked, KB, counts)
    return counts.reshape(N_GRP, N_ROW).astype(jnp.int32)


def steps_of(own_key, shape, pieces, low, largest):
    level = 1.0
    for dim, shards_of in pieces:
        heights = jax.random.uniform(jax.random.fold_in(jax.random.fold_in(own_key, 6), dim), (shards_of,), jnp.float32, low / len(pieces), largest / len(pieces))
        level = level * jnp.repeat(jnp.exp(heights), shape[dim] // shards_of).reshape((-1,) + (1,) * (len(shape) - 1 - dim))
    return level


def noise(key, shape, width, reach, shards=(), dtype=jnp.bfloat16):
    array = jax.random.normal(key, shape, jnp.float32) * width
    if len(shards) > 0:
        array = steps_of(key, shape, shards, -0.22, 0.18) * array
    return jnp.clip(array, min=-reach, max=reach).astype(dtype)


def setup_inputs(seed: int = 0) -> dict:
    seeds = jax.random.split(jax.random.key(seed), 7)
    return {
        "tiles": noise(seeds[0], (N_GRP, N_ROW, KB, BS, BS), (KB * N_GRP * 2 * BS // BR_DEV) ** -0.5, 0.046875, ((0, 4), (1, 32))),
        "tile_rows": draw_tile_rows(jax.random.fold_in(seeds[6], 71), 0),
        "tile_cols": draw_tile_cols(jax.random.fold_in(seeds[6], 71), 0),
        "live_tiles": draw_live_tiles(jax.random.fold_in(seeds[6], 71), 0),
        "dual_shift": jnp.clip(jnp.exp(math.log(2.0) - 1.3862944 * jax.random.uniform(seeds[4], (N,), jnp.float32) ** steps_of(seeds[4], (N,), ((0, 32),), -0.2, 0.2)), 0.5, 2.0),
        "start_block": noise(seeds[5], (K, N), 1.0, 6.0, ((1, 32),), jnp.float32),
    }


def inner_product(left, right):
    return lax.dot_general(left.astype(jnp.float32), right.astype(jnp.float32), (((1,), (1,)), ((), ())), precision=lax.Precision.HIGHEST, preferred_element_type=jnp.float32)

def apply_matrix(left, right):
    return jnp.dot(left.astype(jnp.float32), right.astype(jnp.float32), precision=lax.Precision.HIGHEST, preferred_element_type=jnp.float32)

def operate(vectors, tiles, tile_rows, tile_cols, live_tiles):
    rounded = vectors.astype(jnp.bfloat16).astype(jnp.float32).reshape(K, N_ROW, BR_DEV, BS)

    def visit(device, totals):
        direct_sum, back_sum = totals
        group = (device // N_ROW).astype(jnp.int32)
        owner = (device % N_ROW).astype(jnp.int32)
        matrix = tiles[group, owner].astype(jnp.float32)
        rows_here = tile_rows[group, owner]
        cols_here = tile_cols[group, owner]
        live_mask = (jnp.arange(KB) < live_tiles[group, owner]).astype(jnp.float32)
        column_part = lax.dynamic_slice_in_dim(rounded, group * QB, QB, 2).reshape(K, NCG, BS)
        own_part = lax.dynamic_index_in_dim(rounded, owner, 1, False)
        forward = jnp.einsum('kbc,brc->kbr', column_part[:, cols_here], matrix)
        row_table = (rows_here[:, None] == jnp.arange(BR_DEV)[None, :]).astype(jnp.float32) * live_mask[:, None]
        direct = jnp.einsum('kbr,bi->kir', forward, row_table)
        backward = jnp.einsum('kbr,brc->kbc', own_part[:, rows_here], matrix)
        col_table = (cols_here[:, None] == jnp.arange(NCG)[None, :]).astype(jnp.float32) * live_mask[:, None]
        spread = jnp.einsum('kbc,bj->kjc', backward, col_table).reshape(K, N_ROW, QB, BS)
        old_direct = lax.dynamic_index_in_dim(direct_sum, owner, 1, False)
        direct_sum = lax.dynamic_update_index_in_dim(direct_sum, old_direct + direct, owner, 1)
        old_back = lax.dynamic_index_in_dim(back_sum, group, 2, False)
        back_sum = lax.dynamic_update_index_in_dim(back_sum, old_back + spread, group, 2)
        return (direct_sum, back_sum)
    begin = (jnp.zeros((K, N_ROW, BR_DEV, BS), jnp.float32), jnp.zeros((K, N_ROW, N_GRP, QB, BS), jnp.float32))
    direct_sum, back_sum = lax.fori_loop(0, N_GRP * N_ROW, visit, begin)
    return 0.5 * (direct_sum.reshape(K, N) + back_sum.reshape(K, N))

def orthonormal(block):
    lower_factor = jnp.linalg.cholesky(inner_product(block, block))
    return (lax.linalg.triangular_solve(lower_factor, block, left_side=True, lower=True), lower_factor)

def reference(tiles, tile_rows, tile_cols, live_tiles, dual_shift, start_block):
    current, unused = orthonormal(start_block)
    basis_rows = jnp.zeros((M, N), jnp.float32)
    proj_list = []
    factor_list = []
    for step_index in range(ITERS):
        basis_rows = basis_rows.at[step_index * K:(step_index + 1) * K].set(current)
        image = operate(current, tiles, tile_rows, tile_cols, live_tiles) - current * dual_shift[None, :]
        first_coef = inner_product(image, basis_rows)
        image = image - apply_matrix(first_coef, basis_rows)
        current, lower_factor = orthonormal(image)
        proj_list.append(first_coef)
        factor_list.append(lower_factor)
    return (jnp.stack(proj_list), jnp.stack(factor_list), current)
```

```python
import jax
import jax.numpy as jnp
from jax import lax
from jax.sharding import PartitionSpec as P

ITERS = 4
SHIFT = 1.0625
PULL = 0.375

F32 = jnp.float32
BF16 = jnp.bfloat16
HIGHEST = lax.Precision.HIGHEST


def exchange(parts, axis):
    return lax.all_to_all(parts, axis, split_axis=0, concat_axis=0, tiled=True)


def copies(value, axis):
    return exchange(jnp.broadcast_to(value[None], (lax.axis_size(axis), *value.shape)), axis)


def dot(left, right, dims):
    return lax.dot_general(
        left, right, (dims, ((), ())), precision=HIGHEST, preferred_element_type=F32
    )


def per_device(tiles, tile_rows, tile_cols, live_tiles, dual_shift, start_block):
    matrix = tiles[0, 0]
    rows_here = tile_rows[0, 0]
    cols_here = tile_cols[0, 0]
    tile_count, edge, _ = matrix.shape
    width, row_count = start_block.shape
    blocks = row_count // edge
    owners = lax.axis_size("row")
    group = lax.axis_index("grp")
    live_mask = (jnp.arange(tile_count) < live_tiles[0, 0]).astype(F32)
    row_table = (rows_here[:, None] == jnp.arange(blocks)[None, :]).astype(F32) * live_mask[:, None]
    col_table = (cols_here[:, None] == jnp.arange(owners)[None, :]).astype(F32) * live_mask[:, None]

    def forward(columns):
        products = jnp.einsum(
            "bkc,brc->bkr", jnp.take(columns, cols_here, axis=0), matrix,
            preferred_element_type=F32,
        )
        return jnp.einsum("bkr,bi->ikr", products, row_table)

    def backward(own_rows):
        products = jnp.einsum(
            "bkr,brc->bkc", jnp.take(own_rows, rows_here, axis=0), matrix,
            preferred_element_type=F32,
        )
        return jnp.einsum("bkc,bj->jkc", products, col_table)

    full = jnp.moveaxis(start_block.reshape(width, blocks, edge), 1, 0)
    shift_own = lax.dynamic_index_in_dim(dual_shift.reshape(blocks, edge), group, 0, False)
    own = lax.dynamic_index_in_dim(full, group, 0, False)
    before = None
    basis = [full]
    for step in range(ITERS):
        columns = copies(own.astype(BF16), "row")
        back = exchange(backward(full.astype(BF16)).astype(BF16), "row")
        direct = exchange(forward(columns), "grp")
        image = 0.5 * (back.astype(F32).sum(0) + direct.sum(0))
        following = image + (SHIFT - shift_own)[None, :] * own
        if before is not None:
            following = following - PULL * before
        before, own = own, following
        full = copies(own, "grp")
        basis.append(full)

    vectors = jnp.concatenate(basis, 1)
    total = (ITERS + 1) * width
    partial = sum(dot(vectors[i], vectors[i], ((1,), (1,))) for i in range(blocks))
    gram = exchange(partial.reshape(owners, total // owners, total), "row").sum(0)
    gram = copies(gram, "row").reshape(total, total)
    lower = jnp.linalg.cholesky(gram)
    inverse = lax.linalg.triangular_solve(lower, jnp.eye(total, dtype=F32), left_side=True, lower=True)
    used = ITERS * width
    image_rows = lower[width:] - SHIFT * lower[:used]
    image_rows = image_rows + PULL * jnp.concatenate([jnp.zeros((width, total), F32), lower[: used - width]])
    hessenberg = dot(inverse[:used, :used], image_rows, ((1,), (0,)))
    blocked = hessenberg.reshape(ITERS, width, ITERS + 1, width)
    at = jnp.arange(ITERS)
    keep = (jnp.arange(ITERS)[None, :] <= at[:, None]).astype(F32)
    projections = (blocked[:, :, :ITERS] * keep[:, None, :, None]).reshape(ITERS, width, used)
    factors = jnp.stack([blocked[j, :, j + 1] for j in range(ITERS)]) * jnp.tril(jnp.ones((width, width), F32))
    last = jnp.stack([dot(inverse[used:], vectors[i], ((1,), (0,))) for i in range(blocks)], 1)
    return (projections, factors, last.reshape(width, row_count))


def solution(mesh):
    in_specs = (
        P("grp", "row", None, None, None),
        P("grp", "row", None),
        P("grp", "row", None),
        P("grp", "row"),
        P("row"),
        P(None, "row"),
    )
    out_specs = (P(), P(), P(None, "row"))
    return jax.shard_map(
        per_device, mesh=mesh, in_specs=in_specs, out_specs=out_specs, check_vma=False
    )
```

```python
import functools

import jax
import jax.numpy as jnp
from jax import lax
from jax.experimental import pallas as pl
from jax.experimental.pallas import tpu as pltpu
from jax.sharding import PartitionSpec as P

ITERS = 4
SHIFT = 1.0625
PULL = 0.375
CHUNKS = 4

F32 = jnp.float32
BF16 = jnp.bfloat16
HIGHEST = lax.Precision.HIGHEST
VMEM = pltpu.VMEM
SMEM = pltpu.SMEM


def spec(space):
    return pl.BlockSpec(memory_space=space)


def exchange(parts, axis):
    return lax.all_to_all(parts, axis, split_axis=0, concat_axis=0, tiled=True)


def from_behind(value, axis, distance):
    size = lax.axis_size(axis)
    return lax.ppermute(value, axis, [(i, (i + distance) % size) for i in range(size)])


def dot(left, right, dims):
    return lax.dot_general(
        left, right, (dims, ((), ())), precision=HIGHEST, preferred_element_type=F32
    )


def products_kernel(
    transposed, groups, rows_ref, cols_ref, info_ref, vec_ref, tiles_ref, out_ref, held, total, sems
):
    count = tiles_ref.shape[0]
    per_chunk = count // CHUNKS
    copies = [
        pltpu.make_async_copy(
            tiles_ref.at[pl.ds(c * per_chunk, per_chunk)],
            held.at[pl.ds(c * per_chunk, per_chunk)],
            sems.at[c],
        )
        for c in range(CHUNKS)
    ]
    for copy in copies:
        copy.start()
    live = info_ref[0]
    group = info_ref[1]
    total[...] = jnp.zeros_like(total)
    for c in range(CHUNKS):
        copies[c].wait()
        for k in range(c * per_chunk, (c + 1) * per_chunk):
            row = rows_ref[k]
            col = cols_ref[k]
            if transposed:
                source = lax.rem(group - row + groups, groups)
                target = col
            else:
                source = col
                target = lax.rem(row - group + groups, groups)
            product = lax.dot_general(
                vec_ref[source].astype(BF16),
                held[k],
                (((1,), (0,) if transposed else (1,)), ((), ())),
                preferred_element_type=F32,
            )
            total[target] += jnp.where(k < live, product, jnp.zeros_like(product))
    out_ref[...] = total[...].astype(out_ref.dtype)


def products(transposed, groups, rows, cols, info, vectors, tiles, targets, dtype):
    count, edge, _ = tiles.shape
    width = vectors.shape[1]
    return pl.pallas_call(
        functools.partial(products_kernel, transposed, groups),
        out_shape=jax.ShapeDtypeStruct((targets, width, edge), dtype),
        in_specs=[spec(SMEM), spec(SMEM), spec(SMEM), spec(VMEM), spec(pl.ANY)],
        out_specs=spec(VMEM),
        scratch_shapes=[
            pltpu.VMEM((count, edge, edge), BF16),
            pltpu.VMEM((targets, width, edge), F32),
            pltpu.SemaphoreType.DMA((CHUNKS,)),
        ],
        cost_estimate=pl.CostEstimate(
            flops=2 * count * width * edge * edge, bytes_accessed=2 * count * edge * edge, transcendentals=0
        ),
        name="products_back" if transposed else "products_ahead",
    )(rows, cols, info, vectors, tiles)


def combine_kernel(owners, back_ref, d0, d1, d2, d3, now_ref, before_ref, coef_ref, out_ref, sent_ref):
    image = back_ref[0].astype(F32)
    for r in range(1, owners):
        image = image + back_ref[r].astype(F32)
    image = image + ((d0[0] + d1[...]) + (d2[...] + d3[...]))
    new = 0.5 * image + coef_ref[...] * now_ref[...] - PULL * before_ref[...]
    out_ref[...] = new
    if sent_ref is not None:
        rounded = new.astype(BF16)
        for r in range(owners):
            sent_ref[r] = rounded


def combine(back, direct, now, before, coef, last):
    owners, width, edge = back.shape
    shapes = [jax.ShapeDtypeStruct((width, edge), F32)]
    if not last:
        shapes.append(jax.ShapeDtypeStruct((owners, width, edge), BF16))

    def kernel(*refs):
        combine_kernel(owners, *refs, *([None] if last else []))

    return pl.pallas_call(
        kernel,
        out_shape=shapes,
        in_specs=[spec(VMEM)] * 8,
        out_specs=[spec(VMEM)] * len(shapes),
        name="combine",
    )(back, *direct, now, before, coef)


def gram_kernel(*refs):
    out_ref = refs[-1]
    ins = refs[:-1]
    groups, width, _ = ins[0].shape
    out_ref[...] = jnp.zeros_like(out_ref)
    for i in range(len(ins)):
        for k in range(i + 1):
            value = dot(ins[i][0], ins[k][0], ((1,), (1,)))
            for s in range(1, groups):
                value = value + dot(ins[i][s], ins[k][s], ((1,), (1,)))
            out_ref[pl.ds(i * width, width), pl.ds(k * width, width)] = value


def factor(block):
    width = block.shape[0]
    row_id = lax.broadcasted_iota(jnp.int32, (width, 2 * width), 0)
    col_id = lax.broadcasted_iota(jnp.int32, (width, 2 * width), 1)
    work = jnp.concatenate([block, jnp.zeros_like(block)], 1) + jnp.where(
        col_id == row_id + width, 1.0, 0.0
    )
    result = jnp.zeros_like(work)
    for k in range(width):
        row = work[k : k + 1, :]
        scale = lax.rsqrt(row[:, k : k + 1])
        row = row * scale
        column = work[:, k : k + 1] * scale
        result = jnp.where(row_id == k, jnp.broadcast_to(row, work.shape), result)
        if k + 1 < width:
            work = work - jnp.where(row_id > k, column, 0.0) * row
    return result[:, :width], result[:, width:]


def finish_kernel(groups, info_ref, gram_ref, *refs):
    basis = refs[: ITERS + 1]
    proj_ref, fact_ref, out_ref, low, inv = refs[ITERS + 1 :]
    width = basis[0].shape[1]
    edge = basis[0].shape[2]
    group = info_ref[1]
    low[...] = jnp.zeros_like(low)
    inv[...] = jnp.zeros_like(inv)
    proj_ref[...] = jnp.zeros_like(proj_ref)
    for j in range(ITERS + 1):
        here = pl.ds(j * width, width)
        done = pl.ds(0, j * width)
        schur = gram_ref[here, here]
        if j > 0:
            left = dot(gram_ref[here, done], inv[done, done], ((1,), (1,)))
            schur = schur - dot(left, left, ((1,), (1,)))
        upper, own_inverse = factor(schur)
        low[here, here] = upper.T
        inv[here, here] = own_inverse
        if j > 0:
            low[here, done] = left
            inv[here, done] = -dot(own_inverse, dot(left, inv[done, done], ((1,), (0,))), ((1,), (0,)))
    used = ITERS * width
    for j in range(ITERS):
        here = pl.ds(j * width, width)
        value = low[pl.ds(width, (j + 1) * width), :] - SHIFT * low[pl.ds(0, (j + 1) * width), :]
        if j > 0:
            value = value + PULL * jnp.concatenate(
                [jnp.zeros((width, value.shape[1]), F32), low[pl.ds(0, j * width), :]], 0
            )
        image = dot(inv[here, pl.ds(0, (j + 1) * width)], value, ((1,), (0,)))
        lane = lax.broadcasted_iota(jnp.int32, (width, used), 1)
        proj_ref[j] = jnp.where(lane < (j + 1) * width, image[:, :used], 0.0)
        corner = image[:, (j + 1) * width : (j + 2) * width]
        fact_ref[j] = jnp.where(
            lax.broadcasted_iota(jnp.int32, (width, width), 0)
            >= lax.broadcasted_iota(jnp.int32, (width, width), 1),
            corner,
            0.0,
        )
    for s in range(groups):
        value = dot(inv[pl.ds(used, width), pl.ds(0, width)], basis[0][s], ((1,), (0,)))
        for i in range(1, ITERS + 1):
            value = value + dot(inv[pl.ds(used, width), pl.ds(i * width, width)], basis[i][s], ((1,), (0,)))
        out_ref[lax.rem(group - s + groups, groups)] = value


def per_device(tiles, tile_rows, tile_cols, live_tiles, dual_shift, start_block):
    matrix = tiles[0, 0]
    rows_here = tile_rows[0, 0]
    cols_here = tile_cols[0, 0]
    tile_count, edge, _ = matrix.shape
    width, row_count = start_block.shape
    groups = lax.axis_size("grp")
    owners = lax.axis_size("row")
    group = lax.axis_index("grp")
    info = jnp.stack([live_tiles[0, 0], group]).astype(jnp.int32)

    blocks = jnp.moveaxis(start_block.reshape(width, groups, edge), 1, 0)
    slots = lax.rem(group - jnp.arange(groups) + groups, groups)
    full = jnp.take(blocks, slots, axis=0)
    coef = SHIFT - lax.dynamic_index_in_dim(dual_shift.reshape(groups, edge), group, 0, True)
    own = full[0]
    before = jnp.zeros_like(own)
    sent = jnp.broadcast_to(own.astype(BF16)[None], (owners, width, edge))
    basis = [full]
    for step in range(ITERS):
        columns = exchange(sent, "row")
        if step > 0:
            full = jnp.stack([own] + [from_behind(own, "grp", k) for k in range(1, groups)])
            basis.append(full)
        back = products(True, groups, rows_here, cols_here, info, full, matrix, owners, BF16)
        back = exchange(back, "row")
        direct = products(False, groups, rows_here, cols_here, info, columns, matrix, groups, F32)
        direct = [direct] + [from_behind(direct[k], "grp", k) for k in range(1, groups)]
        last = step == ITERS - 1
        new = combine(back, direct, own, before, coef, last)
        before, own = own, new[0]
        sent = None if last else new[1]
    full = jnp.stack([own] + [from_behind(own, "grp", k) for k in range(1, groups)])
    basis.append(full)

    total = (ITERS + 1) * width
    partial = pl.pallas_call(
        gram_kernel,
        out_shape=jax.ShapeDtypeStruct((total, total), F32),
        in_specs=[spec(VMEM)] * (ITERS + 1),
        out_specs=spec(VMEM),
        name="gram",
    )(*basis)
    part = exchange(partial.reshape(owners, total // owners, total), "row").sum(0)
    gram = exchange(jnp.broadcast_to(part[None], (owners, *part.shape)), "row").reshape(total, total)
    projections, factors, last_block = pl.pallas_call(
        functools.partial(finish_kernel, groups),
        out_shape=[
            jax.ShapeDtypeStruct((ITERS, width, ITERS * width), F32),
            jax.ShapeDtypeStruct((ITERS, width, width), F32),
            jax.ShapeDtypeStruct((groups, width, edge), F32),
        ],
        in_specs=[spec(SMEM)] + [spec(VMEM)] * (ITERS + 2),
        out_specs=[spec(VMEM)] * 3,
        scratch_shapes=[pltpu.VMEM((total, total), F32), pltpu.VMEM((total, total), F32)],
        name="finish",
    )(info, gram, *basis)
    return (projections, factors, jnp.moveaxis(last_block, 0, 1).reshape(width, row_count))


def solution(mesh):
    in_specs = (
        P("grp", "row", None, None, None),
        P("grp", "row", None),
        P("grp", "row", None),
        P("grp", "row"),
        P("row"),
        P(None, "row"),
    )
    out_specs = (P(), P(), P(None, "row"))
    return jax.shard_map(
        per_device, mesh=mesh, in_specs=in_specs, out_specs=out_specs, check_vma=False
    )
```

```python
import functools

import jax
import jax.numpy as jnp
from jax import lax
from jax.experimental import pallas as pl
from jax.experimental.pallas import tpu as pltpu
from jax.sharding import PartitionSpec as P


ITERS = 4
SHIFT = 1.0625
PULL = 0.375
CHUNKS = 4
LANES = 128
EXTRA = 8

F32 = jnp.float32
BF16 = jnp.bfloat16
HIGHEST = lax.Precision.HIGHEST
VMEM = pltpu.VMEM
SMEM = pltpu.SMEM


def spec(space):
    return pl.BlockSpec(memory_space=space)


def call(kernel, out_shape, in_spaces, operands, limit_mib, scratch=(), flops=2_000_000):
    return pl.pallas_call(
        kernel,
        out_shape=out_shape,
        in_specs=[spec(space) for space in in_spaces],
        out_specs=[spec(VMEM)] * len(out_shape),
        scratch_shapes=list(scratch),
        compiler_params=pltpu.CompilerParams(vmem_limit_bytes=limit_mib << 20),
        cost_estimate=pl.CostEstimate(flops=flops, bytes_accessed=1 << 20, transcendentals=0),
    )(*operands)


def shape(*dims, dtype=F32):
    return jax.ShapeDtypeStruct(dims, dtype)


def exchange(parts, axis):
    return lax.all_to_all(parts, axis, split_axis=0, concat_axis=0, tiled=True)


def from_behind(value, axis, distance):
    size = lax.axis_size(axis)
    return lax.ppermute(value, axis, [(i, (i + distance) % size) for i in range(size)])


def dot(left, right, dims):
    return lax.dot_general(
        left, right, (dims, ((), ())), precision=HIGHEST, preferred_element_type=F32
    )


def plain(left, right):
    return dot(left, right, ((1,), (0,)))


def across(left, right):
    return dot(left, right, ((1,), (1,)))


def pieces(value):
    high = value.astype(BF16).astype(F32)
    rest = value - high
    middle = rest.astype(BF16).astype(F32)
    return high, middle, rest - middle


def stacked(high, middle, low):
    line = lax.broadcasted_iota(jnp.int32, (EXTRA, high.shape[1]), 0)
    value = jnp.where(line == 2, low, 0.0)
    value = jnp.where(line == 1, middle, value)
    return jnp.where(line == 0, high, value)


def init_kernel(groups, owners, start_ref, shift_ref, *outs):
    slots, sent_ref, coef_ref = outs[:groups], outs[groups], outs[groups + 1]
    edge = coef_ref.shape[1]
    group = lax.axis_index("grp")
    for s in range(groups):
        block = lax.rem(group - s + groups, groups)
        slots[s][...] = start_ref[:, pl.ds(pl.multiple_of(block * edge, edge), edge)]
    rounded = slots[0][...].astype(BF16)
    for r in range(owners):
        sent_ref[r] = rounded
    coef_ref[...] = SHIFT - shift_ref[:, pl.ds(pl.multiple_of(group * edge, edge), edge)]


def fetches(tiles_ref, held, sems):
    per_chunk = held.shape[0] // CHUNKS
    return [
        pltpu.make_async_copy(
            tiles_ref.at[0, 0, pl.ds(c * per_chunk, per_chunk)],
            held.at[pl.ds(c * per_chunk, per_chunk)],
            sems.at[c],
        )
        for c in range(CHUNKS)
    ]


def back_kernel(groups, steps, rows_ref, cols_ref, live_ref, tiles_ref, *refs):
    count = steps + 1
    vectors = [refs[i * groups : (i + 1) * groups] for i in range(count)]
    out_ref, held, total, rounded, sems = refs[count * groups :]
    copies = fetches(tiles_ref, held, sems)
    for copy in copies:
        copy.start()
    owners, width, edge = total.shape
    group = lax.axis_index("grp")
    live = live_ref[0, 0]
    for s in range(groups):
        rounded[s] = vectors[steps][s][...].astype(BF16)
    total[...] = jnp.zeros_like(total)
    grams = []
    for i in range(count):
        value = across(vectors[steps][0][...], vectors[i][0][...])
        for s in range(1, groups):
            value = value + across(vectors[steps][s][...], vectors[i][s][...])
        grams.append(value)
    if count * width < LANES:
        grams.append(jnp.zeros((width, LANES - count * width), F32))
    high, middle, low = pieces(jnp.concatenate(grams, 1))
    for r in range(owners):
        value = stacked(high[r : r + 1], middle[r : r + 1], low[r : r + 1])
        value = jnp.concatenate([value, jnp.zeros((EXTRA, edge - LANES), F32)], 1)
        out_ref[r, pl.ds(width, EXTRA), :] = value.astype(BF16)
    per_chunk = held.shape[0] // CHUNKS
    for c in range(CHUNKS):
        copies[c].wait()
        for k in range(c * per_chunk, (c + 1) * per_chunk):
            source = lax.rem(group - rows_ref[0, 0, k] + groups, groups)
            product = lax.dot_general(
                rounded[source], held[k], (((1,), (0,)), ((), ())), preferred_element_type=F32
            )
            total[cols_ref[0, 0, k]] += jnp.where(k < live, product, jnp.zeros_like(product))
    for r in range(owners):
        out_ref[r, pl.ds(0, width), :] = total[r].astype(BF16)


def ahead_kernel(groups, rows_ref, cols_ref, live_ref, tiles_ref, columns_ref, *refs):
    outs = refs[:groups]
    held, total, sems = refs[groups:]
    copies = fetches(tiles_ref, held, sems)
    for copy in copies:
        copy.start()
    width = total.shape[1]
    group = lax.axis_index("grp")
    live = live_ref[0, 0]
    total[...] = jnp.zeros_like(total)
    per_chunk = held.shape[0] // CHUNKS
    for c in range(CHUNKS):
        copies[c].wait()
        for k in range(c * per_chunk, (c + 1) * per_chunk):
            target = lax.rem(rows_ref[0, 0, k] - group + groups, groups)
            product = lax.dot_general(
                columns_ref[cols_ref[0, 0, k], pl.ds(0, width), :],
                held[k],
                (((1,), (1,)), ((), ())),
                preferred_element_type=F32,
            )
            total[target] += jnp.where(k < live, product, jnp.zeros_like(product))
    for s in range(groups):
        outs[s][...] = total[s]


def combine_kernel(groups, last, back_ref, *refs):
    direct = refs[:groups]
    now_ref, before_ref, coef_ref = refs[groups : groups + 3]
    outs = refs[groups + 3 :]
    owners = back_ref.shape[0]
    width = now_ref.shape[0]
    edge = now_ref.shape[1]
    image = direct[0][...]
    for s in range(1, groups):
        image = image + direct[s][...]
    for r in range(owners):
        image = image + back_ref[r, pl.ds(0, width), :].astype(F32)
    new = 0.5 * image + coef_ref[...] * now_ref[...] - PULL * before_ref[...]
    outs[0][...] = new
    sums = back_ref[0, pl.ds(width, EXTRA), pl.ds(0, LANES)].astype(F32)
    for r in range(1, owners):
        sums = sums + back_ref[r, pl.ds(width, EXTRA), pl.ds(0, LANES)].astype(F32)
    row = sums[0:1] + (sums[1:2] + sums[2:3])
    if last:
        outs[1][...] = jnp.broadcast_to(row, (EXTRA, LANES))
    else:
        rounded = new.astype(BF16)
        extra = stacked(*pieces(row))
        extra = jnp.concatenate([extra, jnp.zeros((EXTRA, edge - LANES), F32)], 1).astype(BF16)
        for r in range(owners):
            outs[1][r, pl.ds(0, width), :] = rounded
            outs[1][r, pl.ds(width, EXTRA), :] = extra


def factor(block):
    width = block.shape[0]
    row_id = lax.broadcasted_iota(jnp.int32, (width, 2 * width), 0)
    col_id = lax.broadcasted_iota(jnp.int32, (width, 2 * width), 1)
    work = jnp.concatenate([block, jnp.zeros_like(block)], 1) + jnp.where(
        col_id == row_id + width, 1.0, 0.0
    )
    result = jnp.zeros_like(work)
    for k in range(width):
        row = work[k : k + 1, :]
        scale = lax.rsqrt(row[:, k : k + 1])
        row = row * scale
        column = work[:, k : k + 1] * scale
        result = jnp.where(row_id == k, jnp.broadcast_to(row, work.shape), result)
        if k + 1 < width:
            work = work - jnp.where(row_id > k, column, 0.0) * row
    return result[:, :width], result[:, width:]


def next_rows(j, gram_row, low, inv):
    width = gram_row.shape[0]
    here, done = pl.ds(j * width, width), pl.ds(0, j * width)
    low[here, :] = jnp.zeros((width, low.shape[1]), F32)
    inv[here, :] = jnp.zeros((width, inv.shape[1]), F32)
    schur = gram_row[:, j * width : (j + 1) * width]
    if j > 0:
        left = across(gram_row[:, : j * width], inv[done, done])
        schur = schur - across(left, left)
        back = plain(left, inv[done, done])
    upper, own_inverse = factor(schur)
    low[here, here] = upper.T
    inv[here, here] = own_inverse
    if j > 0:
        low[here, done] = left
        inv[here, done] = -plain(own_inverse, back)


def step_results(j, low, inv, width):
    used = (j + 1) * width
    value = low[pl.ds(width, used), :] - SHIFT * low[pl.ds(0, used), :]
    if j > 0:
        value = value + PULL * jnp.concatenate(
            [jnp.zeros((width, value.shape[1]), F32), low[pl.ds(0, j * width), :]], 0
        )
    image = plain(inv[pl.ds(j * width, width), pl.ds(0, used)], value)
    lane = lax.broadcasted_iota(jnp.int32, (width, ITERS * width), 1)
    square = (width, width)
    keep = lax.broadcasted_iota(jnp.int32, square, 0) >= lax.broadcasted_iota(jnp.int32, square, 1)
    return (
        jnp.where(lane < used, image[:, : ITERS * width], 0.0),
        jnp.where(keep, image[:, used : used + width], 0.0),
    )


def block_kernel(j, columns_ref, *refs):
    olds, (low_ref, inv_ref) = refs[:-2], refs[-2:]
    owners = columns_ref.shape[0]
    width = low_ref.shape[0] // (ITERS + 1)
    if j > 0:
        low_ref[...] = olds[0][...]
        inv_ref[...] = olds[1][...]
    rows = []
    for r in range(owners):
        three = columns_ref[r, pl.ds(width, EXTRA), pl.ds(0, LANES)].astype(F32)
        rows.append(three[0:1] + (three[1:2] + three[2:3]))
    next_rows(j, jnp.concatenate(rows, 0), low_ref, inv_ref)


def gram_kernel(groups, chunk_ref, *refs):
    out_ref = refs[-1]
    vectors = [refs[i * groups : (i + 1) * groups] for i in range(ITERS + 1)]
    owners = out_ref.shape[0]
    width = vectors[0][0].shape[0]
    grams = []
    for i in range(ITERS + 1):
        value = across(vectors[ITERS][0][...], vectors[i][0][...])
        for s in range(1, groups):
            value = value + across(vectors[ITERS][s][...], vectors[i][s][...])
        grams.append(value)
    parts = LANES // width
    rows = width // parts
    packed = jnp.concatenate([grams[ITERS][p * rows : (p + 1) * rows] for p in range(parts)], 1)
    value = jnp.concatenate(
        [jnp.concatenate(grams[:ITERS], 1), packed, jnp.broadcast_to(chunk_ref[0:1], (EXTRA, LANES))], 0
    )
    for r in range(owners):
        out_ref[r] = value


def finish_kernel(groups, parts_ref, old_low, old_inv, *refs):
    vectors = [refs[i * groups : (i + 1) * groups] for i in range(ITERS + 1)]
    proj_ref, fact_ref, out_ref, low, inv = refs[(ITERS + 1) * groups :]
    owners = parts_ref.shape[0]
    width, edge = vectors[0][0].shape
    group = lax.axis_index("grp")
    low[...] = old_low[...]
    inv[...] = old_inv[...]
    last = parts_ref.shape[1] - EXTRA
    rows = [parts_ref[r, pl.ds(last, EXTRA), :][0:1] for r in range(owners)]
    next_rows(ITERS - 1, jnp.concatenate(rows, 0), low, inv)
    sums = parts_ref[0, pl.ds(0, last), :]
    for r in range(1, owners):
        sums = sums + parts_ref[r, pl.ds(0, last), :]
    count = LANES // width
    corner = jnp.concatenate([sums[width:, p * width : (p + 1) * width] for p in range(count)], 0)
    next_rows(ITERS, jnp.concatenate([sums[:width], corner], 1), low, inv)
    for j in range(ITERS):
        proj_ref[j], fact_ref[j] = step_results(j, low, inv, width)
    for s in range(groups):
        value = plain(inv[pl.ds(ITERS * width, width), pl.ds(0, width)], vectors[0][s][...])
        for i in range(1, ITERS + 1):
            value = value + plain(
                inv[pl.ds(ITERS * width, width), pl.ds(i * width, width)], vectors[i][s][...]
            )
        block = lax.rem(group - s + groups, groups)
        out_ref[:, pl.ds(pl.multiple_of(block * edge, edge), edge)] = value


def per_device(tiles, tile_rows, tile_cols, live_tiles, dual_shift, start_block):
    count, edge = tiles.shape[2], tiles.shape[3]
    width, row_count = start_block.shape
    groups = lax.axis_size("grp")
    owners = lax.axis_size("row")
    total = (ITERS + 1) * width
    tables = (tile_rows, tile_cols, live_tiles, tiles)
    spaces = [SMEM, SMEM, SMEM, pl.ANY]
    held = pltpu.VMEM((count, edge, edge), BF16)
    flops = 2 * count * width * edge * edge

    *slots, sent, coef = call(
        functools.partial(init_kernel, groups, owners),
        [shape(width, edge)] * groups + [shape(owners, width, edge, dtype=BF16), shape(1, edge)],
        [VMEM, VMEM],
        (start_block, dual_shift[None, :]),
        4,
    )
    before = jnp.zeros((width, edge), F32)
    basis = [slots]
    state = ()
    for step in range(ITERS):
        own = basis[step][0]
        columns = exchange(sent, "row")
        flat = [slot for slots in basis for slot in slots]
        (parts,) = call(
            functools.partial(back_kernel, groups, step),
            [shape(owners, width + EXTRA, edge, dtype=BF16)],
            spaces + [VMEM] * len(flat),
            (*tables, *flat),
            12,
            [
                held,
                pltpu.VMEM((owners, width, edge), F32),
                pltpu.VMEM((groups, width, edge), BF16),
                pltpu.SemaphoreType.DMA((CHUNKS,)),
            ],
            flops,
        )
        arrived = exchange(parts, "row")
        direct = call(
            functools.partial(ahead_kernel, groups),
            [shape(width, edge)] * groups,
            spaces + [VMEM],
            (*tables, columns),
            12,
            [held, pltpu.VMEM((groups, width, edge), F32), pltpu.SemaphoreType.DMA((CHUNKS,))],
            flops,
        )
        direct = [direct[0]] + [from_behind(direct[k], "grp", k) for k in range(1, groups)]
        if step > 0:
            state = call(
                functools.partial(block_kernel, step - 1),
                [shape(total, total)] * 2,
                [VMEM] * (1 + len(state)),
                (columns, *state),
                4,
            )
        last = step == ITERS - 1
        second = shape(EXTRA, LANES) if last else shape(owners, width + EXTRA, edge, dtype=BF16)
        new, sent = call(
            functools.partial(combine_kernel, groups, last),
            [shape(width, edge), second],
            [VMEM] * (groups + 4),
            (arrived, *direct, own, before, coef),
            4,
        )
        before = own
        basis.append([new] + [from_behind(new, "grp", k) for k in range(1, groups)])

    flat = [slot for slots in basis for slot in slots]
    (parts,) = call(
        functools.partial(gram_kernel, groups),
        [shape(owners, width + width * width // LANES + EXTRA, LANES)],
        [VMEM] * (1 + len(flat)),
        (sent, *flat),
        6,
    )
    parts = exchange(parts, "row")
    return call(
        functools.partial(finish_kernel, groups),
        [shape(ITERS, width, ITERS * width), shape(ITERS, width, width), shape(width, row_count)],
        [VMEM] * (3 + len(flat)),
        (parts, *state, *flat),
        8,
        [pltpu.VMEM((total, total), F32), pltpu.VMEM((total, total), F32)],
    )


def solution(mesh):
    in_specs = (
        P("grp", "row", None, None, None),
        P("grp", "row", None),
        P("grp", "row", None),
        P("grp", "row"),
        P("row"),
        P(None, "row"),
    )
    out_specs = (P(), P(), P(None, "row"))
    return jax.shard_map(
        per_device, mesh=mesh, in_specs=in_specs, out_specs=out_specs, check_vma=False
    )
```

```python
import functools

import jax
import jax.numpy as jnp
from jax import lax
from jax.experimental import pallas as pl
from jax.experimental.pallas import tpu as pltpu
from jax.sharding import PartitionSpec as P


ITERS = 4
SHIFT = 1.0625
PULL = 0.375
CHUNKS = 4
LANES = 128
EXTRA = 8

F32 = jnp.float32
BF16 = jnp.bfloat16
HIGHEST = lax.Precision.HIGHEST
VMEM = pltpu.VMEM
SMEM = pltpu.SMEM


def spec(space):
    return pl.BlockSpec(memory_space=space)


def call(kernel, out_shape, in_spaces, operands, limit_mib, scratch=(), flops=2_000_000):
    return pl.pallas_call(
        kernel,
        out_shape=out_shape,
        in_specs=[spec(space) for space in in_spaces],
        out_specs=[spec(VMEM)] * len(out_shape),
        scratch_shapes=list(scratch),
        compiler_params=pltpu.CompilerParams(vmem_limit_bytes=limit_mib << 20),
        cost_estimate=pl.CostEstimate(flops=flops, bytes_accessed=1 << 20, transcendentals=0),
    )(*operands)


def shape(*dims, dtype=F32):
    return jax.ShapeDtypeStruct(dims, dtype)


def exchange(parts, axis):
    return lax.all_to_all(parts, axis, split_axis=0, concat_axis=0, tiled=True)


def from_behind(value, axis, distance):
    size = lax.axis_size(axis)
    return lax.ppermute(value, axis, [(i, (i + distance) % size) for i in range(size)])


def dot(left, right, dims):
    return lax.dot_general(
        left, right, (dims, ((), ())), precision=HIGHEST, preferred_element_type=F32
    )


def plain(left, right):
    return dot(left, right, ((1,), (0,)))


def across(left, right):
    return dot(left, right, ((1,), (1,)))


def halves(value):
    return jnp.concatenate([value[:, :LANES], value[:, LANES:]], 0)


def whole(ref, r, width):
    return jnp.concatenate([ref[r, pl.ds(0, width), :], ref[r, pl.ds(width, width), :]], 1)


def pieces(value):
    high = value.astype(BF16).astype(F32)
    rest = value - high
    middle = rest.astype(BF16).astype(F32)
    return high, middle, rest - middle


def stacked(high, middle, low):
    line = lax.broadcasted_iota(jnp.int32, (EXTRA, high.shape[1]), 0)
    value = jnp.where(line == 2, low, 0.0)
    value = jnp.where(line == 1, middle, value)
    return jnp.where(line == 0, high, value)


def init_kernel(groups, owners, start_ref, shift_ref, *outs):
    slots, sent_ref, coef_ref = outs[:groups], outs[groups], outs[groups + 1]
    edge = coef_ref.shape[1]
    group = lax.axis_index("grp")
    for s in range(groups):
        block = lax.rem(group - s + groups, groups)
        slots[s][...] = start_ref[:, pl.ds(pl.multiple_of(block * edge, edge), edge)]
    rounded = halves(slots[0][...]).astype(BF16)
    for r in range(owners):
        sent_ref[r] = rounded
    coef_ref[...] = SHIFT - shift_ref[:, pl.ds(pl.multiple_of(group * edge, edge), edge)]


def fetches(tiles_ref, held, sems):
    per_chunk = held.shape[0] // CHUNKS
    return [
        pltpu.make_async_copy(
            tiles_ref.at[0, 0, pl.ds(c * per_chunk, per_chunk)],
            held.at[pl.ds(c * per_chunk, per_chunk)],
            sems.at[c],
        )
        for c in range(CHUNKS)
    ]


def back_kernel(groups, steps, rows_ref, cols_ref, live_ref, tiles_ref, *refs):
    count = steps + 1
    vectors = [refs[i * groups : (i + 1) * groups] for i in range(count)]
    out_ref, held, total, rounded, sems = refs[count * groups :]
    copies = fetches(tiles_ref, held, sems)
    for copy in copies:
        copy.start()
    owners, width, _ = total.shape
    group = lax.axis_index("grp")
    live = live_ref[0, 0]
    for s in range(groups):
        rounded[s] = vectors[steps][s][...].astype(BF16)
    total[...] = jnp.zeros_like(total)
    grams = []
    for i in range(count):
        value = across(vectors[steps][0][...], vectors[i][0][...])
        for s in range(1, groups):
            value = value + across(vectors[steps][s][...], vectors[i][s][...])
        grams.append(value)
    if count * width < LANES:
        grams.append(jnp.zeros((width, LANES - count * width), F32))
    high, middle, low = pieces(jnp.concatenate(grams, 1))
    for r in range(owners):
        value = stacked(high[r : r + 1], middle[r : r + 1], low[r : r + 1])
        out_ref[r, pl.ds(2 * width, EXTRA), :] = value.astype(BF16)
    per_chunk = held.shape[0] // CHUNKS
    for c in range(CHUNKS):
        copies[c].wait()
        for k in range(c * per_chunk, (c + 1) * per_chunk):
            source = lax.rem(group - rows_ref[0, 0, k] + groups, groups)
            product = lax.dot_general(
                rounded[source], held[k], (((1,), (0,)), ((), ())), preferred_element_type=F32
            )
            total[cols_ref[0, 0, k]] += jnp.where(k < live, product, jnp.zeros_like(product))
    for r in range(owners):
        out_ref[r, pl.ds(0, 2 * width), :] = halves(total[r]).astype(BF16)


def ahead_kernel(groups, rows_ref, cols_ref, live_ref, tiles_ref, columns_ref, *refs):
    outs = refs[:groups]
    held, total, sems = refs[groups:]
    copies = fetches(tiles_ref, held, sems)
    for copy in copies:
        copy.start()
    width = total.shape[1]
    group = lax.axis_index("grp")
    live = live_ref[0, 0]
    total[...] = jnp.zeros_like(total)
    per_chunk = held.shape[0] // CHUNKS
    for c in range(CHUNKS):
        copies[c].wait()
        for k in range(c * per_chunk, (c + 1) * per_chunk):
            target = lax.rem(rows_ref[0, 0, k] - group + groups, groups)
            product = lax.dot_general(
                whole(columns_ref, cols_ref[0, 0, k], width),
                held[k],
                (((1,), (1,)), ((), ())),
                preferred_element_type=F32,
            )
            total[target] += jnp.where(k < live, product, jnp.zeros_like(product))
    for s in range(groups):
        outs[s][...] = total[s].astype(outs[s].dtype)


def combine_kernel(groups, last, back_ref, *refs):
    direct = refs[:groups]
    now_ref, before_ref, coef_ref = refs[groups : groups + 3]
    outs = refs[groups + 3 :]
    owners = back_ref.shape[0]
    width = now_ref.shape[0]
    image = direct[0][...]
    for s in range(1, groups):
        image = image + direct[s][...].astype(F32)
    for r in range(owners):
        image = image + whole(back_ref, r, width).astype(F32)
    new = 0.5 * image + coef_ref[...] * now_ref[...] - PULL * before_ref[...]
    outs[0][...] = new
    sums = back_ref[0, pl.ds(2 * width, EXTRA), :].astype(F32)
    for r in range(1, owners):
        sums = sums + back_ref[r, pl.ds(2 * width, EXTRA), :].astype(F32)
    row = sums[0:1] + (sums[1:2] + sums[2:3])
    if last:
        outs[1][...] = jnp.broadcast_to(row, (EXTRA, LANES))
    else:
        rounded = halves(new).astype(BF16)
        extra = stacked(*pieces(row)).astype(BF16)
        for r in range(owners):
            outs[1][r, pl.ds(0, 2 * width), :] = rounded
            outs[1][r, pl.ds(2 * width, EXTRA), :] = extra


def factor(block):
    width = block.shape[0]
    row_id = lax.broadcasted_iota(jnp.int32, (width, 2 * width), 0)
    col_id = lax.broadcasted_iota(jnp.int32, (width, 2 * width), 1)
    work = jnp.concatenate([block, jnp.zeros_like(block)], 1) + jnp.where(
        col_id == row_id + width, 1.0, 0.0
    )
    result = jnp.zeros_like(work)
    for k in range(width):
        row = work[k : k + 1, :]
        scale = lax.rsqrt(row[:, k : k + 1])
        row = row * scale
        column = work[:, k : k + 1] * scale
        result = jnp.where(row_id == k, jnp.broadcast_to(row, work.shape), result)
        if k + 1 < width:
            work = work - jnp.where(row_id > k, column, 0.0) * row
    return result[:, :width], result[:, width:]


def next_rows(j, gram_row, low, inv):
    width = gram_row.shape[0]
    here, done = pl.ds(j * width, width), pl.ds(0, j * width)
    low[here, :] = jnp.zeros((width, low.shape[1]), F32)
    inv[here, :] = jnp.zeros((width, inv.shape[1]), F32)
    schur = gram_row[:, j * width : (j + 1) * width]
    if j > 0:
        left = across(gram_row[:, : j * width], inv[done, done])
        schur = schur - across(left, left)
        back = plain(left, inv[done, done])
    upper, own_inverse = factor(schur)
    low[here, here] = upper.T
    inv[here, here] = own_inverse
    if j > 0:
        low[here, done] = left
        inv[here, done] = -plain(own_inverse, back)


def step_results(j, low, inv, width):
    used = (j + 1) * width
    value = low[pl.ds(width, used), :] - SHIFT * low[pl.ds(0, used), :]
    if j > 0:
        value = value + PULL * jnp.concatenate(
            [jnp.zeros((width, value.shape[1]), F32), low[pl.ds(0, j * width), :]], 0
        )
    image = plain(inv[pl.ds(j * width, width), pl.ds(0, used)], value)
    lane = lax.broadcasted_iota(jnp.int32, (width, ITERS * width), 1)
    square = (width, width)
    keep = lax.broadcasted_iota(jnp.int32, square, 0) >= lax.broadcasted_iota(jnp.int32, square, 1)
    return (
        jnp.where(lane < used, image[:, : ITERS * width], 0.0),
        jnp.where(keep, image[:, used : used + width], 0.0),
    )


def block_kernel(j, columns_ref, *refs):
    olds, (low_ref, inv_ref) = refs[:-2], refs[-2:]
    owners = columns_ref.shape[0]
    width = low_ref.shape[0] // (ITERS + 1)
    if j > 0:
        low_ref[...] = olds[0][...]
        inv_ref[...] = olds[1][...]
    rows = []
    for r in range(owners):
        three = columns_ref[r, pl.ds(2 * width, EXTRA), :].astype(F32)
        rows.append(three[0:1] + (three[1:2] + three[2:3]))
    next_rows(j, jnp.concatenate(rows, 0), low_ref, inv_ref)


def gram_kernel(groups, chunk_ref, *refs):
    out_ref = refs[-1]
    vectors = [refs[i * groups : (i + 1) * groups] for i in range(ITERS + 1)]
    owners = out_ref.shape[0]
    width = vectors[0][0].shape[0]
    grams = []
    for i in range(ITERS + 1):
        value = across(vectors[ITERS][0][...], vectors[i][0][...])
        for s in range(1, groups):
            value = value + across(vectors[ITERS][s][...], vectors[i][s][...])
        grams.append(value)
    parts = LANES // width
    rows = width // parts
    packed = jnp.concatenate([grams[ITERS][p * rows : (p + 1) * rows] for p in range(parts)], 1)
    value = jnp.concatenate(
        [jnp.concatenate(grams[:ITERS], 1), packed, jnp.broadcast_to(chunk_ref[0:1], (EXTRA, LANES))], 0
    )
    for r in range(owners):
        out_ref[r] = value


def finish_kernel(groups, parts_ref, old_low, old_inv, *refs):
    vectors = [refs[i * groups : (i + 1) * groups] for i in range(ITERS + 1)]
    proj_ref, fact_ref, out_ref, low, inv = refs[(ITERS + 1) * groups :]
    owners = parts_ref.shape[0]
    width, edge = vectors[0][0].shape
    group = lax.axis_index("grp")
    low[...] = old_low[...]
    inv[...] = old_inv[...]
    last = parts_ref.shape[1] - EXTRA
    rows = [parts_ref[r, pl.ds(last, EXTRA), :][0:1] for r in range(owners)]
    next_rows(ITERS - 1, jnp.concatenate(rows, 0), low, inv)
    sums = parts_ref[0, pl.ds(0, last), :]
    for r in range(1, owners):
        sums = sums + parts_ref[r, pl.ds(0, last), :]
    count = LANES // width
    corner = jnp.concatenate([sums[width:, p * width : (p + 1) * width] for p in range(count)], 0)
    next_rows(ITERS, jnp.concatenate([sums[:width], corner], 1), low, inv)
    for j in range(ITERS):
        proj_ref[j], fact_ref[j] = step_results(j, low, inv, width)
    for s in range(groups):
        value = plain(inv[pl.ds(ITERS * width, width), pl.ds(0, width)], vectors[0][s][...])
        for i in range(1, ITERS + 1):
            value = value + plain(
                inv[pl.ds(ITERS * width, width), pl.ds(i * width, width)], vectors[i][s][...]
            )
        block = lax.rem(group - s + groups, groups)
        out_ref[:, pl.ds(pl.multiple_of(block * edge, edge), edge)] = value


def per_device(tiles, tile_rows, tile_cols, live_tiles, dual_shift, start_block):
    count, edge = tiles.shape[2], tiles.shape[3]
    width, row_count = start_block.shape
    groups = lax.axis_size("grp")
    owners = lax.axis_size("row")
    total = (ITERS + 1) * width
    tables = (tile_rows, tile_cols, live_tiles, tiles)
    spaces = [SMEM, SMEM, SMEM, pltpu.HBM]
    held = pltpu.VMEM((count, edge, edge), BF16)
    flops = 2 * count * width * edge * edge

    *slots, sent, coef = call(
        functools.partial(init_kernel, groups, owners),
        [shape(width, edge)] * groups + [shape(owners, 2 * width, LANES, dtype=BF16), shape(1, edge)],
        [VMEM, VMEM],
        (start_block, dual_shift[None, :]),
        4,
    )
    before = jnp.zeros((width, edge), F32)
    basis = [slots]
    state = ()
    for step in range(ITERS):
        own = basis[step][0]
        columns = exchange(sent, "row")
        flat = [slot for slots in basis for slot in slots]
        (parts,) = call(
            functools.partial(back_kernel, groups, step),
            [shape(owners, 2 * width + EXTRA, LANES, dtype=BF16)],
            spaces + [VMEM] * len(flat),
            (*tables, *flat),
            50,
            [
                held,
                pltpu.VMEM((owners, width, edge), F32),
                pltpu.VMEM((groups, width, edge), BF16),
                pltpu.SemaphoreType.DMA((CHUNKS,)),
            ],
            flops,
        )
        arrived = exchange(parts, "row")
        direct = call(
            functools.partial(ahead_kernel, groups),
            [shape(width, edge)] + [shape(width, edge, dtype=BF16)] * (groups - 1),
            spaces + [VMEM],
            (*tables, columns),
            50,
            [held, pltpu.VMEM((groups, width, edge), F32), pltpu.SemaphoreType.DMA((CHUNKS,))],
            flops,
        )
        direct = [direct[0]] + [from_behind(direct[k], "grp", k) for k in range(1, groups)]
        if step > 0:
            state = call(
                functools.partial(block_kernel, step - 1),
                [shape(total, total)] * 2,
                [VMEM] * (1 + len(state)),
                (columns, *state),
                4,
            )
        last = step == ITERS - 1
        second = shape(EXTRA, LANES) if last else shape(owners, 2 * width + EXTRA, LANES, dtype=BF16)
        new, sent = call(
            functools.partial(combine_kernel, groups, last),
            [shape(width, edge), second],
            [VMEM] * (groups + 4),
            (arrived, *direct, own, before, coef),
            4,
        )
        before = own
        basis.append([new] + [from_behind(new, "grp", k) for k in range(1, groups)])

    flat = [slot for slots in basis for slot in slots]
    (parts,) = call(
        functools.partial(gram_kernel, groups),
        [shape(owners, width + width * width // LANES + EXTRA, LANES)],
        [VMEM] * (1 + len(flat)),
        (sent, *flat),
        6,
    )
    parts = exchange(parts, "row")
    return call(
        functools.partial(finish_kernel, groups),
        [shape(ITERS, width, ITERS * width), shape(ITERS, width, width), shape(width, row_count)],
        [VMEM] * (3 + len(flat)),
        (parts, *state, *flat),
        8,
        [pltpu.VMEM((total, total), F32), pltpu.VMEM((total, total), F32)],
    )


def solution(mesh):
    in_specs = (
        P("grp", "row", None, None, None),
        P("grp", "row", None),
        P("grp", "row", None),
        P("grp", "row"),
        P("row"),
        P(None, "row"),
    )
    out_specs = (P(), P(), P(None, "row"))
    return jax.shard_map(
        per_device, mesh=mesh, in_specs=in_specs, out_specs=out_specs, check_vma=False
    )
```

```python
import functools

import jax
import jax.numpy as jnp
from jax import lax
from jax.experimental import pallas as pl
from jax.experimental.pallas import tpu as pltpu
from jax.sharding import PartitionSpec as P


ITERS = 4
SHIFT = 1.0625
PULL = 0.375
KEEP = 8
CHUNKS = 6
GRANT = 50
LANES = 128
EXTRA = 8

F32 = jnp.float32
BF16 = jnp.bfloat16
HIGHEST = lax.Precision.HIGHEST
VMEM = pltpu.VMEM
SMEM = pltpu.SMEM


def spec(space):
    return pl.BlockSpec(memory_space=space)


def call(kernel, out_shape, in_spaces, operands, limit_mib, scratch=(), flops=2_000_000):
    return pl.pallas_call(
        kernel,
        out_shape=out_shape,
        in_specs=[spec(space) for space in in_spaces],
        out_specs=[spec(VMEM)] * len(out_shape),
        scratch_shapes=list(scratch),
        compiler_params=pltpu.CompilerParams(vmem_limit_bytes=limit_mib << 20),
        cost_estimate=pl.CostEstimate(flops=flops, bytes_accessed=1 << 20, transcendentals=0),
    )(*operands)


def shape(*dims, dtype=F32):
    return jax.ShapeDtypeStruct(dims, dtype)


def exchange(parts, axis):
    return lax.all_to_all(parts, axis, split_axis=0, concat_axis=0, tiled=True)


def gather_same_core(parts):
    owners = lax.axis_size("row")
    groups = [list(range(core, owners, 2)) for core in range(2)]
    same = lax.all_to_all(parts, "row", 0, 0, axis_index_groups=groups, tiled=True)
    other = lax.ppermute(same, "row", [(i, i ^ 1) for i in range(owners)])
    return same, other


def from_behind(value, axis, distance):
    size = lax.axis_size(axis)
    return lax.ppermute(value, axis, [(i, (i + distance) % size) for i in range(size)])


def dot(left, right, dims):
    return lax.dot_general(
        left, right, (dims, ((), ())), precision=HIGHEST, preferred_element_type=F32
    )


def plain(left, right):
    return dot(left, right, ((1,), (0,)))


def across(left, right):
    return dot(left, right, ((1,), (1,)))


def halves(value):
    return jnp.concatenate([value[:, :LANES], value[:, LANES:]], 0)


def whole(ref, r, width):
    return jnp.concatenate([ref[r, pl.ds(0, width), :], ref[r, pl.ds(width, width), :]], 1)


def pieces(value):
    high = value.astype(BF16).astype(F32)
    rest = value - high
    middle = rest.astype(BF16).astype(F32)
    return high, middle, rest - middle


def stacked(high, middle, low):
    line = lax.broadcasted_iota(jnp.int32, (EXTRA, high.shape[1]), 0)
    value = jnp.where(line == 2, low, 0.0)
    value = jnp.where(line == 1, middle, value)
    return jnp.where(line == 0, high, value)


def init_kernel(groups, owners, start_ref, shift_ref, *outs):
    slots, sent_ref, coef_ref = outs[:groups], outs[groups], outs[groups + 1]
    edge = coef_ref.shape[1]
    group = lax.axis_index("grp")
    for s in range(groups):
        block = lax.rem(group - s + groups, groups)
        slots[s][...] = start_ref[:, pl.ds(pl.multiple_of(block * edge, edge), edge)]
    rounded = halves(slots[0][...]).astype(BF16)
    for r in range(owners):
        sent_ref[r] = rounded
    coef_ref[...] = SHIFT - shift_ref[:, pl.ds(pl.multiple_of(group * edge, edge), edge)]


def load_kernel(tiles_ref, out_ref, sem):
    copy = pltpu.make_async_copy(tiles_ref.at[0, 0, pl.ds(0, out_ref.shape[0])], out_ref, sem)
    copy.start()
    copy.wait()


def fetch(tiles_ref, rest, sems):
    per_chunk = rest.shape[0] // CHUNKS
    copies = [
        pltpu.make_async_copy(
            tiles_ref.at[0, 0, pl.ds(KEEP + c * per_chunk, per_chunk)],
            rest.at[pl.ds(c * per_chunk, per_chunk)],
            sems.at[c],
        )
        for c in range(CHUNKS)
    ]
    for copy in copies:
        copy.start()
    return copies


def each_tile(kept_ref, rest, copies):
    per_chunk = rest.shape[0] // CHUNKS
    for k in range(KEEP):
        yield k, kept_ref[k]
    for c in range(CHUNKS):
        copies[c].wait()
        for k in range(c * per_chunk, (c + 1) * per_chunk):
            yield KEEP + k, rest[k]


def back_kernel(groups, steps, rows_ref, cols_ref, live_ref, kept_ref, tiles_ref, *refs):
    count = steps + 1
    vectors = [refs[i * groups : (i + 1) * groups] for i in range(count)]
    out_ref, total, rounded, rest, sems = refs[count * groups :]
    copies = fetch(tiles_ref, rest, sems)
    owners, width, _ = total.shape
    group = lax.axis_index("grp")
    live = live_ref[0, 0]
    for s in range(groups):
        rounded[s] = vectors[steps][s][...].astype(BF16)
    total[...] = jnp.zeros_like(total)
    grams = []
    for i in range(count):
        value = across(vectors[steps][0][...], vectors[i][0][...])
        for s in range(1, groups):
            value = value + across(vectors[steps][s][...], vectors[i][s][...])
        grams.append(value)
    if count * width < LANES:
        grams.append(jnp.zeros((width, LANES - count * width), F32))
    high, middle, low = pieces(jnp.concatenate(grams, 1))
    for r in range(owners):
        value = stacked(high[r : r + 1], middle[r : r + 1], low[r : r + 1])
        out_ref[r, pl.ds(2 * width, EXTRA), :] = value.astype(BF16)
    for k, tile in each_tile(kept_ref, rest, copies):
        source = lax.rem(group - rows_ref[0, 0, k] + groups, groups)
        product = lax.dot_general(
            rounded[source], tile, (((1,), (0,)), ((), ())), preferred_element_type=F32
        )
        total[cols_ref[0, 0, k]] += jnp.where(k < live, product, jnp.zeros_like(product))
    for r in range(owners):
        out_ref[r, pl.ds(0, 2 * width), :] = halves(total[r]).astype(BF16)


def ahead_kernel(
    groups, rows_ref, cols_ref, live_ref, kept_ref, tiles_ref, same_ref, other_ref, *refs
):
    outs, (total, rest, sems) = refs[:groups], refs[groups:]
    copies = fetch(tiles_ref, rest, sems)
    width = total.shape[1]
    group = lax.axis_index("grp")
    core = lax.rem(lax.axis_index("row"), 2)
    live = live_ref[0, 0]
    total[...] = jnp.zeros_like(total)
    for k, tile in each_tile(kept_ref, rest, copies):
        target = lax.rem(rows_ref[0, 0, k] - group + groups, groups)
        col = cols_ref[0, 0, k]
        place = lax.div(col, 2)
        vectors = jnp.where(
            lax.rem(col, 2) == core, whole(same_ref, place, width), whole(other_ref, place, width)
        )
        product = lax.dot_general(
            vectors, tile, (((1,), (1,)), ((), ())), preferred_element_type=F32
        )
        total[target] += jnp.where(k < live, product, jnp.zeros_like(product))
    for s in range(groups):
        outs[s][...] = total[s].astype(outs[s].dtype)


def combine_kernel(groups, last, back_ref, *refs):
    direct = refs[:groups]
    now_ref, before_ref, coef_ref = refs[groups : groups + 3]
    outs = refs[groups + 3 :]
    owners = back_ref.shape[0]
    width = now_ref.shape[0]
    image = direct[0][...]
    for s in range(1, groups):
        image = image + direct[s][...].astype(F32)
    for r in range(owners):
        image = image + whole(back_ref, r, width).astype(F32)
    new = 0.5 * image + coef_ref[...] * now_ref[...] - PULL * before_ref[...]
    outs[0][...] = new
    sums = back_ref[0, pl.ds(2 * width, EXTRA), :].astype(F32)
    for r in range(1, owners):
        sums = sums + back_ref[r, pl.ds(2 * width, EXTRA), :].astype(F32)
    row = sums[0:1] + (sums[1:2] + sums[2:3])
    if last:
        outs[1][...] = jnp.broadcast_to(row, (EXTRA, LANES))
    else:
        rounded = halves(new).astype(BF16)
        extra = stacked(*pieces(row)).astype(BF16)
        for r in range(outs[1].shape[0]):
            outs[1][r, pl.ds(0, 2 * width), :] = rounded
            outs[1][r, pl.ds(2 * width, EXTRA), :] = extra


def factor(block):
    width = block.shape[0]
    row_id = lax.broadcasted_iota(jnp.int32, (width, 2 * width), 0)
    col_id = lax.broadcasted_iota(jnp.int32, (width, 2 * width), 1)
    work = jnp.concatenate([block, jnp.zeros_like(block)], 1) + jnp.where(
        col_id == row_id + width, 1.0, 0.0
    )
    result = jnp.zeros_like(work)
    for k in range(width):
        row = work[k : k + 1, :]
        scale = lax.rsqrt(row[:, k : k + 1])
        row = row * scale
        column = work[:, k : k + 1] * scale
        result = jnp.where(row_id == k, jnp.broadcast_to(row, work.shape), result)
        if k + 1 < width:
            work = work - jnp.where(row_id > k, column, 0.0) * row
    return result[:, :width], result[:, width:]


def next_rows(j, gram_row, low, inv):
    width = gram_row.shape[0]
    here, done = pl.ds(j * width, width), pl.ds(0, j * width)
    low[here, :] = jnp.zeros((width, low.shape[1]), F32)
    inv[here, :] = jnp.zeros((width, inv.shape[1]), F32)
    schur = gram_row[:, j * width : (j + 1) * width]
    if j > 0:
        left = across(gram_row[:, : j * width], inv[done, done])
        schur = schur - across(left, left)
        back = plain(left, inv[done, done])
    upper, own_inverse = factor(schur)
    low[here, here] = upper.T
    inv[here, here] = own_inverse
    if j > 0:
        low[here, done] = left
        inv[here, done] = -plain(own_inverse, back)


def step_results(j, low, inv, width):
    used = (j + 1) * width
    value = low[pl.ds(width, used), :] - SHIFT * low[pl.ds(0, used), :]
    if j > 0:
        value = value + PULL * jnp.concatenate(
            [jnp.zeros((width, value.shape[1]), F32), low[pl.ds(0, j * width), :]], 0
        )
    image = plain(inv[pl.ds(j * width, width), pl.ds(0, used)], value)
    lane = lax.broadcasted_iota(jnp.int32, (width, ITERS * width), 1)
    square = (width, width)
    keep = lax.broadcasted_iota(jnp.int32, square, 0) >= lax.broadcasted_iota(jnp.int32, square, 1)
    return (
        jnp.where(lane < used, image[:, : ITERS * width], 0.0),
        jnp.where(keep, image[:, used : used + width], 0.0),
    )


def block_kernel(j, same_ref, other_ref, *refs):
    olds, (low_ref, inv_ref) = refs[:-2], refs[-2:]
    pairs = same_ref.shape[0]
    width = low_ref.shape[0] // (ITERS + 1)
    core = lax.rem(lax.axis_index("row"), 2)
    if j > 0:
        low_ref[...] = olds[0][...]
        inv_ref[...] = olds[1][...]
    rows = []
    for r in range(pairs):
        mine = same_ref[r, pl.ds(2 * width, EXTRA), :].astype(F32)
        theirs = other_ref[r, pl.ds(2 * width, EXTRA), :].astype(F32)
        for three in (jnp.where(core == 0, mine, theirs), jnp.where(core == 0, theirs, mine)):
            rows.append(three[0:1] + (three[1:2] + three[2:3]))
    next_rows(j, jnp.concatenate(rows, 0), low_ref, inv_ref)


def gram_kernel(groups, chunk_ref, *refs):
    out_ref = refs[-1]
    vectors = [refs[i * groups : (i + 1) * groups] for i in range(ITERS + 1)]
    owners = out_ref.shape[0]
    width = vectors[0][0].shape[0]
    grams = []
    for i in range(ITERS + 1):
        value = across(vectors[ITERS][0][...], vectors[i][0][...])
        for s in range(1, groups):
            value = value + across(vectors[ITERS][s][...], vectors[i][s][...])
        grams.append(value)
    parts = LANES // width
    rows = width // parts
    packed = jnp.concatenate([grams[ITERS][p * rows : (p + 1) * rows] for p in range(parts)], 1)
    value = jnp.concatenate(
        [jnp.concatenate(grams[:ITERS], 1), packed, jnp.broadcast_to(chunk_ref[0:1], (EXTRA, LANES))], 0
    )
    for r in range(owners):
        out_ref[r] = value


def finish_kernel(groups, parts_ref, old_low, old_inv, *refs):
    vectors = [refs[i * groups : (i + 1) * groups] for i in range(ITERS + 1)]
    proj_ref, fact_ref, out_ref, low, inv = refs[(ITERS + 1) * groups :]
    owners = parts_ref.shape[0]
    width, edge = vectors[0][0].shape
    group = lax.axis_index("grp")
    low[...] = old_low[...]
    inv[...] = old_inv[...]
    last = parts_ref.shape[1] - EXTRA
    rows = [parts_ref[r, pl.ds(last, EXTRA), :][0:1] for r in range(owners)]
    next_rows(ITERS - 1, jnp.concatenate(rows, 0), low, inv)
    sums = parts_ref[0, pl.ds(0, last), :]
    for r in range(1, owners):
        sums = sums + parts_ref[r, pl.ds(0, last), :]
    count = LANES // width
    corner = jnp.concatenate([sums[width:, p * width : (p + 1) * width] for p in range(count)], 0)
    next_rows(ITERS, jnp.concatenate([sums[:width], corner], 1), low, inv)
    for j in range(ITERS):
        proj_ref[j], fact_ref[j] = step_results(j, low, inv, width)
    for s in range(groups):
        value = plain(inv[pl.ds(ITERS * width, width), pl.ds(0, width)], vectors[0][s][...])
        for i in range(1, ITERS + 1):
            value = value + plain(
                inv[pl.ds(ITERS * width, width), pl.ds(i * width, width)], vectors[i][s][...]
            )
        block = lax.rem(group - s + groups, groups)
        out_ref[:, pl.ds(pl.multiple_of(block * edge, edge), edge)] = value


def per_device(tiles, tile_rows, tile_cols, live_tiles, dual_shift, start_block):
    count, edge = tiles.shape[2], tiles.shape[3]
    width, row_count = start_block.shape
    groups = lax.axis_size("grp")
    owners = lax.axis_size("row")
    total = (ITERS + 1) * width
    (kept,) = call(
        load_kernel,
        [shape(KEEP, edge, edge, dtype=BF16)],
        [pltpu.HBM],
        (tiles,),
        GRANT,
        [pltpu.SemaphoreType.DMA],
    )
    tables = (tile_rows, tile_cols, live_tiles, kept, tiles)
    spaces = [SMEM, SMEM, SMEM, VMEM, pltpu.HBM]
    rest = [pltpu.VMEM((count - KEEP, edge, edge), BF16), pltpu.SemaphoreType.DMA((CHUNKS,))]
    flops = 2 * count * width * edge * edge

    *slots, sent, coef = call(
        functools.partial(init_kernel, groups, owners // 2),
        [shape(width, edge)] * groups + [shape(owners // 2, 2 * width, LANES, dtype=BF16), shape(1, edge)],
        [VMEM, VMEM],
        (start_block, dual_shift[None, :]),
        4,
    )
    def block(j, gathered, state):
        return call(
            functools.partial(block_kernel, j),
            [shape(total, total)] * 2,
            [VMEM] * (2 + len(state)),
            (*gathered, *state),
            4,
        )

    before = jnp.zeros((width, edge), F32)
    basis = [slots]
    state = gathered = ()
    for step in range(ITERS):
        own = basis[step][0]
        same, other = gather_same_core(sent)
        flat = [slot for slots in basis for slot in slots]
        (parts,) = call(
            functools.partial(back_kernel, groups, step),
            [shape(owners, 2 * width + EXTRA, LANES, dtype=BF16)],
            spaces + [VMEM] * len(flat),
            (*tables, *flat),
            GRANT,
            [pltpu.VMEM((owners, width, edge), F32), pltpu.VMEM((groups, width, edge), BF16), *rest],
            flops,
        )
        arrived = exchange(parts, "row")
        direct = call(
            functools.partial(ahead_kernel, groups),
            [shape(width, edge)] + [shape(width, edge, dtype=BF16)] * (groups - 1),
            spaces + [VMEM, VMEM],
            (*tables, same, other),
            GRANT,
            [pltpu.VMEM((groups, width, edge), F32), *rest],
            flops,
        )
        direct = [direct[0]] + [from_behind(direct[k], "grp", k) for k in range(1, groups)]
        if step > 1:
            state = block(step - 2, gathered, state)
        gathered = (same, other)
        last = step == ITERS - 1
        second = shape(EXTRA, LANES) if last else shape(owners // 2, 2 * width + EXTRA, LANES, dtype=BF16)
        new, sent = call(
            functools.partial(combine_kernel, groups, last),
            [shape(width, edge), second],
            [VMEM] * (groups + 4),
            (arrived, *direct, own, before, coef),
            4,
        )
        before = own
        basis.append([new] + [from_behind(new, "grp", k) for k in range(1, groups)])

    state = block(ITERS - 2, gathered, state)
    flat = [slot for slots in basis for slot in slots]
    (parts,) = call(
        functools.partial(gram_kernel, groups),
        [shape(owners, width + width * width // LANES + EXTRA, LANES)],
        [VMEM] * (1 + len(flat)),
        (sent, *flat),
        6,
    )
    parts = exchange(parts, "row")
    return call(
        functools.partial(finish_kernel, groups),
        [shape(ITERS, width, ITERS * width), shape(ITERS, width, width), shape(width, row_count)],
        [VMEM] * (3 + len(flat)),
        (parts, *state, *flat),
        8,
        [pltpu.VMEM((total, total), F32), pltpu.VMEM((total, total), F32)],
    )


def solution(mesh):
    in_specs = (
        P("grp", "row", None, None, None),
        P("grp", "row", None),
        P("grp", "row", None),
        P("grp", "row"),
        P("row"),
        P(None, "row"),
    )
    out_specs = (P(), P(), P(None, "row"))
    return jax.shard_map(
        per_device, mesh=mesh, in_specs=in_specs, out_specs=out_specs, check_vma=False
    )
```

```python
import functools

import jax
import jax.numpy as jnp
from jax import lax
from jax.experimental import pallas as pl
from jax.experimental.pallas import tpu as pltpu
from jax.sharding import PartitionSpec as P


ITERS = 4
SHIFT = 1.0625
PULL = 0.375
KEEP = 8
CHUNKS = 6
GRANT = 50
LANES = 128
EXTRA = 8

F32 = jnp.float32
BF16 = jnp.bfloat16
HIGHEST = lax.Precision.HIGHEST
VMEM = pltpu.VMEM
SMEM = pltpu.SMEM


def spec(space):
    return pl.BlockSpec(memory_space=space)


def call(kernel, out_shape, in_spaces, operands, limit_mib, scratch=(), flops=2_000_000):
    return pl.pallas_call(
        kernel,
        out_shape=out_shape,
        in_specs=[spec(space) for space in in_spaces],
        out_specs=[spec(VMEM)] * len(out_shape),
        scratch_shapes=list(scratch),
        compiler_params=pltpu.CompilerParams(vmem_limit_bytes=limit_mib << 20),
        cost_estimate=pl.CostEstimate(flops=flops, bytes_accessed=1 << 20, transcendentals=0),
    )(*operands)


def shape(*dims, dtype=F32):
    return jax.ShapeDtypeStruct(dims, dtype)


def exchange(parts, axis):
    return lax.all_to_all(parts, axis, split_axis=0, concat_axis=0, tiled=True)


def gather_same_core(parts):
    owners = lax.axis_size("row")
    groups = [list(range(core, owners, 2)) for core in range(2)]
    same = lax.all_to_all(parts, "row", 0, 0, axis_index_groups=groups, tiled=True)
    other = lax.ppermute(same, "row", [(i, i ^ 1) for i in range(owners)])
    return same, other


def from_behind(value, axis, distance):
    size = lax.axis_size(axis)
    return lax.ppermute(value, axis, [(i, (i + distance) % size) for i in range(size)])


def dot(left, right, dims):
    return lax.dot_general(
        left, right, (dims, ((), ())), precision=HIGHEST, preferred_element_type=F32
    )


def plain(left, right):
    return dot(left, right, ((1,), (0,)))


def across(left, right):
    return dot(left, right, ((1,), (1,)))


def halves(value):
    return jnp.concatenate([value[:, :LANES], value[:, LANES:]], 0)


def whole(ref, r, width):
    return jnp.concatenate([ref[r, pl.ds(0, width), :], ref[r, pl.ds(width, width), :]], 1)


def pieces(value):
    high = value.astype(BF16).astype(F32)
    rest = value - high
    middle = rest.astype(BF16).astype(F32)
    return high, middle, rest - middle


def stacked(high, middle, low):
    line = lax.broadcasted_iota(jnp.int32, (EXTRA, high.shape[1]), 0)
    value = jnp.where(line == 2, low, 0.0)
    value = jnp.where(line == 1, middle, value)
    return jnp.where(line == 0, high, value)


def init_kernel(groups, owners, start_ref, shift_ref, *outs):
    slots, sent_ref, coef_ref = outs[:groups], outs[groups], outs[groups + 1]
    edge = coef_ref.shape[1]
    group = lax.axis_index("grp")
    for s in range(groups):
        block = lax.rem(group - s + groups, groups)
        slots[s][...] = start_ref[:, pl.ds(pl.multiple_of(block * edge, edge), edge)]
    rounded = halves(slots[0][...]).astype(BF16)
    for r in range(owners):
        sent_ref[r] = rounded
    coef_ref[...] = SHIFT - shift_ref[:, pl.ds(pl.multiple_of(group * edge, edge), edge)]


def load_kernel(tiles_ref, out_ref, sem):
    copy = pltpu.make_async_copy(tiles_ref.at[0, 0, pl.ds(0, out_ref.shape[0])], out_ref, sem)
    copy.start()
    copy.wait()


def fetch(tiles_ref, rest, sems):
    per_chunk = rest.shape[0] // CHUNKS
    copies = [
        pltpu.make_async_copy(
            tiles_ref.at[0, 0, pl.ds(KEEP + c * per_chunk, per_chunk)],
            rest.at[pl.ds(c * per_chunk, per_chunk)],
            sems.at[c],
        )
        for c in range(CHUNKS)
    ]
    for copy in copies:
        copy.start()
    return copies


def each_tile(kept_ref, rest, copies):
    per_chunk = rest.shape[0] // CHUNKS
    for k in range(KEEP):
        yield k, kept_ref[k]
    for c in range(CHUNKS):
        copies[c].wait()
        for k in range(c * per_chunk, (c + 1) * per_chunk):
            yield KEEP + k, rest[k]


def back_kernel(groups, steps, rows_ref, cols_ref, live_ref, kept_ref, tiles_ref, *refs):
    count = steps + 1
    vectors = [refs[i * groups : (i + 1) * groups] for i in range(count)]
    out_ref, total, rounded, rest, sems = refs[count * groups :]
    copies = fetch(tiles_ref, rest, sems)
    owners, width, _ = total.shape
    group = lax.axis_index("grp")
    live = live_ref[0, 0]
    for s in range(groups):
        rounded[s] = vectors[steps][s][...].astype(BF16)
    total[...] = jnp.zeros_like(total)
    grams = []
    for i in range(count):
        value = across(vectors[steps][0][...], vectors[i][0][...])
        for s in range(1, groups):
            value = value + across(vectors[steps][s][...], vectors[i][s][...])
        grams.append(value)
    if count * width < LANES:
        grams.append(jnp.zeros((width, LANES - count * width), F32))
    high, middle, low = pieces(jnp.concatenate(grams, 1))
    for r in range(owners):
        value = stacked(high[r : r + 1], middle[r : r + 1], low[r : r + 1])
        out_ref[r, pl.ds(2 * width, EXTRA), :] = value.astype(BF16)
    for k, tile in each_tile(kept_ref, rest, copies):
        source = lax.rem(group - rows_ref[0, 0, k] + groups, groups)
        product = lax.dot_general(
            rounded[source], tile, (((1,), (0,)), ((), ())), preferred_element_type=F32
        )
        total[cols_ref[0, 0, k]] += jnp.where(k < live, product, jnp.zeros_like(product))
    for r in range(owners):
        out_ref[r, pl.ds(0, 2 * width), :] = halves(total[r]).astype(BF16)


def ahead_kernel(
    groups, rows_ref, cols_ref, live_ref, kept_ref, tiles_ref, same_ref, other_ref, *refs
):
    outs, (total, rest, sems) = refs[:groups], refs[-3:]
    copies = fetch(tiles_ref, rest, sems)
    width = outs[0].shape[0]
    group = lax.axis_index("grp")
    core = lax.rem(lax.axis_index("row"), 2)
    live = live_ref[0, 0]
    total[...] = jnp.zeros_like(total)
    for k, tile in each_tile(kept_ref, rest, copies):
        target = lax.rem(rows_ref[0, 0, k] - group + groups, groups)
        col = cols_ref[0, 0, k]
        place = lax.div(col, 2)
        vectors = jnp.where(
            lax.rem(col, 2) == core, whole(same_ref, place, width), whole(other_ref, place, width)
        )
        product = lax.dot_general(
            tile, vectors, (((1,), (1,)), ((), ())), preferred_element_type=F32
        )
        total[target] += jnp.where(k < live, product, jnp.zeros_like(product))
    for s in range(groups):
        outs[s][...] = total[s].T.astype(outs[s].dtype)
    if same_ref.shape[1] > 2 * width:
        rows = []
        for r in range(same_ref.shape[0]):
            mine = same_ref[r, pl.ds(2 * width, EXTRA), :].astype(F32)
            theirs = other_ref[r, pl.ds(2 * width, EXTRA), :].astype(F32)
            for three in (jnp.where(core == 0, mine, theirs), jnp.where(core == 0, theirs, mine)):
                rows.append(three[0:1] + (three[1:2] + three[2:3]))
        refs[groups][...] = jnp.concatenate(rows, 0)


def combine_kernel(groups, last, back_ref, *refs):
    direct = refs[:groups]
    now_ref, before_ref, coef_ref = refs[groups : groups + 3]
    outs = refs[groups + 3 :]
    owners = back_ref.shape[0]
    width = now_ref.shape[0]
    image = direct[0][...]
    for s in range(1, groups):
        image = image + direct[s][...].astype(F32)
    for r in range(owners):
        image = image + whole(back_ref, r, width).astype(F32)
    new = 0.5 * image + coef_ref[...] * now_ref[...] - PULL * before_ref[...]
    outs[0][...] = new
    sums = back_ref[0, pl.ds(2 * width, EXTRA), :].astype(F32)
    for r in range(1, owners):
        sums = sums + back_ref[r, pl.ds(2 * width, EXTRA), :].astype(F32)
    row = sums[0:1] + (sums[1:2] + sums[2:3])
    if last:
        outs[1][...] = jnp.broadcast_to(row, (EXTRA, LANES))
    else:
        rounded = halves(new).astype(BF16)
        extra = stacked(*pieces(row)).astype(BF16)
        for r in range(outs[1].shape[0]):
            outs[1][r, pl.ds(0, 2 * width), :] = rounded
            outs[1][r, pl.ds(2 * width, EXTRA), :] = extra


def factor(block):
    width = block.shape[0]
    row_id = lax.broadcasted_iota(jnp.int32, (width, 2 * width), 0)
    col_id = lax.broadcasted_iota(jnp.int32, (width, 2 * width), 1)
    work = jnp.concatenate([block, jnp.zeros_like(block)], 1) + jnp.where(
        col_id == row_id + width, 1.0, 0.0
    )
    result = jnp.zeros_like(work)
    for k in range(width):
        row = work[k : k + 1, :]
        scale = lax.rsqrt(row[:, k : k + 1])
        row = row * scale
        column = work[:, k : k + 1] * scale
        result = jnp.where(row_id == k, jnp.broadcast_to(row, work.shape), result)
        if k + 1 < width:
            work = work - jnp.where(row_id > k, column, 0.0) * row
    return result[:, :width], result[:, width:]


def next_rows(j, gram_row, low, inv):
    width = gram_row.shape[0]
    here, done = pl.ds(j * width, width), pl.ds(0, j * width)
    low[here, :] = jnp.zeros((width, low.shape[1]), F32)
    inv[here, :] = jnp.zeros((width, inv.shape[1]), F32)
    schur = gram_row[:, j * width : (j + 1) * width]
    if j > 0:
        left = across(gram_row[:, : j * width], inv[done, done])
        schur = schur - across(left, left)
        back = plain(left, inv[done, done])
    upper, own_inverse = factor(schur)
    low[here, here] = upper.T
    inv[here, here] = own_inverse
    if j > 0:
        low[here, done] = left
        inv[here, done] = -plain(own_inverse, back)


def step_results(j, low, inv, width):
    used = (j + 1) * width
    value = low[pl.ds(width, used), :] - SHIFT * low[pl.ds(0, used), :]
    if j > 0:
        value = value + PULL * jnp.concatenate(
            [jnp.zeros((width, value.shape[1]), F32), low[pl.ds(0, j * width), :]], 0
        )
    image = plain(inv[pl.ds(j * width, width), pl.ds(0, used)], value)
    lane = lax.broadcasted_iota(jnp.int32, (width, ITERS * width), 1)
    square = (width, width)
    keep = lax.broadcasted_iota(jnp.int32, square, 0) >= lax.broadcasted_iota(jnp.int32, square, 1)
    return (
        jnp.where(lane < used, image[:, : ITERS * width], 0.0),
        jnp.where(keep, image[:, used : used + width], 0.0),
    )


def block_kernel(j, gram_ref, *refs):
    olds, (low_ref, inv_ref) = refs[:-2], refs[-2:]
    if j > 0:
        low_ref[...] = olds[0][...]
        inv_ref[...] = olds[1][...]
    next_rows(j, gram_ref[...], low_ref, inv_ref)


def gram_kernel(groups, chunk_ref, *refs):
    out_ref = refs[-1]
    vectors = [refs[i * groups : (i + 1) * groups] for i in range(ITERS + 1)]
    owners = out_ref.shape[0]
    width = vectors[0][0].shape[0]
    grams = []
    for i in range(ITERS + 1):
        value = across(vectors[ITERS][0][...], vectors[i][0][...])
        for s in range(1, groups):
            value = value + across(vectors[ITERS][s][...], vectors[i][s][...])
        grams.append(value)
    parts = LANES // width
    rows = width // parts
    packed = jnp.concatenate([grams[ITERS][p * rows : (p + 1) * rows] for p in range(parts)], 1)
    value = jnp.concatenate(
        [jnp.concatenate(grams[:ITERS], 1), packed, jnp.broadcast_to(chunk_ref[0:1], (EXTRA, LANES))], 0
    )
    for r in range(owners):
        out_ref[r] = value


def finish_kernel(groups, parts_ref, old_low, old_inv, *refs):
    vectors = [refs[i * groups : (i + 1) * groups] for i in range(ITERS + 1)]
    proj_ref, fact_ref, out_ref, low, inv = refs[(ITERS + 1) * groups :]
    owners = parts_ref.shape[0]
    width, edge = vectors[0][0].shape
    group = lax.axis_index("grp")
    low[...] = old_low[...]
    inv[...] = old_inv[...]
    last = parts_ref.shape[1] - EXTRA
    rows = [parts_ref[r, pl.ds(last, EXTRA), :][0:1] for r in range(owners)]
    next_rows(ITERS - 1, jnp.concatenate(rows, 0), low, inv)
    sums = parts_ref[0, pl.ds(0, last), :]
    for r in range(1, owners):
        sums = sums + parts_ref[r, pl.ds(0, last), :]
    count = LANES // width
    corner = jnp.concatenate([sums[width:, p * width : (p + 1) * width] for p in range(count)], 0)
    next_rows(ITERS, jnp.concatenate([sums[:width], corner], 1), low, inv)
    for j in range(ITERS):
        proj_ref[j], fact_ref[j] = step_results(j, low, inv, width)
    for s in range(groups):
        value = plain(inv[pl.ds(ITERS * width, width), pl.ds(0, width)], vectors[0][s][...])
        for i in range(1, ITERS + 1):
            value = value + plain(
                inv[pl.ds(ITERS * width, width), pl.ds(i * width, width)], vectors[i][s][...]
            )
        block = lax.rem(group - s + groups, groups)
        out_ref[:, pl.ds(pl.multiple_of(block * edge, edge), edge)] = value


def per_device(tiles, tile_rows, tile_cols, live_tiles, dual_shift, start_block):
    count, edge = tiles.shape[2], tiles.shape[3]
    width, row_count = start_block.shape
    groups = lax.axis_size("grp")
    owners = lax.axis_size("row")
    total = (ITERS + 1) * width
    (kept,) = call(
        load_kernel,
        [shape(KEEP, edge, edge, dtype=BF16)],
        [pltpu.HBM],
        (tiles,),
        GRANT,
        [pltpu.SemaphoreType.DMA],
    )
    tables = (tile_rows, tile_cols, live_tiles, kept, tiles)
    spaces = [SMEM, SMEM, SMEM, VMEM, pltpu.HBM]
    rest = [pltpu.VMEM((count - KEEP, edge, edge), BF16), pltpu.SemaphoreType.DMA((CHUNKS,))]
    flops = 2 * count * width * edge * edge

    *slots, sent, coef = call(
        functools.partial(init_kernel, groups, owners // 2),
        [shape(width, edge)] * groups + [shape(owners // 2, 2 * width, LANES, dtype=BF16), shape(1, edge)],
        [VMEM, VMEM],
        (start_block, dual_shift[None, :]),
        4,
    )
    def block(j, rows, state):
        return call(
            functools.partial(block_kernel, j),
            [shape(total, total)] * 2,
            [VMEM] * (1 + len(state)),
            (rows, *state),
            4,
        )

    before = jnp.zeros((width, edge), F32)
    basis = [slots]
    grams = []
    for step in range(ITERS):
        own = basis[step][0]
        same, other = gather_same_core(sent)
        flat = [slot for slots in basis for slot in slots]
        (parts,) = call(
            functools.partial(back_kernel, groups, step),
            [shape(owners, 2 * width + EXTRA, LANES, dtype=BF16)],
            spaces + [VMEM] * len(flat),
            (*tables, *flat),
            GRANT,
            [pltpu.VMEM((owners, width, edge), F32), pltpu.VMEM((groups, width, edge), BF16), *rest],
            flops,
        )
        arrived = exchange(parts, "row")
        direct = call(
            functools.partial(ahead_kernel, groups),
            [shape(width, edge)]
            + [shape(width, edge, dtype=BF16)] * (groups - 1)
            + [shape(width, LANES)] * (step > 0),
            spaces + [VMEM, VMEM],
            (*tables, same, other),
            GRANT,
            [pltpu.VMEM((groups, edge, width), F32), *rest],
            flops,
        )
        grams += direct[groups:]
        direct = [direct[0]] + [from_behind(direct[k], "grp", k) for k in range(1, groups)]
        last = step == ITERS - 1
        second = shape(EXTRA, LANES) if last else shape(owners // 2, 2 * width + EXTRA, LANES, dtype=BF16)
        new, sent = call(
            functools.partial(combine_kernel, groups, last),
            [shape(width, edge), second],
            [VMEM] * (groups + 4),
            (arrived, *direct, own, before, coef),
            4,
        )
        before = own
        basis.append([new] + [from_behind(new, "grp", k) for k in range(1, groups)])

    flat = [slot for slots in basis for slot in slots]
    (parts,) = call(
        functools.partial(gram_kernel, groups),
        [shape(owners, width + width * width // LANES + EXTRA, LANES)],
        [VMEM] * (1 + len(flat)),
        (sent, *flat),
        6,
    )
    state = ()
    parts = exchange(parts, "row")
    for j, rows in enumerate(grams):
        state = block(j, rows, state)
    return call(
        functools.partial(finish_kernel, groups),
        [shape(ITERS, width, ITERS * width), shape(ITERS, width, width), shape(width, row_count)],
        [VMEM] * (3 + len(flat)),
        (parts, *state, *flat),
        8,
        [pltpu.VMEM((total, total), F32), pltpu.VMEM((total, total), F32)],
    )


def solution(mesh):
    in_specs = (
        P("grp", "row", None, None, None),
        P("grp", "row", None),
        P("grp", "row", None),
        P("grp", "row"),
        P("row"),
        P(None, "row"),
    )
    out_specs = (P(), P(), P(None, "row"))
    return jax.shard_map(
        per_device, mesh=mesh, in_specs=in_specs, out_specs=out_specs, check_vma=False
    )
```

```python
import functools

import jax
import jax.numpy as jnp
from jax import lax
from jax.experimental import pallas as pl
from jax.experimental.pallas import tpu as pltpu
from jax.sharding import PartitionSpec as P


ITERS = 4
SHIFT = 1.0625
PULL = 0.375
KEEP = 20
CHUNKS = 4
GRANT = 52
LANES = 128
EXTRA = 8

F32 = jnp.float32
BF16 = jnp.bfloat16
HIGHEST = lax.Precision.HIGHEST
VMEM = pltpu.VMEM
SMEM = pltpu.SMEM


def spec(space):
    return pl.BlockSpec(memory_space=space)


def call(kernel, out_shape, in_spaces, operands, limit_mib, scratch=(), flops=2_000_000):
    return pl.pallas_call(
        kernel,
        out_shape=out_shape,
        in_specs=[spec(space) for space in in_spaces],
        out_specs=[spec(VMEM)] * len(out_shape),
        scratch_shapes=list(scratch),
        compiler_params=pltpu.CompilerParams(vmem_limit_bytes=limit_mib << 20),
        cost_estimate=pl.CostEstimate(flops=flops, bytes_accessed=1 << 20, transcendentals=0),
    )(*operands)


def shape(*dims, dtype=F32):
    return jax.ShapeDtypeStruct(dims, dtype)


def exchange(parts, axis):
    return lax.all_to_all(parts, axis, split_axis=0, concat_axis=0, tiled=True)


def same_core(parts):
    owners = lax.axis_size("row")
    groups = [list(range(core, owners, 2)) for core in range(2)]
    return lax.all_to_all(parts, "row", 0, 0, axis_index_groups=groups, tiled=True)


def swapped(value, axis, mask):
    return lax.ppermute(value, axis, [(i, i ^ mask) for i in range(lax.axis_size(axis))])


def all_slots(own):
    one = swapped(own, "grp", 1)
    three = swapped(own, "grp", 3)
    two = swapped(one, "grp", 3)
    return [own, one, two, three]


def to_owners(parts):
    two = swapped(parts[2], "grp", 2)
    one, three = swapped(parts[1], "grp", 1), swapped(parts[3], "grp", 3)
    return [parts[0], one, two, three]


def dot(left, right, dims):
    return lax.dot_general(
        left, right, (dims, ((), ())), precision=HIGHEST, preferred_element_type=F32
    )


def plain(left, right):
    return dot(left, right, ((1,), (0,)))


def across(left, right):
    return dot(left, right, ((1,), (1,)))


def halves(value):
    return jnp.concatenate([value[:, :LANES], value[:, LANES:]], 0)


def whole(ref, r, width):
    return jnp.concatenate([ref[r, pl.ds(0, width), :], ref[r, pl.ds(width, width), :]], 1)


def pieces(value):
    high = value.astype(BF16).astype(F32)
    rest = value - high
    middle = rest.astype(BF16).astype(F32)
    return high, middle, rest - middle


def stacked(high, middle, low):
    line = lax.broadcasted_iota(jnp.int32, (EXTRA, high.shape[1]), 0)
    value = jnp.where(line == 2, low, 0.0)
    value = jnp.where(line == 1, middle, value)
    return jnp.where(line == 0, high, value)


def init_kernel(groups, owners, start_ref, shift_ref, *outs):
    slots, sent_ref, coef_ref = outs[:groups], outs[groups], outs[groups + 1]
    edge = coef_ref.shape[1]
    group = lax.axis_index("grp")
    for s in range(groups):
        block = group ^ s
        slots[s][...] = start_ref[:, pl.ds(pl.multiple_of(block * edge, edge), edge)]
    rounded = halves(slots[0][...]).astype(BF16)
    for r in range(owners):
        sent_ref[r] = rounded
    coef_ref[...] = SHIFT - shift_ref[:, pl.ds(pl.multiple_of(group * edge, edge), edge)]


def load_kernel(tiles_ref, out_ref, sem):
    copy = pltpu.make_async_copy(tiles_ref.at[0, 0, pl.ds(0, out_ref.shape[0])], out_ref, sem)
    copy.start()
    copy.wait()


def fetch(tiles_ref, rest, sems):
    per_chunk = rest.shape[0] // CHUNKS
    copies = [
        pltpu.make_async_copy(
            tiles_ref.at[0, 0, pl.ds(KEEP + c * per_chunk, per_chunk)],
            rest.at[pl.ds(c * per_chunk, per_chunk)],
            sems.at[c],
        )
        for c in range(CHUNKS)
    ]
    for copy in copies:
        copy.start()
    return copies


def clear(total):
    @pl.loop(0, total.shape[0])
    def _(i):
        total[i] = jnp.zeros(total.shape[1:], F32)


def each_tile(kept_ref, rest, copies):
    per_chunk = rest.shape[0] // CHUNKS
    for k in range(KEEP):
        yield k, kept_ref[k]
    for c in range(CHUNKS):
        copies[c].wait()
        for k in range(c * per_chunk, (c + 1) * per_chunk):
            yield KEEP + k, rest[k]


def back_kernel(groups, steps, rows_ref, cols_ref, live_ref, kept_ref, tiles_ref, *refs):
    count = steps + 1
    vectors = [refs[i * groups : (i + 1) * groups] for i in range(count)]
    out_ref, total, rounded, rest, sems = refs[count * groups :]
    copies = fetch(tiles_ref, rest, sems)
    owners, width, _ = total.shape
    group = lax.axis_index("grp")
    live = live_ref[0, 0]
    clear(total)
    for s in range(groups):
        rounded[s] = vectors[steps][s][...].astype(BF16)
    grams = []
    for i in range(count):
        value = across(vectors[steps][0][...], vectors[i][0][...])
        for s in range(1, groups):
            value = value + across(vectors[steps][s][...], vectors[i][s][...])
        grams.append(value)
    if count * width < LANES:
        grams.append(jnp.zeros((width, LANES - count * width), F32))
    high, middle, low = pieces(jnp.concatenate(grams, 1))
    for r in range(owners):
        value = stacked(high[r : r + 1], middle[r : r + 1], low[r : r + 1])
        out_ref[r, pl.ds(2 * width, EXTRA), :] = value.astype(BF16)
    for k, tile in each_tile(kept_ref, rest, copies):
        source = rows_ref[0, 0, k] ^ group
        product = lax.dot_general(
            rounded[source], tile, (((1,), (0,)), ((), ())), preferred_element_type=F32
        )
        total[cols_ref[0, 0, k]] += jnp.where(k < live, product, jnp.zeros_like(product))
    for r in range(owners):
        out_ref[r, pl.ds(0, 2 * width), :] = halves(total[r]).astype(BF16)


def ahead_kernel(
    groups, rows_ref, cols_ref, live_ref, kept_ref, tiles_ref, same_ref, other_ref, *refs
):
    outs, (total, rest, sems) = refs[:groups], refs[-3:]
    copies = fetch(tiles_ref, rest, sems)
    width = outs[0].shape[0]
    group = lax.axis_index("grp")
    core = lax.axis_index("row") & 1
    live = live_ref[0, 0]
    clear(total)
    for k, tile in each_tile(kept_ref, rest, copies):
        target = rows_ref[0, 0, k] ^ group
        col = cols_ref[0, 0, k]
        place = col >> 1
        vectors = jnp.where(
            (col & 1) == core, whole(same_ref, place, width), whole(other_ref, place, width)
        )
        product = lax.dot_general(
            vectors, tile, (((1,), (1,)), ((), ())), preferred_element_type=F32
        )
        total[target] += jnp.where(k < live, product, jnp.zeros_like(product))
    for s in range(groups):
        outs[s][...] = total[s].astype(outs[s].dtype)
    if same_ref.shape[1] > 2 * width:
        rows = []
        for r in range(same_ref.shape[0]):
            mine = same_ref[r, pl.ds(2 * width, EXTRA), :].astype(F32)
            theirs = other_ref[r, pl.ds(2 * width, EXTRA), :].astype(F32)
            for three in (jnp.where(core == 0, mine, theirs), jnp.where(core == 0, theirs, mine)):
                rows.append(three[0:1] + (three[1:2] + three[2:3]))
        refs[groups][...] = jnp.concatenate(rows, 0)


def combine_kernel(groups, last, back_ref, *refs):
    direct = refs[:groups]
    now_ref, before_ref, coef_ref = refs[groups : groups + 3]
    outs = refs[groups + 3 :]
    owners = back_ref.shape[0]
    width = now_ref.shape[0]
    image = direct[0][...]
    for s in range(1, groups):
        image = image + direct[s][...].astype(F32)
    for r in range(owners):
        image = image + whole(back_ref, r, width).astype(F32)
    new = 0.5 * image + coef_ref[...] * now_ref[...] - PULL * before_ref[...]
    outs[0][...] = new
    sums = back_ref[0, pl.ds(2 * width, EXTRA), :].astype(F32)
    for r in range(1, owners):
        sums = sums + back_ref[r, pl.ds(2 * width, EXTRA), :].astype(F32)
    row = sums[0:1] + (sums[1:2] + sums[2:3])
    if last:
        outs[1][...] = jnp.broadcast_to(row, (EXTRA, LANES))
    else:
        rounded = halves(new).astype(BF16)
        extra = stacked(*pieces(row)).astype(BF16)
        for r in range(outs[1].shape[0]):
            outs[1][r, pl.ds(0, 2 * width), :] = rounded
            outs[1][r, pl.ds(2 * width, EXTRA), :] = extra


def factor(block):
    width = block.shape[0]
    row_id = lax.broadcasted_iota(jnp.int32, (width, 2 * width), 0)
    col_id = lax.broadcasted_iota(jnp.int32, (width, 2 * width), 1)
    work = jnp.concatenate([block, jnp.zeros_like(block)], 1) + jnp.where(
        col_id == row_id + width, 1.0, 0.0
    )
    result = jnp.zeros_like(work)
    for k in range(0, width, 2):
        first = jnp.broadcast_to(work[:, k : k + 1], work.shape)
        second = jnp.broadcast_to(work[:, k + 1 : k + 2], work.shape)
        scale = lax.rsqrt(first[k : k + 1])
        link = first[k + 1 : k + 2] * scale
        scale2 = lax.rsqrt(second[k + 1 : k + 2] - link * link)
        row = work[k : k + 1] * scale
        row2 = (work[k + 1 : k + 2] - link * row) * scale2
        result = jnp.where(row_id == k, row, jnp.where(row_id == k + 1, row2, result))
        if k + 2 < width:
            column = first * scale
            column2 = (second - column * link) * scale2
            work = work - jnp.where(row_id > k + 1, column * row + column2 * row2, 0.0)
    return result[:, :width], result[:, width:]


def next_rows(j, gram_row, low, inv):
    width = gram_row.shape[0]
    here, done = pl.ds(j * width, width), pl.ds(0, j * width)
    low[here, :] = jnp.zeros((width, low.shape[1]), F32)
    inv[here, :] = jnp.zeros((width, inv.shape[1]), F32)
    schur = gram_row[:, j * width : (j + 1) * width]
    if j > 0:
        left = across(gram_row[:, : j * width], inv[done, done])
        schur = schur - across(left, left)
        back = plain(left, inv[done, done])
    upper, own_inverse = factor(schur)
    low[here, here] = upper.T
    inv[here, here] = own_inverse
    if j > 0:
        low[here, done] = left
        inv[here, done] = -plain(own_inverse, back)


def step_results(j, low, inv, width):
    used = (j + 1) * width
    value = low[pl.ds(width, used), :] - SHIFT * low[pl.ds(0, used), :]
    if j > 0:
        value = value + PULL * jnp.concatenate(
            [jnp.zeros((width, value.shape[1]), F32), low[pl.ds(0, j * width), :]], 0
        )
    image = plain(inv[pl.ds(j * width, width), pl.ds(0, used)], value)
    lane = lax.broadcasted_iota(jnp.int32, (width, ITERS * width), 1)
    square = (width, width)
    keep = lax.broadcasted_iota(jnp.int32, square, 0) >= lax.broadcasted_iota(jnp.int32, square, 1)
    return (
        jnp.where(lane < used, image[:, : ITERS * width], 0.0),
        jnp.where(keep, image[:, used : used + width], 0.0),
    )


def block_kernel(j, gram_ref, *refs):
    olds, (low_ref, inv_ref) = refs[:-2], refs[-2:]
    if j > 0:
        low_ref[...] = olds[0][...]
        inv_ref[...] = olds[1][...]
    next_rows(j, gram_ref[...], low_ref, inv_ref)


def gram_kernel(groups, chunk_ref, *refs):
    out_ref = refs[-1]
    vectors = [refs[i * groups : (i + 1) * groups] for i in range(ITERS + 1)]
    width = vectors[0][0].shape[0]
    grams = []
    for i in range(ITERS + 1):
        value = across(vectors[ITERS][0][...], vectors[i][0][...])
        for s in range(1, groups):
            value = value + across(vectors[ITERS][s][...], vectors[i][s][...])
        grams.append(value)
    parts = LANES // width
    rows = width // parts
    packed = jnp.concatenate([grams[ITERS][p * rows : (p + 1) * rows] for p in range(parts)], 1)
    out_ref[...] = jnp.concatenate(
        [jnp.concatenate(grams[:ITERS], 1), packed, jnp.broadcast_to(chunk_ref[0:1], (EXTRA, LANES))], 0
    )


def pair_kernel(mine_ref, theirs_ref, out_ref):
    last = mine_ref.shape[0] - EXTRA
    core = lax.axis_index("row") & 1
    line = lax.broadcasted_iota(jnp.int32, (EXTRA, LANES), 0)
    rows = jnp.where(line == core, mine_ref[pl.ds(last, EXTRA), :], theirs_ref[pl.ds(last, EXTRA), :])
    value = mine_ref[pl.ds(0, last), :] + theirs_ref[pl.ds(0, last), :]
    for r in range(out_ref.shape[0]):
        out_ref[r, pl.ds(0, last), :] = value
        out_ref[r, pl.ds(last, EXTRA), :] = rows


def finish_kernel(groups, parts_ref, old_low, old_inv, *refs):
    vectors = [refs[i * groups : (i + 1) * groups] for i in range(ITERS + 1)]
    proj_ref, fact_ref, out_ref, low, inv = refs[(ITERS + 1) * groups :]
    owners = parts_ref.shape[0]
    width, edge = vectors[0][0].shape
    group = lax.axis_index("grp")
    low[...] = old_low[...]
    inv[...] = old_inv[...]
    last = parts_ref.shape[1] - EXTRA
    rows = [parts_ref[r, pl.ds(last, EXTRA), :][0:2] for r in range(owners)]
    next_rows(ITERS - 1, jnp.concatenate(rows, 0), low, inv)
    sums = parts_ref[0, pl.ds(0, last), :]
    for r in range(1, owners):
        sums = sums + parts_ref[r, pl.ds(0, last), :]
    count = LANES // width
    corner = jnp.concatenate([sums[width:, p * width : (p + 1) * width] for p in range(count)], 0)
    next_rows(ITERS, jnp.concatenate([sums[:width], corner], 1), low, inv)
    for j in range(ITERS):
        proj_ref[j], fact_ref[j] = step_results(j, low, inv, width)
    for s in range(groups):
        value = plain(inv[pl.ds(ITERS * width, width), pl.ds(0, width)], vectors[0][s][...])
        for i in range(1, ITERS + 1):
            value = value + plain(
                inv[pl.ds(ITERS * width, width), pl.ds(i * width, width)], vectors[i][s][...]
            )
        block = group ^ s
        out_ref[:, pl.ds(pl.multiple_of(block * edge, edge), edge)] = value


def per_device(tiles, tile_rows, tile_cols, live_tiles, dual_shift, start_block):
    count, edge = tiles.shape[2], tiles.shape[3]
    width, row_count = start_block.shape
    groups = lax.axis_size("grp")
    owners = lax.axis_size("row")
    total = (ITERS + 1) * width
    (kept,) = call(
        load_kernel,
        [shape(KEEP, edge, edge, dtype=BF16)],
        [pltpu.HBM],
        (tiles,),
        GRANT,
        [pltpu.SemaphoreType.DMA],
    )
    tables = (tile_rows, tile_cols, live_tiles, kept, tiles)
    spaces = [SMEM, SMEM, SMEM, VMEM, pltpu.HBM]
    rest = [pltpu.VMEM((count - KEEP, edge, edge), BF16), pltpu.SemaphoreType.DMA((CHUNKS,))]
    flops = 2 * count * width * edge * edge

    *slots, sent, coef = call(
        functools.partial(init_kernel, groups, owners // 2),
        [shape(width, edge)] * groups + [shape(owners // 2, 2 * width, LANES, dtype=BF16), shape(1, edge)],
        [VMEM, VMEM],
        (start_block, dual_shift[None, :]),
        4,
    )
    def block(j, rows, state):
        return call(
            functools.partial(block_kernel, j),
            [shape(total, total)] * 2,
            [VMEM] * (1 + len(state)),
            (rows, *state),
            4,
        )

    before = jnp.zeros((width, edge), F32)
    basis = [slots]
    grams = []
    for step in range(ITERS):
        own = basis[step][0]
        same = same_core(sent)
        other = swapped(same, "row", 1)
        flat = [slot for slots in basis for slot in slots]
        (parts,) = call(
            functools.partial(back_kernel, groups, step),
            [shape(owners, 2 * width + EXTRA, LANES, dtype=BF16)],
            spaces + [VMEM] * len(flat),
            (*tables, *flat),
            GRANT,
            [pltpu.VMEM((owners, width, edge), F32), pltpu.VMEM((groups, width, edge), BF16), *rest],
            flops,
        )
        arrived = exchange(parts, "row")
        direct = call(
            functools.partial(ahead_kernel, groups),
            [shape(width, edge)]
            + [shape(width, edge, dtype=BF16)] * (groups - 1)
            + [shape(width, LANES)] * (step > 0),
            spaces + [VMEM, VMEM],
            (*tables, same, other),
            GRANT,
            [pltpu.VMEM((groups, width, edge), F32), *rest],
            flops,
        )
        grams += direct[groups:]
        direct = to_owners(direct)
        last = step == ITERS - 1
        second = shape(EXTRA, LANES) if last else shape(owners // 2, 2 * width + EXTRA, LANES, dtype=BF16)
        new, sent = call(
            functools.partial(combine_kernel, groups, last),
            [shape(width, edge), second],
            [VMEM] * (groups + 4),
            (arrived, *direct, own, before, coef),
            4,
        )
        before = own
        basis.append(all_slots(new))

    flat = [slot for slots in basis for slot in slots]
    lines = width + width * width // LANES + EXTRA
    (part,) = call(
        functools.partial(gram_kernel, groups),
        [shape(lines, LANES)],
        [VMEM] * (1 + len(flat)),
        (sent, *flat),
        4,
    )
    (parts,) = call(
        pair_kernel,
        [shape(owners // 2, lines, LANES)],
        [VMEM, VMEM],
        (part, swapped(part, "row", 1)),
        4,
    )
    state = ()
    parts = same_core(parts)
    for j, rows in enumerate(grams):
        state = block(j, rows, state)
    return call(
        functools.partial(finish_kernel, groups),
        [shape(ITERS, width, ITERS * width), shape(ITERS, width, width), shape(width, row_count)],
        [VMEM] * (3 + len(flat)),
        (parts, *state, *flat),
        8,
        [pltpu.VMEM((total, total), F32), pltpu.VMEM((total, total), F32)],
    )


def solution(mesh):
    in_specs = (
        P("grp", "row", None, None, None),
        P("grp", "row", None),
        P("grp", "row", None),
        P("grp", "row"),
        P("row"),
        P(None, "row"),
    )
    out_specs = (P(), P(), P(None, "row"))
    return jax.shard_map(
        per_device, mesh=mesh, in_specs=in_specs, out_specs=out_specs, check_vma=False
    )
```

```python
import functools

import jax
import jax.numpy as jnp
from jax import lax
from jax.experimental import pallas as pl
from jax.experimental.pallas import tpu as pltpu
from jax.sharding import PartitionSpec as P


ITERS = 4
SHIFT = 1.0625
PULL = 0.375
KEEP = 12
CHUNKS = 5
GRANT = 50
LANES = 128
EXTRA = 8

F32 = jnp.float32
BF16 = jnp.bfloat16
HIGHEST = lax.Precision.HIGHEST
VMEM = pltpu.VMEM
SMEM = pltpu.SMEM


def spec(space):
    return pl.BlockSpec(memory_space=space)


def call(kernel, out_shape, in_spaces, operands, limit_mib, scratch=(), flops=2_000_000):
    return pl.pallas_call(
        kernel,
        out_shape=out_shape,
        in_specs=[spec(space) for space in in_spaces],
        out_specs=[spec(VMEM)] * len(out_shape),
        scratch_shapes=list(scratch),
        compiler_params=pltpu.CompilerParams(vmem_limit_bytes=limit_mib << 20),
        cost_estimate=pl.CostEstimate(flops=flops, bytes_accessed=1 << 20, transcendentals=0),
    )(*operands)


def shape(*dims, dtype=F32):
    return jax.ShapeDtypeStruct(dims, dtype)


def exchange(parts, axis):
    return lax.all_to_all(parts, axis, split_axis=0, concat_axis=0, tiled=True)


def same_core(parts):
    owners = lax.axis_size("row")
    groups = [list(range(core, owners, 2)) for core in range(2)]
    return lax.all_to_all(parts, "row", 0, 0, axis_index_groups=groups, tiled=True)


def swapped(value, axis, mask):
    return lax.ppermute(value, axis, [(i, i ^ mask) for i in range(lax.axis_size(axis))])


def trade(parts):
    arrived = [parts[0]]
    for k in range(1, len(parts)):
        arrived.append(swapped(parts[k], "grp", k))
    return arrived


def dot(left, right, dims):
    return lax.dot_general(
        left, right, (dims, ((), ())), precision=HIGHEST, preferred_element_type=F32
    )


def plain(left, right):
    return dot(left, right, ((1,), (0,)))


def across(left, right):
    return dot(left, right, ((1,), (1,)))


def halves(value):
    return jnp.concatenate([value[:, :LANES], value[:, LANES:]], 0)


def whole(ref, r, width):
    return jnp.concatenate([ref[r, pl.ds(0, width), :], ref[r, pl.ds(width, width), :]], 1)


def pieces(value):
    high = value.astype(BF16).astype(F32)
    rest = value - high
    middle = rest.astype(BF16).astype(F32)
    return high, middle, rest - middle


def stacked(high, middle, low):
    line = lax.broadcasted_iota(jnp.int32, (EXTRA, high.shape[1]), 0)
    value = jnp.where(line == 2, low, 0.0)
    value = jnp.where(line == 1, middle, value)
    return jnp.where(line == 0, high, value)


def init_kernel(groups, copies, start_ref, *refs):
    slots, sent_ref = refs[:groups], refs[groups]
    edge = slots[0].shape[1]
    group = lax.axis_index("grp")
    for s in range(groups):
        block = group ^ s
        slots[s][...] = start_ref[:, pl.ds(pl.multiple_of(block * edge, edge), edge)]
    rounded = halves(slots[0][...]).astype(BF16)
    for r in range(copies):
        sent_ref[r] = rounded


def load_kernel(tiles_ref, out_ref, sem):
    copy = pltpu.make_async_copy(tiles_ref.at[0, 0, pl.ds(0, out_ref.shape[0])], out_ref, sem)
    copy.start()
    copy.wait()


def fetch(tiles_ref, rest, sems):
    per_chunk = rest.shape[0] // CHUNKS
    copies = [
        pltpu.make_async_copy(
            tiles_ref.at[0, 0, pl.ds(KEEP + c * per_chunk, per_chunk)],
            rest.at[pl.ds(c * per_chunk, per_chunk)],
            sems.at[c],
        )
        for c in range(CHUNKS)
    ]
    for copy in copies:
        copy.start()
    return copies


def clear(total):
    @pl.loop(0, total.shape[0])
    def _(i):
        total[i] = jnp.zeros(total.shape[1:], F32)


def each_tile(kept_ref, rest, copies):
    per_chunk = rest.shape[0] // CHUNKS
    for k in range(KEEP):
        yield k, kept_ref[k]
    for c in range(CHUNKS):
        copies[c].wait()
        for k in range(c * per_chunk, (c + 1) * per_chunk):
            yield KEEP + k, rest[k]


def back_kernel(groups, steps, rows_ref, cols_ref, live_ref, kept_ref, tiles_ref, *refs):
    count = steps + 1
    vectors = [refs[i * groups : (i + 1) * groups] for i in range(count)]
    out_ref, total, rounded, rest, sems = refs[count * groups :]
    copies = fetch(tiles_ref, rest, sems)
    owners, width, _ = total.shape
    group = lax.axis_index("grp")
    live = live_ref[0, 0]
    clear(total)
    for s in range(groups):
        rounded[s] = vectors[steps][s][...].astype(BF16)
    grams = []
    for i in range(count):
        value = across(vectors[steps][0][...], vectors[i][0][...])
        for s in range(1, groups):
            value = value + across(vectors[steps][s][...], vectors[i][s][...])
        grams.append(value)
    if count * width < LANES:
        grams.append(jnp.zeros((width, LANES - count * width), F32))
    high, middle, low = pieces(jnp.concatenate(grams, 1))
    for r in range(owners):
        value = stacked(high[r : r + 1], middle[r : r + 1], low[r : r + 1])
        out_ref[r, pl.ds(2 * width, EXTRA), :] = value.astype(BF16)
    for k, tile in each_tile(kept_ref, rest, copies):
        source = rows_ref[0, 0, k] ^ group
        product = lax.dot_general(
            rounded[source], tile, (((1,), (0,)), ((), ())), preferred_element_type=F32
        )
        total[cols_ref[0, 0, k]] += jnp.where(k < live, product, jnp.zeros_like(product))
    for r in range(owners):
        out_ref[r, pl.ds(0, 2 * width), :] = halves(total[r]).astype(BF16)


def ahead_kernel(
    groups, rows_ref, cols_ref, live_ref, kept_ref, tiles_ref, same_ref, other_ref, *refs
):
    outs, (total, rest, sems) = refs[:groups], refs[-3:]
    copies = fetch(tiles_ref, rest, sems)
    width = outs[0].shape[0]
    group = lax.axis_index("grp")
    core = lax.axis_index("row") & 1
    live = live_ref[0, 0]
    clear(total)
    for k, tile in each_tile(kept_ref, rest, copies):
        target = rows_ref[0, 0, k] ^ group
        col = cols_ref[0, 0, k]
        place = col >> 1
        vectors = jnp.where(
            (col & 1) == core, whole(same_ref, place, width), whole(other_ref, place, width)
        )
        product = lax.dot_general(
            vectors, tile, (((1,), (1,)), ((), ())), preferred_element_type=F32
        )
        total[target] += jnp.where(k < live, product, jnp.zeros_like(product))
    for s in range(groups):
        outs[s][...] = total[s].astype(outs[s].dtype)
    if same_ref.shape[1] > 2 * width:
        rows = []
        for r in range(same_ref.shape[0]):
            mine = same_ref[r, pl.ds(2 * width, EXTRA), :].astype(F32)
            theirs = other_ref[r, pl.ds(2 * width, EXTRA), :].astype(F32)
            for three in (jnp.where(core == 0, mine, theirs), jnp.where(core == 0, theirs, mine)):
                rows.append(three[0:1] + (three[1:2] + three[2:3]))
        refs[groups][...] = jnp.concatenate(rows, 0)


def combine_kernel(groups, last, back_ref, *refs):
    direct = refs[:groups]
    now_ref, before_ref, shift_ref = refs[groups : groups + 3]
    outs = refs[groups + 3 :]
    owners = back_ref.shape[0]
    width = now_ref.shape[0]
    image = direct[0][...]
    for s in range(1, groups):
        image = image + direct[s][...].astype(F32)
    for r in range(owners):
        image = image + whole(back_ref, r, width).astype(F32)
    edge = now_ref.shape[1]
    block = lax.axis_index("grp")
    shift = shift_ref[:, pl.ds(pl.multiple_of(block * edge, edge), edge)]
    new = 0.5 * image + (SHIFT - shift) * now_ref[...] - PULL * before_ref[...]
    outs[0][...] = new
    sums = back_ref[0, pl.ds(2 * width, EXTRA), :].astype(F32)
    for r in range(1, owners):
        sums = sums + back_ref[r, pl.ds(2 * width, EXTRA), :].astype(F32)
    row = sums[0:1] + (sums[1:2] + sums[2:3])
    if last:
        outs[1][...] = jnp.broadcast_to(row, (EXTRA, LANES))
    else:
        rounded = halves(new).astype(BF16)
        extra = stacked(*pieces(row)).astype(BF16)
        for r in range(outs[1].shape[0]):
            outs[1][r, pl.ds(0, 2 * width), :] = rounded
            outs[1][r, pl.ds(2 * width, EXTRA), :] = extra


def factor(block):
    width = block.shape[0]
    row_id = lax.broadcasted_iota(jnp.int32, (width, 2 * width), 0)
    col_id = lax.broadcasted_iota(jnp.int32, (width, 2 * width), 1)
    work = jnp.concatenate([block, jnp.zeros_like(block)], 1) + jnp.where(
        col_id == row_id + width, 1.0, 0.0
    )
    result = jnp.zeros_like(work)
    for k in range(0, width, 2):
        first = jnp.broadcast_to(work[:, k : k + 1], work.shape)
        second = jnp.broadcast_to(work[:, k + 1 : k + 2], work.shape)
        scale = lax.rsqrt(first[k : k + 1])
        link = first[k + 1 : k + 2] * scale
        scale2 = lax.rsqrt(second[k + 1 : k + 2] - link * link)
        row = work[k : k + 1] * scale
        row2 = (work[k + 1 : k + 2] - link * row) * scale2
        result = jnp.where(row_id == k, row, jnp.where(row_id == k + 1, row2, result))
        if k + 2 < width:
            column = first * scale
            column2 = (second - column * link) * scale2
            work = work - jnp.where(row_id > k + 1, column * row + column2 * row2, 0.0)
    return result[:, :width], result[:, width:]


def next_rows(j, gram_row, low, inv):
    width = gram_row.shape[0]
    here, done = pl.ds(j * width, width), pl.ds(0, j * width)
    low[here, :] = jnp.zeros((width, low.shape[1]), F32)
    inv[here, :] = jnp.zeros((width, inv.shape[1]), F32)
    schur = gram_row[:, j * width : (j + 1) * width]
    if j > 0:
        left = across(gram_row[:, : j * width], inv[done, done])
        schur = schur - across(left, left)
        back = plain(left, inv[done, done])
    upper, own_inverse = factor(schur)
    low[here, here] = upper.T
    inv[here, here] = own_inverse
    if j > 0:
        low[here, done] = left
        inv[here, done] = -plain(own_inverse, back)


def step_results(j, low, inv, width):
    used = (j + 1) * width
    value = low[pl.ds(width, used), :] - SHIFT * low[pl.ds(0, used), :]
    if j > 0:
        value = value + PULL * jnp.concatenate(
            [jnp.zeros((width, value.shape[1]), F32), low[pl.ds(0, j * width), :]], 0
        )
    image = plain(inv[pl.ds(j * width, width), pl.ds(0, used)], value)
    lane = lax.broadcasted_iota(jnp.int32, (width, ITERS * width), 1)
    square = (width, width)
    keep = lax.broadcasted_iota(jnp.int32, square, 0) >= lax.broadcasted_iota(jnp.int32, square, 1)
    return (
        jnp.where(lane < used, image[:, : ITERS * width], 0.0),
        jnp.where(keep, image[:, used : used + width], 0.0),
    )


def block_kernel(j, gram_ref, *refs):
    outs = 2 if j == 0 else 4
    olds, (low_ref, inv_ref) = refs[:-outs], refs[-outs:][:2]
    if j > 0:
        low_ref[...] = olds[0][...]
        inv_ref[...] = olds[1][...]
    next_rows(j, gram_ref[...], low_ref, inv_ref)
    if j > 0:
        refs[-2][...], refs[-1][...] = step_results(j - 1, low_ref, inv_ref, gram_ref.shape[0])


def gram_kernel(groups, chunk_ref, *refs):
    out_ref = refs[-1]
    vectors = [refs[i * groups : (i + 1) * groups] for i in range(ITERS + 1)]
    width = vectors[0][0].shape[0]
    grams = []
    for i in range(ITERS + 1):
        value = across(vectors[ITERS][0][...], vectors[i][0][...])
        for s in range(1, groups):
            value = value + across(vectors[ITERS][s][...], vectors[i][s][...])
        grams.append(value)
    parts = LANES // width
    rows = width // parts
    packed = jnp.concatenate([grams[ITERS][p * rows : (p + 1) * rows] for p in range(parts)], 1)
    out_ref[...] = jnp.concatenate(
        [jnp.concatenate(grams[:ITERS], 1), packed, jnp.broadcast_to(chunk_ref[0:1], (EXTRA, LANES))], 0
    )


def pair_kernel(mine_ref, theirs_ref, out_ref):
    last = mine_ref.shape[0] - EXTRA
    core = lax.axis_index("row") & 1
    line = lax.broadcasted_iota(jnp.int32, (EXTRA, LANES), 0)
    rows = jnp.where(line == core, mine_ref[pl.ds(last, EXTRA), :], theirs_ref[pl.ds(last, EXTRA), :])
    value = mine_ref[pl.ds(0, last), :] + theirs_ref[pl.ds(0, last), :]
    for r in range(out_ref.shape[0]):
        out_ref[r, pl.ds(0, last), :] = value
        out_ref[r, pl.ds(last, EXTRA), :] = rows


def finish_kernel(groups, parts_ref, old_low, old_inv, *refs):
    known = ITERS - 2
    early, refs = refs[: 2 * known], refs[2 * known :]
    vectors = [refs[i * groups : (i + 1) * groups] for i in range(ITERS + 1)]
    proj_ref, fact_ref, out_ref, low, inv = refs[(ITERS + 1) * groups :]
    owners = parts_ref.shape[0]
    width, edge = vectors[0][0].shape
    group = lax.axis_index("grp")
    low[...] = old_low[...]
    inv[...] = old_inv[...]
    last = parts_ref.shape[1] - EXTRA
    rows = [parts_ref[r, pl.ds(last, EXTRA), :][0:2] for r in range(owners)]
    next_rows(ITERS - 1, jnp.concatenate(rows, 0), low, inv)
    sums = parts_ref[0, pl.ds(0, last), :]
    for r in range(1, owners):
        sums = sums + parts_ref[r, pl.ds(0, last), :]
    count = LANES // width
    corner = jnp.concatenate([sums[width:, p * width : (p + 1) * width] for p in range(count)], 0)
    next_rows(ITERS, jnp.concatenate([sums[:width], corner], 1), low, inv)
    for j in range(known):
        proj_ref[j], fact_ref[j] = early[2 * j][...], early[2 * j + 1][...]
    for j in range(known, ITERS):
        proj_ref[j], fact_ref[j] = step_results(j, low, inv, width)
    for s in range(groups):
        value = plain(inv[pl.ds(ITERS * width, width), pl.ds(0, width)], vectors[0][s][...])
        for i in range(1, ITERS + 1):
            value = value + plain(
                inv[pl.ds(ITERS * width, width), pl.ds(i * width, width)], vectors[i][s][...]
            )
        block = group ^ s
        out_ref[:, pl.ds(pl.multiple_of(block * edge, edge), edge)] = value


def per_device(tiles, tile_rows, tile_cols, live_tiles, dual_shift, start_block):
    count, edge = tiles.shape[2], tiles.shape[3]
    width, row_count = start_block.shape
    groups = lax.axis_size("grp")
    owners = lax.axis_size("row")
    total = (ITERS + 1) * width
    (kept,) = call(
        load_kernel,
        [shape(KEEP, edge, edge, dtype=BF16)],
        [pltpu.HBM],
        (tiles,),
        GRANT,
        [pltpu.SemaphoreType.DMA],
    )
    tables = (tile_rows, tile_cols, live_tiles, kept, tiles)
    spaces = [SMEM, SMEM, SMEM, VMEM, pltpu.HBM]
    rest = [pltpu.VMEM((count - KEEP, edge, edge), BF16), pltpu.SemaphoreType.DMA((CHUNKS,))]
    flops = 2 * count * width * edge * edge

    *slots, sent = call(
        functools.partial(init_kernel, groups, owners // 2),
        [shape(width, edge)] * groups + [shape(owners // 2, 2 * width, LANES, dtype=BF16)],
        [VMEM],
        (start_block,),
        4,
    )
    shift = dual_shift[None, :]
    def block(j, rows, state):
        return call(
            functools.partial(block_kernel, j),
            [shape(total, total)] * 2
            + [shape(width, ITERS * width), shape(width, width)] * (j > 0),
            [VMEM] * (1 + len(state)),
            (rows, *state),
            4,
        )

    before = jnp.zeros((width, edge), F32)
    basis = [slots]
    grams = []
    for step in range(ITERS):
        own = basis[step][0]
        same = same_core(sent)
        other = swapped(same, "row", 1)
        flat = [slot for slots in basis for slot in slots]
        (parts,) = call(
            functools.partial(back_kernel, groups, step),
            [shape(owners, 2 * width + EXTRA, LANES, dtype=BF16)],
            spaces + [VMEM] * len(flat),
            (*tables, *flat),
            GRANT,
            [pltpu.VMEM((owners, width, edge), F32), pltpu.VMEM((groups, width, edge), BF16), *rest],
            flops,
        )
        arrived = exchange(parts, "row")
        direct = call(
            functools.partial(ahead_kernel, groups),
            [shape(width, edge)]
            + [shape(width, edge, dtype=BF16)] * (groups - 1)
            + [shape(width, LANES)] * (step > 0),
            spaces + [VMEM, VMEM],
            (*tables, same, other),
            GRANT,
            [pltpu.VMEM((groups, width, edge), F32), *rest],
            flops,
        )
        grams += direct[groups:]
        direct = trade(direct[:groups])
        last = step == ITERS - 1
        second = shape(EXTRA, LANES) if last else shape(owners // 2, 2 * width + EXTRA, LANES, dtype=BF16)
        new, sent = call(
            functools.partial(combine_kernel, groups, last),
            [shape(width, edge), second],
            [VMEM] * (groups + 4),
            (arrived, *direct, own, before, shift),
            4,
        )
        before = own
        basis.append(trade([new] * groups))

    flat = [slot for slots in basis for slot in slots]
    lines = width + width * width // LANES + EXTRA
    (part,) = call(
        functools.partial(gram_kernel, groups),
        [shape(lines, LANES)],
        [VMEM] * (1 + len(flat)),
        (sent, *flat),
        4,
    )
    (parts,) = call(
        pair_kernel,
        [shape(owners // 2, lines, LANES)],
        [VMEM, VMEM],
        (part, swapped(part, "row", 1)),
        4,
    )
    state = ()
    parts = same_core(parts)
    early = []
    for j, rows in enumerate(grams):
        *state, proj, fact = [*block(j, rows, state), None, None][:4]
        early += [proj, fact] * (j > 0)
    return call(
        functools.partial(finish_kernel, groups),
        [shape(ITERS, width, ITERS * width), shape(ITERS, width, width), shape(width, row_count)],
        [VMEM] * (3 + len(early) + len(flat)),
        (parts, *state, *early, *flat),
        8,
        [pltpu.VMEM((total, total), F32), pltpu.VMEM((total, total), F32)],
    )


def solution(mesh):
    in_specs = (
        P("grp", "row", None, None, None),
        P("grp", "row", None),
        P("grp", "row", None),
        P("grp", "row"),
        P("row"),
        P(None, "row"),
    )
    out_specs = (P(), P(), P(None, "row"))
    return jax.shard_map(
        per_device, mesh=mesh, in_specs=in_specs, out_specs=out_specs, check_vma=False
    )
```

```python
import functools

import jax
import jax.numpy as jnp
from jax import lax
from jax.experimental import pallas as pl
from jax.experimental.pallas import tpu as pltpu
from jax.sharding import PartitionSpec as P


ITERS = 4
KEEP = 12
CHUNKS = 5
GRANT = 50
LANES = 128
EXTRA = 8

F32 = jnp.float32
BF16 = jnp.bfloat16
HIGHEST = lax.Precision.HIGHEST
VMEM = pltpu.VMEM
SMEM = pltpu.SMEM


def spec(space):
    return pl.BlockSpec(memory_space=space)


def call(kernel, out_shape, in_spaces, operands, limit_mib, scratch=(), flops=2_000_000):
    return pl.pallas_call(
        kernel,
        out_shape=out_shape,
        in_specs=[spec(space) for space in in_spaces],
        out_specs=[spec(VMEM)] * len(out_shape),
        scratch_shapes=list(scratch),
        compiler_params=pltpu.CompilerParams(vmem_limit_bytes=limit_mib << 20),
        cost_estimate=pl.CostEstimate(flops=flops, bytes_accessed=1 << 20, transcendentals=0),
    )(*operands)


def shape(*dims, dtype=F32):
    return jax.ShapeDtypeStruct(dims, dtype)


def exchange(parts, axis):
    return lax.all_to_all(parts, axis, split_axis=0, concat_axis=0, tiled=True)


def same_core(parts):
    owners = lax.axis_size("row")
    groups = [list(range(core, owners, 2)) for core in range(2)]
    return lax.all_to_all(parts, "row", 0, 0, axis_index_groups=groups, tiled=True)


def swapped(value, axis, mask):
    return lax.ppermute(value, axis, [(i, i ^ mask) for i in range(lax.axis_size(axis))])


def trade(parts):
    arrived = [parts[0]]
    for k in range(1, len(parts)):
        arrived.append(swapped(parts[k], "grp", k))
    return arrived


def dot(left, right, dims):
    return lax.dot_general(
        left, right, (dims, ((), ())), precision=HIGHEST, preferred_element_type=F32
    )


def plain(left, right):
    return dot(left, right, ((1,), (0,)))


def across(left, right):
    return dot(left, right, ((1,), (1,)))


def halves(value):
    return jnp.concatenate([value[:, :LANES], value[:, LANES:]], 0)


def whole(ref, r, width):
    return jnp.concatenate([ref[r, pl.ds(0, width), :], ref[r, pl.ds(width, width), :]], 1)


def pieces(value):
    high = value.astype(BF16).astype(F32)
    rest = value - high
    middle = rest.astype(BF16).astype(F32)
    return high, middle, rest - middle


def stacked(*rows):
    line = lax.broadcasted_iota(jnp.int32, (EXTRA, rows[0].shape[1]), 0)
    value = jnp.zeros(line.shape, F32)
    for i, row in enumerate(rows):
        value = jnp.where(line == i, row, value)
    return value


def lane_sums(value):
    value = jnp.sum(value, 0, keepdims=True)
    parts = [value[:, i : i + LANES] for i in range(0, value.shape[1], LANES)]
    return sum(parts[1:], parts[0])


def squares(slots):
    return lane_sums(sum(slot[...] * slot[...] for slot in slots))


def init_kernel(groups, copies, start_ref, *refs):
    slots, sent_ref = refs[:groups], refs[groups]
    edge = slots[0].shape[1]
    group = lax.axis_index("grp")
    for s in range(groups):
        block = group ^ s
        slots[s][...] = start_ref[:, pl.ds(pl.multiple_of(block * edge, edge), edge)]
    rounded = halves(slots[0][...]).astype(BF16)
    for r in range(copies):
        sent_ref[r] = rounded


def load_kernel(tiles_ref, out_ref, sem):
    copy = pltpu.make_async_copy(tiles_ref.at[0, 0, pl.ds(0, out_ref.shape[0])], out_ref, sem)
    copy.start()
    copy.wait()


def fetch(tiles_ref, rest, sems):
    per_chunk = rest.shape[0] // CHUNKS
    copies = [
        pltpu.make_async_copy(
            tiles_ref.at[0, 0, pl.ds(KEEP + c * per_chunk, per_chunk)],
            rest.at[pl.ds(c * per_chunk, per_chunk)],
            sems.at[c],
        )
        for c in range(CHUNKS)
    ]
    for copy in copies:
        copy.start()
    return copies


def clear(total):
    @pl.loop(0, total.shape[0])
    def _(i):
        total[i] = jnp.zeros(total.shape[1:], F32)


def each_tile(kept_ref, rest, copies):
    per_chunk = rest.shape[0] // CHUNKS
    for k in range(KEEP):
        yield k, kept_ref[k]
    for c in range(CHUNKS):
        copies[c].wait()
        for k in range(c * per_chunk, (c + 1) * per_chunk):
            yield KEEP + k, rest[k]


def back_kernel(groups, steps, rows_ref, cols_ref, live_ref, kept_ref, tiles_ref, *refs):
    count = steps + 1
    vectors = [refs[i * groups : (i + 1) * groups] for i in range(count)]
    *shifts, out_ref, total, rounded, rest, sems = refs[count * groups :]
    copies = fetch(tiles_ref, rest, sems)
    owners, width, _ = total.shape
    group = lax.axis_index("grp")
    live = live_ref[0, 0]
    clear(total)
    for s in range(groups):
        rounded[s] = vectors[steps][s][...].astype(BF16)
    grams = []
    for i in range(count):
        value = across(vectors[steps][0][...], vectors[i][0][...])
        for s in range(1, groups):
            value = value + across(vectors[steps][s][...], vectors[i][s][...])
        grams.append(value)
    if count * width < LANES:
        grams.append(jnp.zeros((width, LANES - count * width), F32))
    high, middle, low = pieces(jnp.concatenate(grams, 1))
    scales = []
    if steps == 0:
        scales = pieces(lane_sums(shifts[0][...]))[:2]
    elif steps == 1:
        scales = pieces(squares(vectors[1]))[:2] + pieces(squares(vectors[0]))[:2]
    for r in range(owners):
        value = stacked(high[r : r + 1], middle[r : r + 1], low[r : r + 1], *scales)
        out_ref[r, pl.ds(2 * width, EXTRA), :] = value.astype(BF16)
    for k, tile in each_tile(kept_ref, rest, copies):
        source = rows_ref[0, 0, k] ^ group
        product = lax.dot_general(
            rounded[source], tile, (((1,), (0,)), ((), ())), preferred_element_type=F32
        )
        total[cols_ref[0, 0, k]] += jnp.where(k < live, product, jnp.zeros_like(product))
    for r in range(owners):
        out_ref[r, pl.ds(0, 2 * width), :] = halves(total[r]).astype(BF16)


def ahead_kernel(
    groups, rows_ref, cols_ref, live_ref, kept_ref, tiles_ref, same_ref, other_ref, *refs
):
    outs, (total, rest, sems) = refs[:groups], refs[-3:]
    copies = fetch(tiles_ref, rest, sems)
    width = outs[0].shape[0]
    group = lax.axis_index("grp")
    core = lax.axis_index("row") & 1
    live = live_ref[0, 0]
    clear(total)
    for k, tile in each_tile(kept_ref, rest, copies):
        target = rows_ref[0, 0, k] ^ group
        col = cols_ref[0, 0, k]
        place = col >> 1
        vectors = jnp.where(
            (col & 1) == core, whole(same_ref, place, width), whole(other_ref, place, width)
        )
        product = lax.dot_general(
            vectors, tile, (((1,), (1,)), ((), ())), preferred_element_type=F32
        )
        total[target] += jnp.where(k < live, product, jnp.zeros_like(product))
    for s in range(groups):
        outs[s][...] = total[s].astype(outs[s].dtype)
    if same_ref.shape[1] > 2 * width:
        rows = []
        for r in range(same_ref.shape[0]):
            mine = same_ref[r, pl.ds(2 * width, EXTRA), :].astype(F32)
            theirs = other_ref[r, pl.ds(2 * width, EXTRA), :].astype(F32)
            for three in (jnp.where(core == 0, mine, theirs), jnp.where(core == 0, theirs, mine)):
                rows.append(three[0:1] + (three[1:2] + three[2:3]))
        refs[groups][...] = jnp.concatenate(rows, 0)


def combine_kernel(groups, step, back_ref, *refs):
    direct = refs[:groups]
    now_ref, shift_ref = refs[groups : groups + 2]
    refs = refs[groups + 2 :]
    width, edge = now_ref.shape
    owners = back_ref.shape[0]
    image = direct[0][...]
    for s in range(1, groups):
        image = image + direct[s][...].astype(F32)
    for r in range(owners):
        image = image + whole(back_ref, r, width).astype(F32)
    sums = back_ref[0, pl.ds(2 * width, EXTRA), :].astype(F32)
    for r in range(1, owners):
        sums = sums + back_ref[r, pl.ds(2 * width, EXTRA), :].astype(F32)
    row = sums[0:1] + (sums[1:2] + sums[2:3])
    total = jnp.sum(sums, 1, keepdims=True)
    block = lax.axis_index("grp")
    diagonal = shift_ref[:, pl.ds(pl.multiple_of(block * edge, edge), edge)]
    line = lax.broadcasted_iota(jnp.int32, (EXTRA, LANES), 0)
    if step == 0:
        new_ref, sent_ref, coef_ref = refs
        shift = (total[3:4] + total[4:5]) * (1.0 / (owners * shift_ref.shape[1]))
        coef_ref[...] = jnp.broadcast_to(shift, coef_ref.shape)
        new = 0.5 * image + (shift - diagonal) * now_ref[...]
    else:
        before_ref, old_ref, new_ref, sent_ref = refs[:4]
        shift, pull = old_ref[0:1, 0:1], old_ref[1:2, 0:1]
        if step == 1:
            pull = (total[3:4] + total[4:5]) / (total[5:6] + total[6:7])
            refs[4][...] = jnp.where(line == 0, shift, pull)
        new = 0.5 * image + (shift - diagonal) * now_ref[...] - pull * before_ref[...]
    new_ref[...] = new
    if step == ITERS - 1:
        sent_ref[...] = jnp.broadcast_to(row, (EXTRA, LANES))
    else:
        rounded = halves(new).astype(BF16)
        extra = stacked(*pieces(row)).astype(BF16)
        for r in range(sent_ref.shape[0]):
            sent_ref[r, pl.ds(0, 2 * width), :] = rounded
            sent_ref[r, pl.ds(2 * width, EXTRA), :] = extra


def factor(block):
    width = block.shape[0]
    row_id = lax.broadcasted_iota(jnp.int32, (width, 2 * width), 0)
    col_id = lax.broadcasted_iota(jnp.int32, (width, 2 * width), 1)
    work = jnp.concatenate([block, jnp.zeros_like(block)], 1) + jnp.where(
        col_id == row_id + width, 1.0, 0.0
    )
    result = jnp.zeros_like(work)
    for k in range(0, width, 2):
        first = jnp.broadcast_to(work[:, k : k + 1], work.shape)
        second = jnp.broadcast_to(work[:, k + 1 : k + 2], work.shape)
        scale = lax.rsqrt(first[k : k + 1])
        link = first[k + 1 : k + 2] * scale
        scale2 = lax.rsqrt(second[k + 1 : k + 2] - link * link)
        row = work[k : k + 1] * scale
        row2 = (work[k + 1 : k + 2] - link * row) * scale2
        result = jnp.where(row_id == k, row, jnp.where(row_id == k + 1, row2, result))
        if k + 2 < width:
            column = first * scale
            column2 = (second - column * link) * scale2
            work = work - jnp.where(row_id > k + 1, column * row + column2 * row2, 0.0)
    return result[:, :width], result[:, width:]


def next_rows(j, gram_row, low, inv):
    width = gram_row.shape[0]
    here, done = pl.ds(j * width, width), pl.ds(0, j * width)
    low[here, :] = jnp.zeros((width, low.shape[1]), F32)
    inv[here, :] = jnp.zeros((width, inv.shape[1]), F32)
    schur = gram_row[:, j * width : (j + 1) * width]
    if j > 0:
        left = across(gram_row[:, : j * width], inv[done, done])
        schur = schur - across(left, left)
        back = plain(left, inv[done, done])
    upper, own_inverse = factor(schur)
    low[here, here] = upper.T
    inv[here, here] = own_inverse
    if j > 0:
        low[here, done] = left
        inv[here, done] = -plain(own_inverse, back)


def step_results(j, low, inv, coef_ref, width):
    used = (j + 1) * width
    shift, pull = coef_ref[0:1, 0:1], coef_ref[1:2, 0:1]
    value = low[pl.ds(width, used), :] - shift * low[pl.ds(0, used), :]
    if j > 0:
        value = value + pull * jnp.concatenate(
            [jnp.zeros((width, value.shape[1]), F32), low[pl.ds(0, j * width), :]], 0
        )
    image = plain(inv[pl.ds(j * width, width), pl.ds(0, used)], value)
    lane = lax.broadcasted_iota(jnp.int32, (width, ITERS * width), 1)
    square = (width, width)
    keep = lax.broadcasted_iota(jnp.int32, square, 0) >= lax.broadcasted_iota(jnp.int32, square, 1)
    return (
        jnp.where(lane < used, image[:, : ITERS * width], 0.0),
        jnp.where(keep, image[:, used : used + width], 0.0),
    )


def block_kernel(j, gram_ref, coef_ref, *refs):
    outs = 2 if j == 0 else 4
    olds, (low_ref, inv_ref) = refs[:-outs], refs[-outs:][:2]
    if j > 0:
        low_ref[...] = olds[0][...]
        inv_ref[...] = olds[1][...]
    next_rows(j, gram_ref[...], low_ref, inv_ref)
    if j > 0:
        refs[-2][...], refs[-1][...] = step_results(
            j - 1, low_ref, inv_ref, coef_ref, gram_ref.shape[0]
        )


def gram_kernel(groups, chunk_ref, *refs):
    out_ref = refs[-1]
    vectors = [refs[i * groups : (i + 1) * groups] for i in range(ITERS + 1)]
    width = vectors[0][0].shape[0]
    grams = []
    for i in range(ITERS + 1):
        value = across(vectors[ITERS][0][...], vectors[i][0][...])
        for s in range(1, groups):
            value = value + across(vectors[ITERS][s][...], vectors[i][s][...])
        grams.append(value)
    parts = LANES // width
    rows = width // parts
    packed = jnp.concatenate([grams[ITERS][p * rows : (p + 1) * rows] for p in range(parts)], 1)
    out_ref[...] = jnp.concatenate(
        [jnp.concatenate(grams[:ITERS], 1), packed, jnp.broadcast_to(chunk_ref[0:1], (EXTRA, LANES))], 0
    )


def pair_kernel(mine_ref, theirs_ref, out_ref):
    last = mine_ref.shape[0] - EXTRA
    core = lax.axis_index("row") & 1
    line = lax.broadcasted_iota(jnp.int32, (EXTRA, LANES), 0)
    rows = jnp.where(line == core, mine_ref[pl.ds(last, EXTRA), :], theirs_ref[pl.ds(last, EXTRA), :])
    value = mine_ref[pl.ds(0, last), :] + theirs_ref[pl.ds(0, last), :]
    for r in range(out_ref.shape[0]):
        out_ref[r, pl.ds(0, last), :] = value
        out_ref[r, pl.ds(last, EXTRA), :] = rows


def finish_kernel(groups, parts_ref, coef_ref, old_low, old_inv, *refs):
    known = ITERS - 2
    early, refs = refs[: 2 * known], refs[2 * known :]
    vectors = [refs[i * groups : (i + 1) * groups] for i in range(ITERS + 1)]
    proj_ref, fact_ref, out_ref, low, inv = refs[(ITERS + 1) * groups :]
    owners = parts_ref.shape[0]
    width, edge = vectors[0][0].shape
    group = lax.axis_index("grp")
    low[...] = old_low[...]
    inv[...] = old_inv[...]
    last = parts_ref.shape[1] - EXTRA
    rows = [parts_ref[r, pl.ds(last, EXTRA), :][0:2] for r in range(owners)]
    next_rows(ITERS - 1, jnp.concatenate(rows, 0), low, inv)
    sums = parts_ref[0, pl.ds(0, last), :]
    for r in range(1, owners):
        sums = sums + parts_ref[r, pl.ds(0, last), :]
    count = LANES // width
    corner = jnp.concatenate([sums[width:, p * width : (p + 1) * width] for p in range(count)], 0)
    next_rows(ITERS, jnp.concatenate([sums[:width], corner], 1), low, inv)
    for j in range(known):
        proj_ref[j], fact_ref[j] = early[2 * j][...], early[2 * j + 1][...]
    for j in range(known, ITERS):
        proj_ref[j], fact_ref[j] = step_results(j, low, inv, coef_ref, width)
    for s in range(groups):
        value = plain(inv[pl.ds(ITERS * width, width), pl.ds(0, width)], vectors[0][s][...])
        for i in range(1, ITERS + 1):
            value = value + plain(
                inv[pl.ds(ITERS * width, width), pl.ds(i * width, width)], vectors[i][s][...]
            )
        block = group ^ s
        out_ref[:, pl.ds(pl.multiple_of(block * edge, edge), edge)] = value


def per_device(tiles, tile_rows, tile_cols, live_tiles, dual_shift, start_block):
    count, edge = tiles.shape[2], tiles.shape[3]
    width, row_count = start_block.shape
    groups = lax.axis_size("grp")
    owners = lax.axis_size("row")
    total = (ITERS + 1) * width
    (kept,) = call(
        load_kernel,
        [shape(KEEP, edge, edge, dtype=BF16)],
        [pltpu.HBM],
        (tiles,),
        GRANT,
        [pltpu.SemaphoreType.DMA],
    )
    tables = (tile_rows, tile_cols, live_tiles, kept, tiles)
    spaces = [SMEM, SMEM, SMEM, VMEM, pltpu.HBM]
    rest = [pltpu.VMEM((count - KEEP, edge, edge), BF16), pltpu.SemaphoreType.DMA((CHUNKS,))]
    flops = 2 * count * width * edge * edge

    *slots, sent = call(
        functools.partial(init_kernel, groups, owners // 2),
        [shape(width, edge)] * groups + [shape(owners // 2, 2 * width, LANES, dtype=BF16)],
        [VMEM],
        (start_block,),
        4,
    )
    shift = dual_shift[None, :]
    def block(j, rows, coef, state):
        return call(
            functools.partial(block_kernel, j),
            [shape(total, total)] * 2
            + [shape(width, ITERS * width), shape(width, width)] * (j > 0),
            [VMEM] * (2 + len(state)),
            (rows, coef, *state),
            4,
        )

    before = coef = None
    basis = [slots]
    grams = []
    for step in range(ITERS):
        own = basis[step][0]
        same = same_core(sent)
        other = swapped(same, "row", 1)
        flat = [slot for slots in basis for slot in slots]
        (parts,) = call(
            functools.partial(back_kernel, groups, step),
            [shape(owners, 2 * width + EXTRA, LANES, dtype=BF16)],
            spaces + [VMEM] * (len(flat) + (step == 0)),
            (*tables, *flat, *[shift] * (step == 0)),
            GRANT,
            [pltpu.VMEM((owners, width, edge), F32), pltpu.VMEM((groups, width, edge), BF16), *rest],
            flops,
        )
        arrived = exchange(parts, "row")
        direct = call(
            functools.partial(ahead_kernel, groups),
            [shape(width, edge)]
            + [shape(width, edge, dtype=BF16)] * (groups - 1)
            + [shape(width, LANES)] * (step > 0),
            spaces + [VMEM, VMEM],
            (*tables, same, other),
            GRANT,
            [pltpu.VMEM((groups, width, edge), F32), *rest],
            flops,
        )
        grams += direct[groups:]
        direct = trade(direct[:groups])
        last = step == ITERS - 1
        second = shape(EXTRA, LANES) if last else shape(owners // 2, 2 * width + EXTRA, LANES, dtype=BF16)
        new, sent, *fresh = call(
            functools.partial(combine_kernel, groups, step),
            [shape(width, edge), second] + [shape(EXTRA, LANES)] * (step < 2),
            [VMEM] * (groups + 3 + 2 * (step > 0)),
            (arrived, *direct, own, shift, *[before, coef] * (step > 0)),
            4,
        )
        coef = fresh[0] if fresh else coef
        before = own
        basis.append(trade([new] * groups))

    flat = [slot for slots in basis for slot in slots]
    lines = width + width * width // LANES + EXTRA
    (part,) = call(
        functools.partial(gram_kernel, groups),
        [shape(lines, LANES)],
        [VMEM] * (1 + len(flat)),
        (sent, *flat),
        4,
    )
    (parts,) = call(
        pair_kernel,
        [shape(owners // 2, lines, LANES)],
        [VMEM, VMEM],
        (part, swapped(part, "row", 1)),
        4,
    )
    state = ()
    parts = same_core(parts)
    early = []
    for j, rows in enumerate(grams):
        *state, proj, fact = [*block(j, rows, coef, state), None, None][:4]
        early += [proj, fact] * (j > 0)
    return call(
        functools.partial(finish_kernel, groups),
        [shape(ITERS, width, ITERS * width), shape(ITERS, width, width), shape(width, row_count)],
        [VMEM] * (4 + len(early) + len(flat)),
        (parts, coef, *state, *early, *flat),
        8,
        [pltpu.VMEM((total, total), F32), pltpu.VMEM((total, total), F32)],
    )


def solution(mesh):
    in_specs = (
        P("grp", "row", None, None, None),
        P("grp", "row", None),
        P("grp", "row", None),
        P("grp", "row"),
        P("row"),
        P(None, "row"),
    )
    out_specs = (P(), P(), P(None, "row"))
    return jax.shard_map(
        per_device, mesh=mesh, in_specs=in_specs, out_specs=out_specs, check_vma=False
    )
```

```python
import functools

import jax
import jax.numpy as jnp
from jax import lax
from jax.experimental import pallas as pl
from jax.experimental.pallas import tpu as pltpu
from jax.sharding import PartitionSpec as P


ITERS = 4
FRESH = 0.1

KEEP = 12
CHUNKS = 5
GRANT = 50
LANES = 128
EXTRA = 8

F32 = jnp.float32
BF16 = jnp.bfloat16
HIGHEST = lax.Precision.HIGHEST
VMEM = pltpu.VMEM
SMEM = pltpu.SMEM


def spec(space):
    return pl.BlockSpec(memory_space=space)


def call(kernel, out_shape, in_spaces, operands, limit_mib, scratch=(), flops=2_000_000):
    return pl.pallas_call(
        kernel,
        out_shape=out_shape,
        in_specs=[spec(space) for space in in_spaces],
        out_specs=[spec(VMEM)] * len(out_shape),
        scratch_shapes=list(scratch),
        compiler_params=pltpu.CompilerParams(vmem_limit_bytes=limit_mib << 20),
        cost_estimate=pl.CostEstimate(flops=flops, bytes_accessed=1 << 20, transcendentals=0),
    )(*operands)


def shape(*dims, dtype=F32):
    return jax.ShapeDtypeStruct(dims, dtype)


def exchange(parts, axis):
    return lax.all_to_all(parts, axis, split_axis=0, concat_axis=0, tiled=True)


def same_core(parts):
    owners = lax.axis_size("row")
    groups = [list(range(core, owners, 2)) for core in range(2)]
    return lax.all_to_all(parts, "row", 0, 0, axis_index_groups=groups, tiled=True)


def swapped(value, axis, mask):
    return lax.ppermute(value, axis, [(i, i ^ mask) for i in range(lax.axis_size(axis))])


def trade(parts):
    arrived = [parts[0]]
    for k in range(1, len(parts)):
        arrived.append(swapped(parts[k], "grp", k))
    return arrived


def dot(left, right, dims):
    return lax.dot_general(
        left, right, (dims, ((), ())), precision=HIGHEST, preferred_element_type=F32
    )


def plain(left, right):
    return dot(left, right, ((1,), (0,)))


def across(left, right):
    return dot(left, right, ((1,), (1,)))


def halves(value):
    return jnp.concatenate([value[:, :LANES], value[:, LANES:]], 0)


def whole(ref, r, width):
    return jnp.concatenate([ref[r, pl.ds(0, width), :], ref[r, pl.ds(width, width), :]], 1)


def pieces(value):
    high = value.astype(BF16).astype(F32)
    rest = value - high
    middle = rest.astype(BF16).astype(F32)
    return high, middle, rest - middle


def stacked(*rows):
    line = lax.broadcasted_iota(jnp.int32, (EXTRA, rows[0].shape[1]), 0)
    value = jnp.zeros(line.shape, F32)
    for i, row in enumerate(rows):
        value = jnp.where(line == i, row, value)
    return value


def lane_sums(value):
    value = jnp.sum(value, 0, keepdims=True)
    parts = [value[:, i : i + LANES] for i in range(0, value.shape[1], LANES)]
    return sum(parts[1:], parts[0])


def squares(slots):
    parts = [slot[...] * slot[...] for slot in slots]
    return lane_sums((parts[0] + parts[1]) + (parts[2] + parts[3]))


def init_kernel(groups, copies, start_ref, *refs):
    slots, sent_ref = refs[:groups], refs[groups]
    edge = slots[0].shape[1]
    group = lax.axis_index("grp")
    for s in range(groups):
        block = group ^ s
        slots[s][...] = start_ref[:, pl.ds(pl.multiple_of(block * edge, edge), edge)]
    rounded = halves(slots[0][...]).astype(BF16)
    for r in range(copies):
        sent_ref[r] = rounded


def load_kernel(tiles_ref, out_ref, sem):
    copy = pltpu.make_async_copy(tiles_ref.at[0, 0, pl.ds(0, out_ref.shape[0])], out_ref, sem)
    copy.start()
    copy.wait()


def fetched(tiles_ref, rest, sems, c):
    per_chunk = rest.shape[0] // CHUNKS
    return pltpu.make_async_copy(
        tiles_ref.at[0, 0, pl.ds(KEEP + c * per_chunk, per_chunk)],
        rest.at[pl.ds(c * per_chunk, per_chunk)],
        sems.at[c],
    )


def fetch(tiles_ref, rest, sems):
    for c in range(CHUNKS):
        fetched(tiles_ref, rest, sems, c).start()


def clear(total):
    @pl.loop(0, total.shape[0])
    def _(i):
        total[i] = jnp.zeros(total.shape[1:], F32)


def each_tile(kept_ref, tiles_ref, rest, sems, visit):
    per_chunk = rest.shape[0] // CHUNKS
    for k in range(KEEP):
        visit(k, kept_ref[k])

    @pl.loop(0, CHUNKS)
    def _(c):
        fetched(tiles_ref, rest, sems, c).wait()
        for i in range(per_chunk):
            k = c * per_chunk + i
            visit(KEEP + k, rest[k])


def gram_blocks(vectors, group, ordered):
    groups = len(vectors[0])
    width = vectors[0][0].shape[0]
    for i, slots in enumerate(vectors):
        for s in range(groups):
            ordered[group ^ s, pl.ds(i * width, width), :] = slots[s][...]
    last = pl.ds((len(vectors) - 1) * width, width)
    value = across(ordered[0, last, :], ordered[0])
    for s in range(1, groups):
        value = value + across(ordered[s, last, :], ordered[s])
    return [value[:, i * width : (i + 1) * width] for i in range(len(vectors))]


def back_kernel(groups, steps, rows_ref, cols_ref, live_ref, kept_ref, tiles_ref, *refs):
    count = steps + 1
    vectors = [refs[i * groups : (i + 1) * groups] for i in range(count)]
    *shifts, out_ref, total, rounded, ordered, rest, sems = refs[count * groups :]
    fetch(tiles_ref, rest, sems)
    owners, width, _ = total.shape
    group = lax.axis_index("grp")
    live = live_ref[0, 0]
    clear(total)
    for s in range(groups):
        rounded[s] = vectors[steps][s][...].astype(BF16)
    grams = gram_blocks(vectors, group, ordered)
    if count * width < LANES:
        grams.append(jnp.zeros((width, LANES - count * width), F32))
    high, middle, low = pieces(jnp.concatenate(grams, 1))
    scales = []
    if steps == 0:
        scales = pieces(lane_sums(shifts[0][...]))[:2]
    elif steps == 1:
        scales = pieces(squares(vectors[1]))[:2] + pieces(squares(vectors[0]))[:2]
    for r in range(owners):
        value = stacked(high[r : r + 1], middle[r : r + 1], low[r : r + 1], *scales)
        out_ref[r, pl.ds(2 * width, EXTRA), :] = value.astype(BF16)

    def visit(k, tile):
        source = rows_ref[0, 0, k] ^ group
        product = lax.dot_general(
            rounded[source], tile, (((1,), (0,)), ((), ())), preferred_element_type=F32
        )
        total[cols_ref[0, 0, k]] += jnp.where(k < live, product, jnp.zeros_like(product))

    each_tile(kept_ref, tiles_ref, rest, sems, visit)
    for r in range(owners):
        out_ref[r, pl.ds(0, 2 * width), :] = halves(total[r]).astype(BF16)


def ahead_kernel(
    groups, rows_ref, cols_ref, live_ref, kept_ref, tiles_ref, same_ref, other_ref, *refs
):
    outs, (total, rest, sems) = refs[:groups], refs[-3:]
    fetch(tiles_ref, rest, sems)
    width = outs[0].shape[0]
    group = lax.axis_index("grp")
    core = lax.axis_index("row") & 1
    live = live_ref[0, 0]
    clear(total)

    def visit(k, tile):
        target = rows_ref[0, 0, k] ^ group
        col = cols_ref[0, 0, k]
        place = col >> 1
        vectors = jnp.where(
            (col & 1) == core, whole(same_ref, place, width), whole(other_ref, place, width)
        )
        product = lax.dot_general(
            vectors, tile, (((1,), (1,)), ((), ())), preferred_element_type=F32
        )
        total[target] += jnp.where(k < live, product, jnp.zeros_like(product))

    each_tile(kept_ref, tiles_ref, rest, sems, visit)
    for s in range(groups):
        outs[s][...] = total[s].astype(outs[s].dtype)
    if same_ref.shape[1] > 2 * width:
        rows = []
        for r in range(same_ref.shape[0]):
            mine = same_ref[r, pl.ds(2 * width, EXTRA), :].astype(F32)
            theirs = other_ref[r, pl.ds(2 * width, EXTRA), :].astype(F32)
            for three in (jnp.where(core == 0, mine, theirs), jnp.where(core == 0, theirs, mine)):
                rows.append(three[0:1] + (three[1:2] + three[2:3]))
        refs[groups][...] = jnp.concatenate(rows, 0)


def combine_kernel(groups, step, back_ref, *refs):
    direct = refs[:groups]
    now_ref, shift_ref = refs[groups : groups + 2]
    refs = refs[groups + 2 :]
    width, edge = now_ref.shape
    owners = back_ref.shape[0]
    image = direct[0][...]
    for s in range(1, groups):
        image = image + direct[s][...].astype(F32)
    for r in range(owners):
        image = image + whole(back_ref, r, width).astype(F32)
    sums = back_ref[0, pl.ds(2 * width, EXTRA), :].astype(F32)
    for r in range(1, owners):
        sums = sums + back_ref[r, pl.ds(2 * width, EXTRA), :].astype(F32)
    row = sums[0:1] + (sums[1:2] + sums[2:3])
    total = jnp.sum(sums, 1, keepdims=True)
    block = lax.axis_index("grp")
    diagonal = shift_ref[:, pl.ds(pl.multiple_of(block * edge, edge), edge)]
    line = lax.broadcasted_iota(jnp.int32, (EXTRA, LANES), 0)
    if step == 0:
        new_ref, sent_ref, coef_ref = refs
        shift = (total[3:4] + total[4:5]) * (1.0 / (owners * shift_ref.shape[1]))
        coef_ref[...] = jnp.broadcast_to(shift, coef_ref.shape)
        new = 0.5 * image + (shift - diagonal) * now_ref[...]
    else:
        before_ref, old_ref, new_ref, sent_ref = refs[:4]
        shift, pull = old_ref[0:1, 0:1], old_ref[1:2, 0:1]
        if step == 1:
            pull = (total[3:4] + total[4:5]) / (total[5:6] + total[6:7])
            refs[4][...] = jnp.where(line == 0, shift, pull)
        new = 0.5 * image + (shift - diagonal) * now_ref[...] - pull * before_ref[...]
    new_ref[...] = new
    if step == ITERS - 1:
        sent_ref[...] = jnp.broadcast_to(row, (EXTRA, LANES))
    else:
        rounded = halves(new).astype(BF16)
        extra = stacked(*pieces(row)).astype(BF16)
        for r in range(sent_ref.shape[0]):
            sent_ref[r, pl.ds(0, 2 * width), :] = rounded
            sent_ref[r, pl.ds(2 * width, EXTRA), :] = extra


def factor(block):
    width = block.shape[0]
    row_id = lax.broadcasted_iota(jnp.int32, (width, 2 * width), 0)
    col_id = lax.broadcasted_iota(jnp.int32, (width, 2 * width), 1)
    work = jnp.concatenate([block, jnp.zeros_like(block)], 1) + jnp.where(
        col_id == row_id + width, 1.0, 0.0
    )
    result = jnp.zeros_like(work)
    for k in range(0, width, 2):
        first = jnp.broadcast_to(work[:, k : k + 1], work.shape)
        second = jnp.broadcast_to(work[:, k + 1 : k + 2], work.shape)
        scale = lax.rsqrt(first[k : k + 1])
        link = first[k + 1 : k + 2] * scale
        scale2 = lax.rsqrt(second[k + 1 : k + 2] - link * link)
        row = work[k : k + 1] * scale
        row2 = (work[k + 1 : k + 2] - link * row) * scale2
        result = jnp.where(row_id == k, row, jnp.where(row_id == k + 1, row2, result))
        if k + 2 < width:
            column = first * scale
            column2 = (second - column * link) * scale2
            work = work - jnp.where(row_id > k + 1, column * row + column2 * row2, 0.0)
    return result[:, :width], result[:, width:]


def next_rows(j, gram_row, low, inv):
    width = gram_row.shape[0]
    here, done = pl.ds(j * width, width), pl.ds(0, j * width)
    low[here, :] = jnp.zeros((width, low.shape[1]), F32)
    inv[here, :] = jnp.zeros((width, inv.shape[1]), F32)
    schur = gram_row[:, j * width : (j + 1) * width]
    if j > 0:
        left = across(gram_row[:, : j * width], inv[done, done])
        schur = schur - across(left, left)
        back = plain(left, inv[done, done])
    upper, own_inverse = factor(schur)
    low[here, here] = upper.T
    inv[here, here] = own_inverse
    if j > 0:
        low[here, done] = left
        inv[here, done] = -plain(own_inverse, back)


def step_results(j, low, inv, coef_ref, width):
    used = (j + 1) * width
    shift, pull = coef_ref[0:1, 0:1], coef_ref[1:2, 0:1]
    value = low[pl.ds(width, used), :] - shift * low[pl.ds(0, used), :]
    if j > 0:
        value = value + pull * jnp.concatenate(
            [jnp.zeros((width, value.shape[1]), F32), low[pl.ds(0, j * width), :]], 0
        )
    image = plain(inv[pl.ds(j * width, width), pl.ds(0, used)], value)
    lane = lax.broadcasted_iota(jnp.int32, (width, ITERS * width), 1)
    square = (width, width)
    keep = lax.broadcasted_iota(jnp.int32, square, 0) >= lax.broadcasted_iota(jnp.int32, square, 1)
    return (
        jnp.where(lane < used, image[:, : ITERS * width], 0.0),
        jnp.where(keep, image[:, used : used + width], 0.0),
    )


def block_kernel(j, gram_ref, coef_ref, *refs):
    outs = 2 if j == 0 else 4
    olds, (low_ref, inv_ref) = refs[:-outs], refs[-outs:][:2]
    if j > 0:
        low_ref[...] = olds[0][...]
        inv_ref[...] = olds[1][...]
    next_rows(j, gram_ref[...], low_ref, inv_ref)
    if j > 0:
        refs[-2][...], refs[-1][...] = step_results(
            j - 1, low_ref, inv_ref, coef_ref, gram_ref.shape[0]
        )


def gram_kernel(groups, chunk_ref, *refs):
    out_ref, ordered = refs[-2:]
    vectors = [refs[i * groups : (i + 1) * groups] for i in range(ITERS + 1)]
    width = vectors[0][0].shape[0]
    grams = gram_blocks(vectors, lax.axis_index("grp"), ordered)
    parts = LANES // width
    rows = width // parts
    packed = jnp.concatenate([grams[ITERS][p * rows : (p + 1) * rows] for p in range(parts)], 1)
    out_ref[...] = jnp.concatenate(
        [jnp.concatenate(grams[:ITERS], 1), packed, jnp.broadcast_to(chunk_ref[0:1], (EXTRA, LANES))], 0
    )


def pair_kernel(mine_ref, theirs_ref, out_ref):
    last = mine_ref.shape[0] - EXTRA
    core = lax.axis_index("row") & 1
    line = lax.broadcasted_iota(jnp.int32, (EXTRA, LANES), 0)
    rows = jnp.where(line == core, mine_ref[pl.ds(last, EXTRA), :], theirs_ref[pl.ds(last, EXTRA), :])
    value = mine_ref[pl.ds(0, last), :] + theirs_ref[pl.ds(0, last), :]
    for r in range(out_ref.shape[0]):
        out_ref[r, pl.ds(0, last), :] = value
        out_ref[r, pl.ds(last, EXTRA), :] = rows


def finish_kernel(groups, parts_ref, coef_ref, old_low, old_inv, *refs):
    known = ITERS - 2
    early, refs = refs[: 2 * known], refs[2 * known :]
    vectors = [refs[i * groups : (i + 1) * groups] for i in range(ITERS + 1)]
    proj_ref, fact_ref, out_ref, fresh_ref, low, inv = refs[(ITERS + 1) * groups :]
    owners = parts_ref.shape[0]
    width, edge = vectors[0][0].shape
    group = lax.axis_index("grp")
    low[...] = old_low[...]
    inv[...] = old_inv[...]
    last = parts_ref.shape[1] - EXTRA
    rows = [parts_ref[r, pl.ds(last, EXTRA), :][0:2] for r in range(owners)]
    next_rows(ITERS - 1, jnp.concatenate(rows, 0), low, inv)
    sums = parts_ref[0, pl.ds(0, last), :]
    for r in range(1, owners):
        sums = sums + parts_ref[r, pl.ds(0, last), :]
    count = LANES // width
    corner = jnp.concatenate([sums[width:, p * width : (p + 1) * width] for p in range(count)], 0)
    next_rows(ITERS, jnp.concatenate([sums[:width], corner], 1), low, inv)
    square = low[...] * low[...]
    on_diagonal = lax.broadcasted_iota(jnp.int32, square.shape, 0) == lax.broadcasted_iota(
        jnp.int32, square.shape, 1
    )
    kept = jnp.sum(jnp.where(on_diagonal, square, 0.0), 1, keepdims=True)
    bad = jnp.where(kept > FRESH * jnp.sum(square, 1, keepdims=True), 0.0, 1.0)
    fresh_ref[...] = jnp.broadcast_to(jnp.max(bad, 0, keepdims=True), fresh_ref.shape)
    for j in range(known):
        proj_ref[j], fact_ref[j] = early[2 * j][...], early[2 * j + 1][...]
    for j in range(known, ITERS):
        proj_ref[j], fact_ref[j] = step_results(j, low, inv, coef_ref, width)
    for s in range(groups):
        value = plain(inv[pl.ds(ITERS * width, width), pl.ds(0, width)], vectors[0][s][...])
        for i in range(1, ITERS + 1):
            value = value + plain(
                inv[pl.ds(ITERS * width, width), pl.ds(i * width, width)], vectors[i][s][...]
            )
        block = group ^ s
        out_ref[:, pl.ds(pl.multiple_of(block * edge, edge), edge)] = value


def in_order(parts, dim):
    parts = jnp.moveaxis(parts, 0, dim)
    lengths = parts.shape
    return parts.reshape(*lengths[:dim], lengths[dim] * lengths[dim + 1], *lengths[dim + 2 :])


def copy_for_each(value, axis):
    size = lax.axis_size(axis)
    return lax.all_to_all(
        jnp.broadcast_to(value[None], (size, *value.shape)), axis, 0, 0, tiled=True
    )


def gathered_copies(value, axis, dim):
    return in_order(lax.all_gather(value, axis), dim)


def split_up(value, dim, size):
    before, after = (value.shape[:dim], value.shape[dim + 1 :])
    return jnp.moveaxis(value.reshape(*before, size, -1, *after), dim, 0)


def sent_and_summed(value, axis, dim):
    parts = split_up(value, dim, lax.axis_size(axis))
    arrived = lax.all_to_all(parts, axis, split_axis=0, concat_axis=0, tiled=True)
    return arrived.astype(jnp.float32).sum(axis=0)


def of_everyone(value, axis):
    return copy_for_each(value, axis).sum(axis=0)


def inner_product(left, right):
    return lax.dot_general(
        left,
        right,
        (((1,), (1,)), ((), ())),
        precision=lax.Precision.HIGHEST,
        preferred_element_type=jnp.float32,
    )


def apply_matrix(left, right):
    return jnp.dot(left, right, precision=lax.Precision.HIGHEST, preferred_element_type=jnp.float32)


def step_by_step(tiles, tile_rows, tile_cols, live_tiles, dual_shift, start_block):
    matrix = tiles[0, 0]
    rows_here = tile_rows[0, 0]
    cols_here = tile_cols[0, 0]
    tile_count = matrix.shape[0]
    tile_edge = matrix.shape[1]
    vec_width = start_block.shape[0]
    row_count = start_block.shape[1]
    group_count = lax.axis_size("grp")
    owner_count = lax.axis_size("row")
    owned_blocks = row_count // tile_edge
    quarter_tiles = owned_blocks // group_count
    column_tiles = quarter_tiles * owner_count
    group_index = lax.axis_index("grp")
    live_mask = (jnp.arange(tile_count) < live_tiles[0, 0]).astype(jnp.float32)
    row_table = (rows_here[:, None] == jnp.arange(owned_blocks)[None, :]).astype(
        jnp.float32
    ) * live_mask[:, None]
    col_table = (cols_here[:, None] == jnp.arange(column_tiles)[None, :]).astype(
        jnp.float32
    ) * live_mask[:, None]

    def partial_of(full_rows, group_rows):
        gathered = gathered_copies(group_rows, "row", 1)
        forward = jnp.einsum(
            "kbc,brc->kbr",
            jnp.take(gathered, cols_here, axis=1),
            matrix,
            preferred_element_type=jnp.float32,
        )
        direct = jnp.einsum("kbr,bi->kir", forward, row_table)
        backward = jnp.einsum(
            "kbr,brc->kbc",
            jnp.take(full_rows, rows_here, axis=1),
            matrix,
            preferred_element_type=jnp.float32,
        )
        spread = jnp.einsum("kbc,bj->kjc", backward, col_table)
        mine = sent_and_summed(spread.astype(jnp.bfloat16), "row", 1)
        placed = lax.dynamic_update_slice_in_dim(
            jnp.zeros_like(direct), mine, group_index * quarter_tiles, 1
        )
        return 0.5 * (direct + placed)

    def split_parts(vectors):
        rounded = vectors.astype(jnp.bfloat16).reshape(vec_width, owned_blocks, tile_edge)
        return (
            rounded,
            lax.dynamic_slice_in_dim(rounded, group_index * quarter_tiles, quarter_tiles, 1),
        )

    def finish_sum(partial_value):
        return of_everyone(partial_value, "grp").reshape(vec_width, row_count)

    def reduce_dots(values):
        return lax.psum(values, "row")

    def orthonormal(block, gram_matrix):
        lower_factor = jnp.linalg.cholesky(gram_matrix)
        return (
            lax.linalg.triangular_solve(lower_factor, block, left_side=True, lower=True),
            lower_factor,
        )

    current, _ = orthonormal(start_block, reduce_dots(inner_product(start_block, start_block)))
    total_cols = ITERS * vec_width
    basis_rows = jnp.zeros((total_cols, current.shape[1]), jnp.float32)
    projections = jnp.zeros((ITERS, vec_width, total_cols), jnp.float32)
    factors = jnp.zeros((ITERS, vec_width, vec_width), jnp.float32)

    def lanczos_step(step_index, state_now):
        current, basis_rows, projections, factors = state_now
        basis_rows = lax.dynamic_update_slice_in_dim(basis_rows, current, step_index * vec_width, 0)
        full_rows, group_rows = split_parts(current)
        image = finish_sum(partial_of(full_rows, group_rows)) - current * dual_shift[None, :]
        first_coef = reduce_dots(inner_product(image, basis_rows))
        image = image - apply_matrix(first_coef, basis_rows)
        gram_matrix = reduce_dots(inner_product(image, image))
        current, lower_factor = orthonormal(image, gram_matrix)
        projections = lax.dynamic_update_index_in_dim(projections, first_coef, step_index, 0)
        factors = lax.dynamic_update_index_in_dim(factors, lower_factor, step_index, 0)
        return (current, basis_rows, projections, factors)

    current, basis_rows, projections, factors = lax.fori_loop(
        0, ITERS, lanczos_step, (current, basis_rows, projections, factors)
    )
    return (projections, factors, current)


def per_device(tiles, tile_rows, tile_cols, live_tiles, dual_shift, start_block):
    count, edge = tiles.shape[2], tiles.shape[3]
    width, row_count = start_block.shape
    groups = lax.axis_size("grp")
    owners = lax.axis_size("row")
    total = (ITERS + 1) * width
    (kept,) = call(
        load_kernel,
        [shape(KEEP, edge, edge, dtype=BF16)],
        [pltpu.HBM],
        (tiles,),
        GRANT,
        [pltpu.SemaphoreType.DMA],
    )
    tables = (tile_rows, tile_cols, live_tiles, kept, tiles)
    spaces = [SMEM, SMEM, SMEM, VMEM, pltpu.HBM]
    rest = [pltpu.VMEM((count - KEEP, edge, edge), BF16), pltpu.SemaphoreType.DMA((CHUNKS,))]
    flops = 2 * count * width * edge * edge

    *slots, sent = call(
        functools.partial(init_kernel, groups, owners // 2),
        [shape(width, edge)] * groups + [shape(owners // 2, 2 * width, LANES, dtype=BF16)],
        [VMEM],
        (start_block,),
        4,
    )
    shift = dual_shift[None, :]

    def block(j, rows, coef, state):
        return call(
            functools.partial(block_kernel, j),
            [shape(total, total)] * 2
            + [shape(width, ITERS * width), shape(width, width)] * (j > 0),
            [VMEM] * (2 + len(state)),
            (rows, coef, *state),
            4,
        )

    before = coef = None
    basis = [slots]
    grams = []
    for step in range(ITERS):
        own = basis[step][0]
        same = same_core(sent)
        other = swapped(same, "row", 1)
        flat = [slot for slots in basis for slot in slots]
        (parts,) = call(
            functools.partial(back_kernel, groups, step),
            [shape(owners, 2 * width + EXTRA, LANES, dtype=BF16)],
            spaces + [VMEM] * (len(flat) + (step == 0)),
            (*tables, *flat, *[shift] * (step == 0)),
            GRANT,
            [
                pltpu.VMEM((owners, width, edge), F32),
                pltpu.VMEM((groups, width, edge), BF16),
                pltpu.VMEM((groups, (step + 1) * width, edge), F32),
                *rest,
            ],
            flops,
        )
        arrived = exchange(parts, "row")
        direct = call(
            functools.partial(ahead_kernel, groups),
            [shape(width, edge)]
            + [shape(width, edge, dtype=BF16)] * (groups - 1)
            + [shape(width, LANES)] * (step > 0),
            spaces + [VMEM, VMEM],
            (*tables, same, other),
            GRANT,
            [pltpu.VMEM((groups, width, edge), F32), *rest],
            flops,
        )
        grams += direct[groups:]
        direct = trade(direct[:groups])
        last = step == ITERS - 1
        second = shape(EXTRA, LANES) if last else shape(owners // 2, 2 * width + EXTRA, LANES, dtype=BF16)
        new, sent, *fresh = call(
            functools.partial(combine_kernel, groups, step),
            [shape(width, edge), second] + [shape(EXTRA, LANES)] * (step < 2),
            [VMEM] * (groups + 3 + 2 * (step > 0)),
            (arrived, *direct, own, shift, *[before, coef] * (step > 0)),
            4,
        )
        coef = fresh[0] if fresh else coef
        before = own
        basis.append(trade([new] * groups))

    flat = [slot for slots in basis for slot in slots]
    lines = width + width * width // LANES + EXTRA
    (part,) = call(
        functools.partial(gram_kernel, groups),
        [shape(lines, LANES)],
        [VMEM] * (1 + len(flat)),
        (sent, *flat),
        4,
        [pltpu.VMEM((groups, total, edge), F32)],
    )
    (parts,) = call(
        pair_kernel,
        [shape(owners // 2, lines, LANES)],
        [VMEM, VMEM],
        (part, swapped(part, "row", 1)),
        4,
    )
    state = ()
    parts = same_core(parts)
    early = []
    for j, rows in enumerate(grams):
        *state, proj, fact = [*block(j, rows, coef, state), None, None][:4]
        early += [proj, fact] * (j > 0)
    *results, bad = call(
        functools.partial(finish_kernel, groups),
        [
            shape(ITERS, width, ITERS * width),
            shape(ITERS, width, width),
            shape(width, row_count),
            shape(EXTRA, LANES),
        ],
        [VMEM] * (4 + len(early) + len(flat)),
        (parts, coef, *state, *early, *flat),
        8,
        [pltpu.VMEM((total, total), F32), pltpu.VMEM((total, total), F32)],
    )
    inputs = (tiles, tile_rows, tile_cols, live_tiles, dual_shift, start_block)
    return lax.cond(bad[0, 0] < 0.5, lambda: tuple(results), lambda: step_by_step(*inputs))


def solution(mesh):
    in_specs = (
        P("grp", "row", None, None, None),
        P("grp", "row", None),
        P("grp", "row", None),
        P("grp", "row"),
        P("row"),
        P(None, "row"),
    )
    out_specs = (P(), P(), P(None, "row"))
    return jax.shard_map(
        per_device, mesh=mesh, in_specs=in_specs, out_specs=out_specs, check_vma=False
    )
```

```python
import functools

import jax
import jax.numpy as jnp
from jax import lax
from jax.experimental import pallas as pl
from jax.experimental.pallas import tpu as pltpu
from jax.sharding import PartitionSpec as P


ITERS = 4
FRESH = 0.1

KEEP = 12
CHUNKS = 5
GRANT = 50
LANES = 128
EXTRA = 8

F32 = jnp.float32
BF16 = jnp.bfloat16
HIGHEST = lax.Precision.HIGHEST
VMEM = pltpu.VMEM
SMEM = pltpu.SMEM


def spec(space):
    return pl.BlockSpec(memory_space=space)


def call(kernel, out_shape, in_spaces, operands, limit_mib, scratch=(), flops=2_000_000):
    return pl.pallas_call(
        kernel,
        out_shape=out_shape,
        in_specs=[spec(space) for space in in_spaces],
        out_specs=[spec(SMEM if one.dtype == jnp.int32 else VMEM) for one in out_shape],
        scratch_shapes=list(scratch),
        compiler_params=pltpu.CompilerParams(vmem_limit_bytes=limit_mib << 20),
        cost_estimate=pl.CostEstimate(flops=flops, bytes_accessed=1 << 20, transcendentals=0),
    )(*operands)


def shape(*dims, dtype=F32):
    return jax.ShapeDtypeStruct(dims, dtype)


def exchange(parts, axis):
    return lax.all_to_all(parts, axis, split_axis=0, concat_axis=0, tiled=True)


def same_core(parts):
    owners = lax.axis_size("row")
    groups = [list(range(core, owners, 2)) for core in range(2)]
    return lax.all_to_all(parts, "row", 0, 0, axis_index_groups=groups, tiled=True)


def swapped(value, axis, mask):
    return lax.ppermute(value, axis, [(i, i ^ mask) for i in range(lax.axis_size(axis))])


def trade(parts):
    arrived = [parts[0]]
    for k in range(1, len(parts)):
        arrived.append(swapped(parts[k], "grp", k))
    return arrived


def dot(left, right, dims):
    return lax.dot_general(
        left, right, (dims, ((), ())), precision=HIGHEST, preferred_element_type=F32
    )


def plain(left, right):
    return dot(left, right, ((1,), (0,)))


def across(left, right):
    return dot(left, right, ((1,), (1,)))


def halves(value):
    return jnp.concatenate([value[:, :LANES], value[:, LANES:]], 0)


def whole(ref, r, width):
    return jnp.concatenate([ref[r, pl.ds(0, width), :], ref[r, pl.ds(width, width), :]], 1)


def pieces(value):
    high = value.astype(BF16).astype(F32)
    rest = value - high
    middle = rest.astype(BF16).astype(F32)
    return high, middle, rest - middle


def stacked(*rows):
    line = lax.broadcasted_iota(jnp.int32, (EXTRA, rows[0].shape[1]), 0)
    value = jnp.zeros(line.shape, F32)
    for i, row in enumerate(rows):
        value = jnp.where(line == i, row, value)
    return value


def lane_sums(value):
    value = jnp.sum(value, 0, keepdims=True)
    parts = [value[:, i : i + LANES] for i in range(0, value.shape[1], LANES)]
    return sum(parts[1:], parts[0])


def squares(slots):
    parts = [slot[...] * slot[...] for slot in slots]
    return lane_sums((parts[0] + parts[1]) + (parts[2] + parts[3]))


def init_kernel(groups, copies, start_ref, *refs):
    slots, sent_ref = refs[:groups], refs[groups]
    edge = slots[0].shape[1]
    group = lax.axis_index("grp")
    for s in range(groups):
        block = group ^ s
        slots[s][...] = start_ref[:, pl.ds(pl.multiple_of(block * edge, edge), edge)]
    rounded = halves(slots[0][...]).astype(BF16)
    for r in range(copies):
        sent_ref[r] = rounded


def load_kernel(tiles_ref, out_ref, sem):
    copy = pltpu.make_async_copy(tiles_ref.at[0, 0, pl.ds(0, out_ref.shape[0])], out_ref, sem)
    copy.start()
    copy.wait()


def fetched(tiles_ref, rest, sems, c):
    per_chunk = rest.shape[0] // CHUNKS
    return pltpu.make_async_copy(
        tiles_ref.at[0, 0, pl.ds(KEEP + c * per_chunk, per_chunk)],
        rest.at[pl.ds(c * per_chunk, per_chunk)],
        sems.at[c],
    )


def fetch(tiles_ref, rest, sems):
    for c in range(CHUNKS):
        fetched(tiles_ref, rest, sems, c).start()


def clear(total):
    @pl.loop(0, total.shape[0])
    def _(i):
        total[i] = jnp.zeros(total.shape[1:], F32)


def each_tile(kept_ref, tiles_ref, rest, sems, visit):
    per_chunk = rest.shape[0] // CHUNKS
    for k in range(KEEP):
        visit(k, kept_ref[k])

    @pl.loop(0, CHUNKS)
    def _(c):
        fetched(tiles_ref, rest, sems, c).wait()
        for i in range(per_chunk):
            k = c * per_chunk + i
            visit(KEEP + k, rest[k])


def gram_blocks(vectors, group, ordered):
    groups = len(vectors[0])
    width = vectors[0][0].shape[0]
    for i, slots in enumerate(vectors):
        for s in range(groups):
            ordered[group ^ s, pl.ds(i * width, width), :] = slots[s][...]
    last = pl.ds((len(vectors) - 1) * width, width)
    value = across(ordered[0, last, :], ordered[0])
    for s in range(1, groups):
        value = value + across(ordered[s, last, :], ordered[s])
    return [value[:, i * width : (i + 1) * width] for i in range(len(vectors))]


def back_kernel(groups, steps, rows_ref, cols_ref, live_ref, kept_ref, tiles_ref, *refs):
    count = steps + 1
    vectors = [refs[i * groups : (i + 1) * groups] for i in range(count)]
    *shifts, out_ref, total, rounded, ordered, rest, sems = refs[count * groups :]
    fetch(tiles_ref, rest, sems)
    owners, width, _ = total.shape
    group = lax.axis_index("grp")
    live = live_ref[0, 0]
    clear(total)
    for s in range(groups):
        rounded[s] = vectors[steps][s][...].astype(BF16)
    grams = gram_blocks(vectors, group, ordered)
    if count * width < LANES:
        grams.append(jnp.zeros((width, LANES - count * width), F32))
    high, middle, low = pieces(jnp.concatenate(grams, 1))
    scales = []
    if steps == 0:
        scales = pieces(lane_sums(shifts[0][...]))[:2]
    elif steps == 1:
        scales = pieces(squares(vectors[1]))[:2] + pieces(squares(vectors[0]))[:2]
    for r in range(owners):
        value = stacked(high[r : r + 1], middle[r : r + 1], low[r : r + 1], *scales)
        out_ref[r, pl.ds(2 * width, EXTRA), :] = value.astype(BF16)

    def visit(k, tile):
        source = rows_ref[0, 0, k] ^ group
        product = lax.dot_general(
            rounded[source], tile, (((1,), (0,)), ((), ())), preferred_element_type=F32
        )
        total[cols_ref[0, 0, k]] += jnp.where(k < live, product, jnp.zeros_like(product))

    each_tile(kept_ref, tiles_ref, rest, sems, visit)
    for r in range(owners):
        out_ref[r, pl.ds(0, 2 * width), :] = halves(total[r]).astype(BF16)


def ahead_kernel(
    groups, rows_ref, cols_ref, live_ref, kept_ref, tiles_ref, same_ref, other_ref, *refs
):
    outs, (total, rest, sems) = refs[:groups], refs[-3:]
    fetch(tiles_ref, rest, sems)
    width = outs[0].shape[0]
    group = lax.axis_index("grp")
    core = lax.axis_index("row") & 1
    live = live_ref[0, 0]
    clear(total)

    def visit(k, tile):
        target = rows_ref[0, 0, k] ^ group
        col = cols_ref[0, 0, k]
        place = col >> 1
        vectors = jnp.where(
            (col & 1) == core, whole(same_ref, place, width), whole(other_ref, place, width)
        )
        product = lax.dot_general(
            vectors, tile, (((1,), (1,)), ((), ())), preferred_element_type=F32
        )
        total[target] += jnp.where(k < live, product, jnp.zeros_like(product))

    each_tile(kept_ref, tiles_ref, rest, sems, visit)
    for s in range(groups):
        outs[s][...] = total[s].astype(outs[s].dtype)
    if same_ref.shape[1] > 2 * width:
        rows = []
        for r in range(same_ref.shape[0]):
            mine = same_ref[r, pl.ds(2 * width, EXTRA), :].astype(F32)
            theirs = other_ref[r, pl.ds(2 * width, EXTRA), :].astype(F32)
            for three in (jnp.where(core == 0, mine, theirs), jnp.where(core == 0, theirs, mine)):
                rows.append(three[0:1] + (three[1:2] + three[2:3]))
        refs[groups][...] = jnp.concatenate(rows, 0)


def combine_kernel(groups, step, back_ref, *refs):
    direct = refs[:groups]
    now_ref, shift_ref = refs[groups : groups + 2]
    refs = refs[groups + 2 :]
    width, edge = now_ref.shape
    owners = back_ref.shape[0]
    image = direct[0][...]
    for s in range(1, groups):
        image = image + direct[s][...].astype(F32)
    for r in range(owners):
        image = image + whole(back_ref, r, width).astype(F32)
    sums = back_ref[0, pl.ds(2 * width, EXTRA), :].astype(F32)
    for r in range(1, owners):
        sums = sums + back_ref[r, pl.ds(2 * width, EXTRA), :].astype(F32)
    row = sums[0:1] + (sums[1:2] + sums[2:3])
    total = jnp.sum(sums, 1, keepdims=True)
    block = lax.axis_index("grp")
    diagonal = shift_ref[:, pl.ds(pl.multiple_of(block * edge, edge), edge)]
    line = lax.broadcasted_iota(jnp.int32, (EXTRA, LANES), 0)
    if step == 0:
        new_ref, sent_ref, coef_ref = refs
        shift = (total[3:4] + total[4:5]) * (1.0 / (owners * shift_ref.shape[1]))
        coef_ref[...] = jnp.broadcast_to(shift, coef_ref.shape)
        new = 0.5 * image + (shift - diagonal) * now_ref[...]
    else:
        before_ref, old_ref, new_ref, sent_ref = refs[:4]
        shift, pull = old_ref[0:1, 0:1], old_ref[1:2, 0:1]
        if step == 1:
            pull = (total[3:4] + total[4:5]) / (total[5:6] + total[6:7])
            refs[4][...] = jnp.where(line == 0, shift, pull)
        new = 0.5 * image + (shift - diagonal) * now_ref[...] - pull * before_ref[...]
    new_ref[...] = new
    if step == ITERS - 1:
        sent_ref[...] = jnp.broadcast_to(row, (EXTRA, LANES))
    else:
        rounded = halves(new).astype(BF16)
        extra = stacked(*pieces(row)).astype(BF16)
        for r in range(sent_ref.shape[0]):
            sent_ref[r, pl.ds(0, 2 * width), :] = rounded
            sent_ref[r, pl.ds(2 * width, EXTRA), :] = extra


def factor(block):
    width = block.shape[0]
    row_id = lax.broadcasted_iota(jnp.int32, (width, 2 * width), 0)
    col_id = lax.broadcasted_iota(jnp.int32, (width, 2 * width), 1)
    work = jnp.concatenate([block, jnp.zeros_like(block)], 1) + jnp.where(
        col_id == row_id + width, 1.0, 0.0
    )
    result = jnp.zeros_like(work)
    for k in range(0, width, 2):
        first = jnp.broadcast_to(work[:, k : k + 1], work.shape)
        second = jnp.broadcast_to(work[:, k + 1 : k + 2], work.shape)
        scale = lax.rsqrt(first[k : k + 1])
        link = first[k + 1 : k + 2] * scale
        scale2 = lax.rsqrt(second[k + 1 : k + 2] - link * link)
        row = work[k : k + 1] * scale
        row2 = (work[k + 1 : k + 2] - link * row) * scale2
        result = jnp.where(row_id == k, row, jnp.where(row_id == k + 1, row2, result))
        if k + 2 < width:
            column = first * scale
            column2 = (second - column * link) * scale2
            work = work - jnp.where(row_id > k + 1, column * row + column2 * row2, 0.0)
    return result[:, :width], result[:, width:]


def next_rows(j, gram_row, low, inv):
    width = gram_row.shape[0]
    here, done = pl.ds(j * width, width), pl.ds(0, j * width)
    low[here, :] = jnp.zeros((width, low.shape[1]), F32)
    inv[here, :] = jnp.zeros((width, inv.shape[1]), F32)
    schur = gram_row[:, j * width : (j + 1) * width]
    if j > 0:
        left = across(gram_row[:, : j * width], inv[done, done])
        schur = schur - across(left, left)
        back = plain(left, inv[done, done])
    upper, own_inverse = factor(schur)
    low[here, here] = upper.T
    inv[here, here] = own_inverse
    if j > 0:
        low[here, done] = left
        inv[here, done] = -plain(own_inverse, back)


def step_results(j, low, inv, coef_ref, width):
    used = (j + 1) * width
    shift, pull = coef_ref[0:1, 0:1], coef_ref[1:2, 0:1]
    value = low[pl.ds(width, used), :] - shift * low[pl.ds(0, used), :]
    if j > 0:
        value = value + pull * jnp.concatenate(
            [jnp.zeros((width, value.shape[1]), F32), low[pl.ds(0, j * width), :]], 0
        )
    image = plain(inv[pl.ds(j * width, width), pl.ds(0, used)], value)
    lane = lax.broadcasted_iota(jnp.int32, (width, ITERS * width), 1)
    square = (width, width)
    keep = lax.broadcasted_iota(jnp.int32, square, 0) >= lax.broadcasted_iota(jnp.int32, square, 1)
    return (
        jnp.where(lane < used, image[:, : ITERS * width], 0.0),
        jnp.where(keep, image[:, used : used + width], 0.0),
    )


def block_kernel(j, gram_ref, coef_ref, *refs):
    outs = 2 if j == 0 else 4
    olds, (low_ref, inv_ref) = refs[:-outs], refs[-outs:][:2]
    if j > 0:
        low_ref[...] = olds[0][...]
        inv_ref[...] = olds[1][...]
    next_rows(j, gram_ref[...], low_ref, inv_ref)
    if j > 0:
        refs[-2][...], refs[-1][...] = step_results(
            j - 1, low_ref, inv_ref, coef_ref, gram_ref.shape[0]
        )


def gram_kernel(groups, chunk_ref, *refs):
    out_ref, ordered = refs[-2:]
    vectors = [refs[i * groups : (i + 1) * groups] for i in range(ITERS + 1)]
    width = vectors[0][0].shape[0]
    grams = gram_blocks(vectors, lax.axis_index("grp"), ordered)
    parts = LANES // width
    rows = width // parts
    packed = jnp.concatenate([grams[ITERS][p * rows : (p + 1) * rows] for p in range(parts)], 1)
    out_ref[...] = jnp.concatenate(
        [jnp.concatenate(grams[:ITERS], 1), packed, jnp.broadcast_to(chunk_ref[0:1], (EXTRA, LANES))], 0
    )


def pair_kernel(mine_ref, theirs_ref, out_ref):
    last = mine_ref.shape[0] - EXTRA
    core = lax.axis_index("row") & 1
    line = lax.broadcasted_iota(jnp.int32, (EXTRA, LANES), 0)
    rows = jnp.where(line == core, mine_ref[pl.ds(last, EXTRA), :], theirs_ref[pl.ds(last, EXTRA), :])
    value = mine_ref[pl.ds(0, last), :] + theirs_ref[pl.ds(0, last), :]
    for r in range(out_ref.shape[0]):
        out_ref[r, pl.ds(0, last), :] = value
        out_ref[r, pl.ds(last, EXTRA), :] = rows


def finish_kernel(groups, parts_ref, coef_ref, old_low, old_inv, *refs):
    known = ITERS - 2
    early, refs = refs[: 2 * known], refs[2 * known :]
    vectors = [refs[i * groups : (i + 1) * groups] for i in range(ITERS + 1)]
    proj_ref, fact_ref, out_ref, bad_ref, low, inv = refs[(ITERS + 1) * groups :]
    owners = parts_ref.shape[0]
    width, edge = vectors[0][0].shape
    group = lax.axis_index("grp")
    low[...] = old_low[...]
    inv[...] = old_inv[...]
    last = parts_ref.shape[1] - EXTRA
    rows = [parts_ref[r, pl.ds(last, EXTRA), :][0:2] for r in range(owners)]
    next_rows(ITERS - 1, jnp.concatenate(rows, 0), low, inv)
    sums = parts_ref[0, pl.ds(0, last), :]
    for r in range(1, owners):
        sums = sums + parts_ref[r, pl.ds(0, last), :]
    count = LANES // width
    corner = jnp.concatenate([sums[width:, p * width : (p + 1) * width] for p in range(count)], 0)
    next_rows(ITERS, jnp.concatenate([sums[:width], corner], 1), low, inv)
    square = low[...] * low[...]
    on_diagonal = lax.broadcasted_iota(jnp.int32, square.shape, 0) == lax.broadcasted_iota(
        jnp.int32, square.shape, 1
    )
    kept = jnp.sum(jnp.where(on_diagonal, square, 0.0), 1, keepdims=True)
    bad = jnp.where(kept > FRESH * jnp.sum(square, 1, keepdims=True), 0.0, 1.0)
    bad_ref[0, 0] = jnp.max(bad).astype(jnp.int32)
    for j in range(known):
        proj_ref[j], fact_ref[j] = early[2 * j][...], early[2 * j + 1][...]
    for j in range(known, ITERS):
        proj_ref[j], fact_ref[j] = step_results(j, low, inv, coef_ref, width)
    for s in range(groups):
        value = plain(inv[pl.ds(ITERS * width, width), pl.ds(0, width)], vectors[0][s][...])
        for i in range(1, ITERS + 1):
            value = value + plain(
                inv[pl.ds(ITERS * width, width), pl.ds(i * width, width)], vectors[i][s][...]
            )
        block = group ^ s
        out_ref[:, pl.ds(pl.multiple_of(block * edge, edge), edge)] = value


def in_order(parts, dim):
    parts = jnp.moveaxis(parts, 0, dim)
    lengths = parts.shape
    return parts.reshape(*lengths[:dim], lengths[dim] * lengths[dim + 1], *lengths[dim + 2 :])


def copy_for_each(value, axis):
    size = lax.axis_size(axis)
    return lax.all_to_all(
        jnp.broadcast_to(value[None], (size, *value.shape)), axis, 0, 0, tiled=True
    )


def gathered_copies(value, axis, dim):
    return in_order(lax.all_gather(value, axis), dim)


def split_up(value, dim, size):
    before, after = (value.shape[:dim], value.shape[dim + 1 :])
    return jnp.moveaxis(value.reshape(*before, size, -1, *after), dim, 0)


def sent_and_summed(value, axis, dim):
    parts = split_up(value, dim, lax.axis_size(axis))
    arrived = lax.all_to_all(parts, axis, split_axis=0, concat_axis=0, tiled=True)
    return arrived.astype(jnp.float32).sum(axis=0)


def of_everyone(value, axis):
    return copy_for_each(value, axis).sum(axis=0)


def inner_product(left, right):
    return lax.dot_general(
        left,
        right,
        (((1,), (1,)), ((), ())),
        precision=lax.Precision.HIGHEST,
        preferred_element_type=jnp.float32,
    )


def apply_matrix(left, right):
    return jnp.dot(left, right, precision=lax.Precision.HIGHEST, preferred_element_type=jnp.float32)


def step_by_step(tiles, tile_rows, tile_cols, live_tiles, dual_shift, start_block):
    matrix = tiles[0, 0]
    rows_here = tile_rows[0, 0]
    cols_here = tile_cols[0, 0]
    tile_count = matrix.shape[0]
    tile_edge = matrix.shape[1]
    vec_width = start_block.shape[0]
    row_count = start_block.shape[1]
    group_count = lax.axis_size("grp")
    owner_count = lax.axis_size("row")
    owned_blocks = row_count // tile_edge
    quarter_tiles = owned_blocks // group_count
    column_tiles = quarter_tiles * owner_count
    group_index = lax.axis_index("grp")
    live_mask = (jnp.arange(tile_count) < live_tiles[0, 0]).astype(jnp.float32)
    row_table = (rows_here[:, None] == jnp.arange(owned_blocks)[None, :]).astype(
        jnp.float32
    ) * live_mask[:, None]
    col_table = (cols_here[:, None] == jnp.arange(column_tiles)[None, :]).astype(
        jnp.float32
    ) * live_mask[:, None]

    def partial_of(full_rows, group_rows):
        gathered = gathered_copies(group_rows, "row", 1)
        forward = jnp.einsum(
            "kbc,brc->kbr",
            jnp.take(gathered, cols_here, axis=1),
            matrix,
            preferred_element_type=jnp.float32,
        )
        direct = jnp.einsum("kbr,bi->kir", forward, row_table)
        backward = jnp.einsum(
            "kbr,brc->kbc",
            jnp.take(full_rows, rows_here, axis=1),
            matrix,
            preferred_element_type=jnp.float32,
        )
        spread = jnp.einsum("kbc,bj->kjc", backward, col_table)
        mine = sent_and_summed(spread.astype(jnp.bfloat16), "row", 1)
        placed = lax.dynamic_update_slice_in_dim(
            jnp.zeros_like(direct), mine, group_index * quarter_tiles, 1
        )
        return 0.5 * (direct + placed)

    def split_parts(vectors):
        rounded = vectors.astype(jnp.bfloat16).reshape(vec_width, owned_blocks, tile_edge)
        return (
            rounded,
            lax.dynamic_slice_in_dim(rounded, group_index * quarter_tiles, quarter_tiles, 1),
        )

    def finish_sum(partial_value):
        return of_everyone(partial_value, "grp").reshape(vec_width, row_count)

    def reduce_dots(values):
        return lax.psum(values, "row")

    def orthonormal(block, gram_matrix):
        lower_factor = jnp.linalg.cholesky(gram_matrix)
        return (
            lax.linalg.triangular_solve(lower_factor, block, left_side=True, lower=True),
            lower_factor,
        )

    current, _ = orthonormal(start_block, reduce_dots(inner_product(start_block, start_block)))
    total_cols = ITERS * vec_width
    basis_rows = jnp.zeros((total_cols, current.shape[1]), jnp.float32)
    projections = jnp.zeros((ITERS, vec_width, total_cols), jnp.float32)
    factors = jnp.zeros((ITERS, vec_width, vec_width), jnp.float32)

    def lanczos_step(step_index, state_now):
        current, basis_rows, projections, factors = state_now
        basis_rows = lax.dynamic_update_slice_in_dim(basis_rows, current, step_index * vec_width, 0)
        full_rows, group_rows = split_parts(current)
        image = finish_sum(partial_of(full_rows, group_rows)) - current * dual_shift[None, :]
        first_coef = reduce_dots(inner_product(image, basis_rows))
        image = image - apply_matrix(first_coef, basis_rows)
        gram_matrix = reduce_dots(inner_product(image, image))
        current, lower_factor = orthonormal(image, gram_matrix)
        projections = lax.dynamic_update_index_in_dim(projections, first_coef, step_index, 0)
        factors = lax.dynamic_update_index_in_dim(factors, lower_factor, step_index, 0)
        return (current, basis_rows, projections, factors)

    current, basis_rows, projections, factors = lax.fori_loop(
        0, ITERS, lanczos_step, (current, basis_rows, projections, factors)
    )
    return (projections, factors, current)


def per_device(tiles, tile_rows, tile_cols, live_tiles, dual_shift, start_block):
    count, edge = tiles.shape[2], tiles.shape[3]
    width, row_count = start_block.shape
    groups = lax.axis_size("grp")
    owners = lax.axis_size("row")
    total = (ITERS + 1) * width
    (kept,) = call(
        load_kernel,
        [shape(KEEP, edge, edge, dtype=BF16)],
        [pltpu.HBM],
        (tiles,),
        GRANT,
        [pltpu.SemaphoreType.DMA],
    )
    tables = (tile_rows, tile_cols, live_tiles, kept, tiles)
    spaces = [SMEM, SMEM, SMEM, VMEM, pltpu.HBM]
    rest = [pltpu.VMEM((count - KEEP, edge, edge), BF16), pltpu.SemaphoreType.DMA((CHUNKS,))]
    flops = 2 * count * width * edge * edge

    *slots, sent = call(
        functools.partial(init_kernel, groups, owners // 2),
        [shape(width, edge)] * groups + [shape(owners // 2, 2 * width, LANES, dtype=BF16)],
        [VMEM],
        (start_block,),
        4,
    )
    shift = dual_shift[None, :]

    def block(j, rows, coef, state):
        return call(
            functools.partial(block_kernel, j),
            [shape(total, total)] * 2
            + [shape(width, ITERS * width), shape(width, width)] * (j > 0),
            [VMEM] * (2 + len(state)),
            (rows, coef, *state),
            4,
        )

    before = coef = None
    basis = [slots]
    grams = []
    for step in range(ITERS):
        own = basis[step][0]
        same = same_core(sent)
        other = swapped(same, "row", 1)
        flat = [slot for slots in basis for slot in slots]
        (parts,) = call(
            functools.partial(back_kernel, groups, step),
            [shape(owners, 2 * width + EXTRA, LANES, dtype=BF16)],
            spaces + [VMEM] * (len(flat) + (step == 0)),
            (*tables, *flat, *[shift] * (step == 0)),
            GRANT,
            [
                pltpu.VMEM((owners, width, edge), F32),
                pltpu.VMEM((groups, width, edge), BF16),
                pltpu.VMEM((groups, (step + 1) * width, edge), F32),
                *rest,
            ],
            flops,
        )
        arrived = exchange(parts, "row")
        direct = call(
            functools.partial(ahead_kernel, groups),
            [shape(width, edge)]
            + [shape(width, edge, dtype=BF16)] * (groups - 1)
            + [shape(width, LANES)] * (step > 0),
            spaces + [VMEM, VMEM],
            (*tables, same, other),
            GRANT,
            [pltpu.VMEM((groups, width, edge), F32), *rest],
            flops,
        )
        grams += direct[groups:]
        direct = trade(direct[:groups])
        last = step == ITERS - 1
        second = shape(EXTRA, LANES) if last else shape(owners // 2, 2 * width + EXTRA, LANES, dtype=BF16)
        new, sent, *fresh = call(
            functools.partial(combine_kernel, groups, step),
            [shape(width, edge), second] + [shape(EXTRA, LANES)] * (step < 2),
            [VMEM] * (groups + 3 + 2 * (step > 0)),
            (arrived, *direct, own, shift, *[before, coef] * (step > 0)),
            4,
        )
        coef = fresh[0] if fresh else coef
        before = own
        basis.append(trade([new] * groups))

    flat = [slot for slots in basis for slot in slots]
    lines = width + width * width // LANES + EXTRA
    (part,) = call(
        functools.partial(gram_kernel, groups),
        [shape(lines, LANES)],
        [VMEM] * (1 + len(flat)),
        (sent, *flat),
        4,
        [pltpu.VMEM((groups, total, edge), F32)],
    )
    (parts,) = call(
        pair_kernel,
        [shape(owners // 2, lines, LANES)],
        [VMEM, VMEM],
        (part, swapped(part, "row", 1)),
        4,
    )
    state = ()
    parts = same_core(parts)
    early = []
    for j, rows in enumerate(grams):
        *state, proj, fact = [*block(j, rows, coef, state), None, None][:4]
        early += [proj, fact] * (j > 0)
    *results, bad = call(
        functools.partial(finish_kernel, groups),
        [
            shape(ITERS, width, ITERS * width),
            shape(ITERS, width, width),
            shape(width, row_count),
            shape(1, 1, dtype=jnp.int32),
        ],
        [VMEM] * (4 + len(early) + len(flat)),
        (parts, coef, *state, *early, *flat),
        8,
        [pltpu.VMEM((total, total), F32), pltpu.VMEM((total, total), F32)],
    )
    inputs = (tiles, tile_rows, tile_cols, live_tiles, dual_shift, start_block)
    return lax.cond(bad[0, 0] == 0, lambda: tuple(results), lambda: step_by_step(*inputs))


def solution(mesh):
    in_specs = (
        P("grp", "row", None, None, None),
        P("grp", "row", None),
        P("grp", "row", None),
        P("grp", "row"),
        P("row"),
        P(None, "row"),
    )
    out_specs = (P(), P(), P(None, "row"))
    return jax.shard_map(
        per_device, mesh=mesh, in_specs=in_specs, out_specs=out_specs, check_vma=False
    )
```
